8 devices in a mesh: data: 2 (over z, y), expert: 4 (over x, core).
Axes of the slice: x: 2, y: 2, z: 1, core: 2. Of those that a mesh axis runs over, the one named last changes fastest.
Arguments:
- x_a: bfloat16 [1024, 1536], P(('data', 'expert')), parts along dimension 0
- x_b: bfloat16 [1024, 1536], P(('data', 'expert')), parts along dimension 0
- dy_b: bfloat16 [1024, 1536], P(('data', 'expert')), parts along dimension 0
- eid_a: int32 [1024, 8], P(('data', 'expert')), parts along dimension 0
- slot_a: int32 [1024, 8], P(('data', 'expert')), parts along dimension 0
- gate_a: bfloat16 [1024, 8], P(('data', 'expert')), parts along dimension 0
- eid_b: int32 [1024, 8], P(('data', 'expert')), parts along dimension 0
- slot_b: int32 [1024, 8], P(('data', 'expert')), parts along dimension 0
- gate_b: bfloat16 [1024, 8], P(('data', 'expert')), parts along dimension 0
- u_b: bfloat16 [80, 224, 1536], P(('data', 'expert')), parts along dimension 0
- norm_1: bfloat16 [1536], replicated
- norm_2: bfloat16 [1536], replicated
- w_q: bfloat16 [1536, 24, 64], replicated
- w_k: bfloat16 [1536, 8, 64], replicated
- w_v: bfloat16 [1536, 8, 64], replicated
- w_o: bfloat16 [24, 64, 1536], replicated
- w_1: bfloat16 [40, 1536, 512], P('expert')
- w_2: bfloat16 [40, 512, 1536], P('expert')
- w_3: bfloat16 [40, 1536, 512], P('expert')
Outputs:
- output 1: bfloat16 [1024, 1536], P(('data', 'expert')), parts along dimension 0
- output 2: bfloat16 [1024, 1536], P(('data', 'expert')), parts along dimension 0
- output 3: float32 [80, 1536, 512], P(('data', 'expert')), parts along dimension 0
- output 4: float32 [80, 512, 1536], P(('data', 'expert')), parts along dimension 0
- output 5: float32 [80, 1536, 512], P(('data', 'expert')), parts along dimension 0
- output 6: float32 [8, 1536, 24, 64], P(('data', 'expert')), parts along dimension 0
- output 7: float32 [8, 1536, 8, 64], P(('data', 'expert')), parts along dimension 0
- output 8: float32 [8, 1536, 8, 64], P(('data', 'expert')), parts along dimension 0
- output 9: float32 [8, 24, 64, 1536], P(('data', 'expert')), parts along dimension 0
- output 10: float32 [8, 1536], P(('data', 'expert')), parts along dimension 0
- output 11: float32 [8, 1536], P(('data', 'expert')), parts along dimension 0
There are 2 independent parts. The reference program is written for one: setup_inputs(seed, part) draws one part's arguments, and reference() takes and returns one part's arrays. A program takes and returns all parts, laid end to end along the dimension named above; an argument that names none is the same for every part.
All inputs are finite; a program needn't handle non-finite values.
Results may differ from the reference program's by a relative error of at most 0.0190968.
Values are sent between devices in bfloat16 or wider.
A program may use at most 1 GiB of HBM per device.

```python
import jax
import jax.numpy as jnp
from jax import lax

GROUP = 4
TOKENS = 128
MODEL_DIM = 1536
HEADS = 24
KV_HEADS = 8
HEAD_DIM = 64
EXPERTS = 40
FF_DIM = 512
TOP_K = 8
ROWS = GROUP * TOKENS
CAPACITY = ((2 * TOP_K * TOKENS + 8 * EXPERTS - 1) // (8 * EXPERTS)) * 8
HOT_ROWS = min(TOKENS, CAPACITY + CAPACITY // 4)
NORM_EPS = 1e-6


def draw_routing(route_key):
    key_score, key_hot = jax.random.split(route_key, 2)
    scores = jax.random.randint(key_score, (GROUP, TOKENS, EXPERTS), 0, 2 ** 20)
    hot_ids = jax.random.randint(key_hot, (GROUP,), 0, EXPERTS)
    boosted = (jnp.arange(TOKENS)[None, :, None] < HOT_ROWS) & (jnp.arange(EXPERTS)[None, None, :] == hot_ids[:, None, None])
    scores = (scores + boosted.astype(scores.dtype) * 2 ** 20) * EXPERTS + jnp.arange(EXPERTS)
    _, expert_ids = lax.top_k(scores, TOP_K)
    flat_ids = expert_ids.reshape(GROUP, TOKENS * TOP_K)
    onehot = (flat_ids[:, :, None] == jnp.arange(EXPERTS)[None, None, :]).astype(jnp.int32)
    arrival = jnp.sum((jnp.cumsum(onehot, axis=1) - onehot) * onehot, axis=2)
    slots = jnp.where(arrival < CAPACITY, arrival, -1)
    return expert_ids.reshape(ROWS, TOP_K).astype(jnp.int32), slots.reshape(ROWS, TOP_K).astype(jnp.int32)


def slot_columns(slots):
    device_of = jnp.arange(ROWS)[:, None] // TOKENS
    return jnp.where(slots >= 0, device_of * CAPACITY + slots, GROUP * CAPACITY)


def saved_inputs(value_key, expert_ids, slots):
    filled = jnp.zeros((EXPERTS, GROUP * CAPACITY), jnp.float32).at[expert_ids, slot_columns(slots)].set(1.0, mode='drop')
    values = jax.random.normal(value_key, (EXPERTS, GROUP * CAPACITY, MODEL_DIM), jnp.float32)
    return (values * filled[:, :, None]).astype(jnp.bfloat16)


def normal_draw(draw_key, dims, scale):
    return (jax.random.normal(draw_key, dims, jnp.float32) * scale).astype(jnp.bfloat16)


def setup_inputs(seed: int = 0, part: int = 0) -> dict:
    part_key = jax.random.fold_in(jax.random.key(seed), part)
    key_list = jax.random.split(part_key, 8)
    shared = jax.random.split(jax.random.key(seed + 1), 9)
    eid_a, slot_a = draw_routing(key_list[0])
    eid_b, slot_b = draw_routing(key_list[1])
    gate_a = (jax.random.uniform(key_list[2], (ROWS, TOP_K), jnp.float32, 0.5, 1.5) / TOP_K).astype(jnp.bfloat16)
    gate_b = (jax.random.uniform(key_list[3], (ROWS, TOP_K), jnp.float32, 0.5, 1.5) / TOP_K).astype(jnp.bfloat16)
    return {
        'x_a': normal_draw(key_list[4], (ROWS, MODEL_DIM), 1.0),
        'x_b': normal_draw(key_list[5], (ROWS, MODEL_DIM), 1.0),
        'dy_b': normal_draw(key_list[6], (ROWS, MODEL_DIM), 1.0),
        'eid_a': eid_a,
        'slot_a': slot_a,
        'gate_a': gate_a,
        'eid_b': eid_b,
        'slot_b': slot_b,
        'gate_b': gate_b,
        'u_b': saved_inputs(key_list[7], eid_b, slot_b),
        'norm_1': (1.0 + 0.3 * jax.random.normal(shared[0], (MODEL_DIM,), jnp.float32)).astype(jnp.bfloat16),
        'norm_2': (1.0 + 0.3 * jax.random.normal(shared[1], (MODEL_DIM,), jnp.float32)).astype(jnp.bfloat16),
        'w_q': normal_draw(shared[2], (MODEL_DIM, HEADS, HEAD_DIM), MODEL_DIM ** -0.5),
        'w_k': normal_draw(shared[3], (MODEL_DIM, KV_HEADS, HEAD_DIM), MODEL_DIM ** -0.5),
        'w_v': normal_draw(shared[4], (MODEL_DIM, KV_HEADS, HEAD_DIM), MODEL_DIM ** -0.5),
        'w_o': normal_draw(shared[5], (HEADS, HEAD_DIM, MODEL_DIM), 2.0 * (HEADS * HEAD_DIM) ** -0.5),
        'w_1': normal_draw(shared[6], (EXPERTS, MODEL_DIM, FF_DIM), MODEL_DIM ** -0.5),
        'w_2': normal_draw(shared[7], (EXPERTS, FF_DIM, MODEL_DIM), 3.0 * FF_DIM ** -0.5),
        'w_3': normal_draw(shared[8], (EXPERTS, MODEL_DIM, FF_DIM), MODEL_DIM ** -0.5),
    }


def rms_norm(values, gain):
    wide = values.astype(jnp.float32)
    scaled = wide * lax.rsqrt(jnp.mean(wide * wide, axis=-1, keepdims=True) + NORM_EPS)
    return (scaled * gain.astype(jnp.float32)).astype(jnp.bfloat16)


def add_rows(first, second):
    return (first.astype(jnp.float32) + second.astype(jnp.float32)).astype(jnp.bfloat16)


def attn_out(x_rows, norm_gain, w_q, w_k, w_v, w_o):
    normed = rms_norm(x_rows, norm_gain).astype(jnp.float32)
    query = jnp.einsum('td,dhe->the', normed, w_q.astype(jnp.float32)).astype(jnp.bfloat16)
    query = query.reshape(TOKENS, KV_HEADS, HEADS // KV_HEADS, HEAD_DIM).astype(jnp.float32)
    key_proj = jnp.einsum('td,dge->tge', normed, w_k.astype(jnp.float32)).astype(jnp.bfloat16).astype(jnp.float32)
    val_proj = jnp.einsum('td,dge->tge', normed, w_v.astype(jnp.float32)).astype(jnp.bfloat16).astype(jnp.float32)
    scores = jnp.einsum('tgre,mge->grtm', query, key_proj) * HEAD_DIM ** -0.5
    causal = jnp.arange(TOKENS)[:, None] >= jnp.arange(TOKENS)[None, :]
    scores = jnp.where(causal, scores, -1e30)
    probs = jax.nn.softmax(scores, axis=-1).astype(jnp.bfloat16).astype(jnp.float32)
    context = jnp.einsum('grtm,mge->tgre', probs, val_proj).astype(jnp.bfloat16)
    context = context.reshape(TOKENS, HEADS, HEAD_DIM).astype(jnp.float32)
    return jnp.einsum('the,hed->td', context, w_o.astype(jnp.float32)).astype(jnp.bfloat16)


def expert_forward(buf, w_1, w_2, w_3):
    act_1 = jnp.dot(buf, w_1, preferred_element_type=jnp.float32).astype(jnp.bfloat16).astype(jnp.float32)
    act_3 = jnp.dot(buf, w_3, preferred_element_type=jnp.float32).astype(jnp.bfloat16).astype(jnp.float32)
    hidden = (act_1 * jax.nn.sigmoid(act_1) * act_3).astype(jnp.bfloat16)
    return jnp.dot(hidden, w_2, preferred_element_type=jnp.float32).astype(jnp.bfloat16)


def expert_backward(saved, d_out, w_1, w_2, w_3):
    pre_1 = jnp.dot(saved, w_1, preferred_element_type=jnp.float32).astype(jnp.bfloat16).astype(jnp.float32)
    pre_3 = jnp.dot(saved, w_3, preferred_element_type=jnp.float32).astype(jnp.bfloat16).astype(jnp.float32)
    sigma = jax.nn.sigmoid(pre_1)
    silu_1 = pre_1 * sigma
    hidden = (silu_1 * pre_3).astype(jnp.bfloat16)
    grad_w2 = jnp.dot(hidden.T, d_out, preferred_element_type=jnp.float32)
    grad_hid = jnp.dot(d_out, w_2.T, preferred_element_type=jnp.float32).astype(jnp.bfloat16).astype(jnp.float32)
    grad_a1 = (grad_hid * pre_3 * sigma * (1.0 + pre_1 * (1.0 - sigma))).astype(jnp.bfloat16)
    grad_a3 = (grad_hid * silu_1).astype(jnp.bfloat16)
    grad_w1 = jnp.dot(saved.T, grad_a1, preferred_element_type=jnp.float32)
    grad_w3 = jnp.dot(saved.T, grad_a3, preferred_element_type=jnp.float32)
    grad_in = (jnp.dot(grad_a1, w_1.T, preferred_element_type=jnp.float32) + jnp.dot(grad_a3, w_3.T, preferred_element_type=jnp.float32)).astype(jnp.bfloat16)
    return grad_w1, grad_w2, grad_w3, grad_in


def pick_rows(buf, expert_ids, columns):
    padded = jnp.concatenate([buf, jnp.zeros((EXPERTS, 1, MODEL_DIM), buf.dtype)], axis=1)
    return padded[expert_ids, columns]


def reference(x_a, x_b, dy_b, eid_a, slot_a, gate_a, eid_b, slot_b, gate_b, u_b, norm_1, norm_2, w_q, w_k, w_v, w_o, w_1, w_2, w_3):
    def forward_rows(x_dev):
        return add_rows(x_dev, attn_out(x_dev, norm_1, w_q, w_k, w_v, w_o))
    h_a = lax.map(forward_rows, x_a.reshape(GROUP, TOKENS, MODEL_DIM)).reshape(ROWS, MODEL_DIM)
    u_a = rms_norm(h_a, norm_2)
    cols_a = slot_columns(slot_a)
    buf_a = jnp.zeros((EXPERTS, GROUP * CAPACITY, MODEL_DIM), jnp.bfloat16).at[eid_a, cols_a].set(jnp.broadcast_to(u_a[:, None, :], (ROWS, TOP_K, MODEL_DIM)), mode='drop')
    out_a = lax.map(lambda item: expert_forward(item[0], item[1], item[2], item[3]), (buf_a, w_1, w_2, w_3))
    picked = pick_rows(out_a, eid_a, cols_a).astype(jnp.float32)
    mixed = jnp.sum(gate_a.astype(jnp.float32)[:, :, None] * picked, axis=1)
    y_a = (h_a.astype(jnp.float32) + mixed).astype(jnp.bfloat16)
    cols_b = slot_columns(slot_b)
    grad_rows = (gate_b.astype(jnp.float32)[:, :, None] * dy_b.astype(jnp.float32)[:, None, :]).astype(jnp.bfloat16)
    d_out = jnp.zeros((EXPERTS, GROUP * CAPACITY, MODEL_DIM), jnp.bfloat16).at[eid_b, cols_b].set(grad_rows, mode='drop')
    grad_w1, grad_w2, grad_w3, grad_in = lax.map(lambda item: expert_backward(item[0], item[1], item[2], item[3], item[4]), (u_b, d_out, w_1, w_2, w_3))
    du_rows = jnp.sum(pick_rows(grad_in, eid_b, cols_b).astype(jnp.float32), axis=1).astype(jnp.bfloat16)
    def backward_rows(item):
        x_dev, dy_dev, du_dev = item
        attn_val, attn_pull = jax.vjp(attn_out, x_dev, norm_1, w_q, w_k, w_v, w_o)
        h_dev = add_rows(x_dev, attn_val)
        _, norm_pull = jax.vjp(rms_norm, h_dev, norm_2)
        dh_norm, grad_n2 = norm_pull(du_dev)
        dh_dev = add_rows(dy_dev, dh_norm)
        grad_x, grad_n1, grad_q, grad_k, grad_v, grad_o = attn_pull(dh_dev)
        return (add_rows(dh_dev, grad_x), grad_q.astype(jnp.float32), grad_k.astype(jnp.float32), grad_v.astype(jnp.float32), grad_o.astype(jnp.float32), grad_n1.astype(jnp.float32), grad_n2.astype(jnp.float32))
    dx_b, g_q, g_k, g_v, g_o, g_n1, g_n2 = lax.map(backward_rows, (x_b.reshape(GROUP, TOKENS, MODEL_DIM), dy_b.reshape(GROUP, TOKENS, MODEL_DIM), du_rows.reshape(GROUP, TOKENS, MODEL_DIM)))
    return (y_a, dx_b.reshape(ROWS, MODEL_DIM), grad_w1, grad_w2, grad_w3, g_q, g_k, g_v, g_o, g_n1, g_n2)
```

```python
import functools

import jax
import jax.numpy as jnp
from jax import lax
from jax.experimental import pallas as pl
from jax.experimental.pallas import tpu as pltpu
from jax.sharding import PartitionSpec as P

NORM_EPS = 1e-6
BF = jnp.bfloat16
F32 = jnp.float32
VMEM_LIMIT = 62 * 1024 * 1024


def nn(a, b):
    return lax.dot_general(a, b, (((1,), (0,)), ((), ())), preferred_element_type=F32)


def nt(a, b):
    return lax.dot_general(a, b, (((1,), (1,)), ((), ())), preferred_element_type=F32)


def tn(a, b):
    return lax.dot_general(a, b, (((0,), (0,)), ((), ())), preferred_element_type=F32)


def rms_scale(wide):
    return lax.rsqrt(jnp.mean(wide * wide, axis=-1, keepdims=True) + NORM_EPS)


def rms_rows(values, gain):
    wide = values.astype(F32)
    return (wide * rms_scale(wide) * gain).astype(BF)


def rms_pull(wide, gain, cot):
    scale = rms_scale(wide)
    scaled = wide * scale
    grad_gain = jnp.sum(cot * scaled, axis=0, keepdims=True).astype(BF).astype(F32)
    inner = cot * gain
    pull = jnp.mean(inner * wide, axis=-1, keepdims=True)
    grad = scale * inner - scaled * (scale * scale * pull)
    return grad.astype(BF).astype(F32), grad_gain


def probs_of(scores_t):
    rows = lax.broadcasted_iota(jnp.int32, scores_t.shape, 0)
    cols = lax.broadcasted_iota(jnp.int32, scores_t.shape, 1) % scores_t.shape[0]
    masked = jnp.where(rows <= cols, scores_t, -1e30)
    top = jnp.max(masked, axis=0, keepdims=True)
    unnorm = jnp.exp(masked - top)
    return unnorm / jnp.sum(unnorm, axis=0, keepdims=True)


def heads_to_lanes(ref, group, reps, dim, lanes):
    return jnp.concatenate([ref[(group * reps + r) * dim:(group * reps + r + 1) * dim, lanes] for r in range(reps)], axis=1)


def attn_fwd_kernel(kv_heads, reps, dim, x_a, x_b, n1, n2, wq_h, wk_h, wv_h, wo_h,
                    h_a, u_a, h_b, nb, qkv_b, ctx_b,
                    wq, wk, wv, wo, nrm, q_t, k_t, v_t, ctx, sems):
    copies = [pltpu.make_async_copy(s, d, sems.at[i]) for i, (s, d) in enumerate(((wk_h, wk), (wv_h, wv), (wq_h, wq), (wo_h, wo)))]
    for c in copies:
        c.start()
    tokens = x_a.shape[0]
    heads = kv_heads * reps
    gain1 = n1[...].astype(F32)
    nrm[0:tokens] = rms_rows(x_a[...], gain1)
    normed_b = rms_rows(x_b[...], gain1)
    nrm[tokens:2 * tokens] = normed_b
    nb[...] = normed_b
    copies[0].wait()
    k_t[...] = nt(wk[...], nrm[...]).astype(BF)
    copies[1].wait()
    v_t[...] = nt(wv[...], nrm[...]).astype(BF)
    copies[2].wait()
    step = heads * dim // 4
    for i in range(4):
        q_t[i * step:(i + 1) * step] = nt(wq[i * step:(i + 1) * step], nrm[...]).astype(BF)
    for b in range(2):
        lanes = slice(b * tokens, (b + 1) * tokens)
        for g in range(kv_heads):
            kg = k_t[g * dim:(g + 1) * dim, lanes]
            vg = v_t[g * dim:(g + 1) * dim, lanes]
            qg = heads_to_lanes(q_t, g, reps, dim, lanes)
            probs = probs_of(tn(kg, qg) * dim ** -0.5).astype(BF)
            out = nn(vg, probs).astype(BF)
            for r in range(reps):
                ctx[(g * reps + r) * dim:(g * reps + r + 1) * dim, lanes] = out[:, r * tokens:(r + 1) * tokens]
    second = slice(tokens, 2 * tokens)
    qkv_b[0:heads * dim] = q_t[:, second]
    qkv_b[heads * dim:(heads + kv_heads) * dim] = k_t[:, second]
    qkv_b[(heads + kv_heads) * dim:] = v_t[:, second]
    ctx_b[...] = ctx[:, second]
    copies[3].wait()
    attn = tn(ctx[...], wo[...]).astype(BF).astype(F32)
    ha = (x_a[...].astype(F32) + attn[0:tokens]).astype(BF)
    h_a[...] = ha
    h_b[...] = (x_b[...].astype(F32) + attn[tokens:2 * tokens]).astype(BF)
    u_a[...] = rms_rows(ha, n2[...].astype(F32))


def attn_fwd(x_a, x_b, n1, n2, wq, wk, wv, wo, kv_heads, reps, dim):
    tokens, model = x_a.shape
    q_dim, kv_dim = kv_heads * reps * dim, kv_heads * dim
    vm = pl.BlockSpec(memory_space=pltpu.VMEM)
    hb = pl.BlockSpec(memory_space=pl.ANY)
    row = jax.ShapeDtypeStruct((tokens, model), BF)
    return pl.pallas_call(
        functools.partial(attn_fwd_kernel, kv_heads, reps, dim),
        out_shape=(row, row, row, row, jax.ShapeDtypeStruct((q_dim + 2 * kv_dim, tokens), BF), jax.ShapeDtypeStruct((q_dim, tokens), BF)),
        in_specs=[vm] * 4 + [hb] * 4,
        out_specs=(vm,) * 6,
        scratch_shapes=[
            pltpu.VMEM((q_dim, model), BF), pltpu.VMEM((kv_dim, model), BF), pltpu.VMEM((kv_dim, model), BF), pltpu.VMEM((q_dim, model), BF),
            pltpu.VMEM((2 * tokens, model), BF), pltpu.VMEM((q_dim, 2 * tokens), BF), pltpu.VMEM((kv_dim, 2 * tokens), BF), pltpu.VMEM((kv_dim, 2 * tokens), BF),
            pltpu.VMEM((q_dim, 2 * tokens), BF), pltpu.SemaphoreType.DMA((4,)),
        ],
        compiler_params=pltpu.CompilerParams(vmem_limit_bytes=VMEM_LIMIT),
        cost_estimate=pl.CostEstimate(flops=10 ** 10, bytes_accessed=14 * 10 ** 6, transcendentals=0),
        name="attn_fwd",
    )(x_a, x_b, n1, n2, wq, wk, wv, wo)


def attn_bwd_kernel(kv_heads, reps, dim, s0, t0, dy, h_b, x_b, nb, qkv, ctx, n1, n2, wo_h, wq_h, wk_h, wv_h,
                    dx, gq, gk, gv, go, gn1, gn2,
                    wo, wq, wk, wv, oq, ok, ov, oo, dctx, dq, dk, dv, sems, osems):
    copies = [pltpu.make_async_copy(s, d, sems.at[i]) for i, (s, d) in enumerate(((wo_h, wo), (wq_h, wq), (wk_h, wk), (wv_h, wv)))]
    for c in copies:
        c.start()
    tokens = x_b.shape[0]
    q_dim, kv_dim = kv_heads * reps * dim, kv_heads * dim
    du = (s0[...] + t0[...]).astype(BF).astype(F32)
    grad_h, g2 = rms_pull(h_b[...].astype(F32), n2[...].astype(F32), du)
    gn2[...] = g2
    dh = (dy[...].astype(F32) + grad_h).astype(BF)
    copies[0].wait()
    outs = []

    def flush(src, dst):
        c = pltpu.make_async_copy(src, dst, osems.at[len(outs)])
        c.start()
        outs.append(c)

    step = q_dim // 4
    for i in range(4):
        dctx[i * step:(i + 1) * step] = nt(wo[i * step:(i + 1) * step], dh).astype(BF)
    for i in range(4):
        part = slice(i * step, (i + 1) * step)
        oo[part] = nn(ctx[part], dh).astype(BF).astype(F32)
        flush(oo.at[part], go.at[part])
    every = slice(0, tokens)
    normed = nb[...]
    for g in range(kv_heads):
        kv = slice(g * dim, (g + 1) * dim)
        kg = qkv[q_dim + g * dim:q_dim + (g + 1) * dim]
        vg = qkv[q_dim + kv_dim + g * dim:q_dim + kv_dim + (g + 1) * dim]
        qg = heads_to_lanes(qkv, g, reps, dim, every)
        dg = heads_to_lanes(dctx, g, reps, dim, every)
        probs = probs_of(tn(kg, qg) * dim ** -0.5)
        dprobs = tn(vg, dg).astype(BF).astype(F32)
        weighted = probs * dprobs
        dscores = ((weighted - probs * jnp.sum(weighted, axis=0, keepdims=True)) * dim ** -0.5).astype(BF)
        dv[kv] = nt(dg, probs.astype(BF)).astype(BF)
        dk[kv] = nt(qg, dscores).astype(BF)
        dqg = nn(kg, dscores).astype(BF)
        for r in range(reps):
            dq[(g * reps + r) * dim:(g * reps + r + 1) * dim] = dqg[:, r * tokens:(r + 1) * tokens]
        if g % 2 == 1:
            part = slice((g - 1) * reps * dim, (g + 1) * reps * dim)
            oq[part] = nn(dq[part], normed).astype(BF).astype(F32)
            flush(oq.at[part], gq.at[part])
    ok[...] = nn(dk[...], normed).astype(BF).astype(F32)
    flush(ok, gk)
    ov[...] = nn(dv[...], normed).astype(BF).astype(F32)
    flush(ov, gv)
    for c in copies[1:]:
        c.wait()
    dn = (tn(dq[...], wq[...]) + tn(dk[...], wk[...]) + tn(dv[...], wv[...])).astype(BF).astype(F32)
    grad_x, g1 = rms_pull(x_b[...].astype(F32), n1[...].astype(F32), dn)
    gn1[...] = g1
    dx[...] = (dh.astype(F32) + grad_x).astype(BF)
    for c in outs:
        c.wait()


def attn_bwd(s0, t0, dy, h_b, x_b, nb, qkv, ctx, n1, n2, wo, wq, wk, wv, kv_heads, reps, dim):
    tokens, model = x_b.shape
    q_dim, kv_dim = kv_heads * reps * dim, kv_heads * dim
    vm = pl.BlockSpec(memory_space=pltpu.VMEM)
    hb = pl.BlockSpec(memory_space=pl.ANY)
    n_out = 4 + kv_heads // 2 + 2
    return pl.pallas_call(
        functools.partial(attn_bwd_kernel, kv_heads, reps, dim),
        out_shape=(
            jax.ShapeDtypeStruct((tokens, model), BF), jax.ShapeDtypeStruct((q_dim, model), F32), jax.ShapeDtypeStruct((kv_dim, model), F32),
            jax.ShapeDtypeStruct((kv_dim, model), F32), jax.ShapeDtypeStruct((q_dim, model), F32), jax.ShapeDtypeStruct((1, model), F32), jax.ShapeDtypeStruct((1, model), F32),
        ),
        in_specs=[vm] * 10 + [hb] * 4,
        out_specs=(vm, hb, hb, hb, hb, vm, vm),
        scratch_shapes=[
            pltpu.VMEM((q_dim, model), BF), pltpu.VMEM((q_dim, model), BF), pltpu.VMEM((kv_dim, model), BF), pltpu.VMEM((kv_dim, model), BF),
            pltpu.VMEM((q_dim, model), F32), pltpu.VMEM((kv_dim, model), F32), pltpu.VMEM((kv_dim, model), F32), pltpu.VMEM((q_dim, model), F32),
            pltpu.VMEM((q_dim, tokens), BF), pltpu.VMEM((q_dim, tokens), BF), pltpu.VMEM((kv_dim, tokens), BF), pltpu.VMEM((kv_dim, tokens), BF),
            pltpu.SemaphoreType.DMA((4,)), pltpu.SemaphoreType.DMA((n_out,)),
        ],
        compiler_params=pltpu.CompilerParams(vmem_limit_bytes=VMEM_LIMIT),
        cost_estimate=pl.CostEstimate(flops=14 * 10 ** 9, bytes_accessed=40 * 10 ** 6, transcendentals=0),
        name="attn_bwd",
    )(s0, t0, dy, h_b, x_b, nb, qkv, ctx, n1, n2, wo, wq, wk, wv)


def route_rows(infos, base, me, expert):
    wide = [ref[...].astype(F32) for ref in infos]
    top_k = wide[0].shape[0] // 6
    def field(i):
        return jnp.concatenate([w[(base + i) * top_k:(base + i + 1) * top_k] for w in wide], axis=1)
    eid, slot, gate = field(0), field(1), field(2)
    hit = (eid == expert.astype(F32)) & (slot >= 0.0)
    slot_row = jnp.sum(jnp.where(hit, slot + 1.0, 0.0), axis=0, keepdims=True) - 1.0
    gate_row = jnp.sum(jnp.where(hit, gate, 0.0), axis=0, keepdims=True)
    return slot_row, gate_row


def expert_bwd_kernel(capacity, d0, d1, d2, d3, i0, i1, i2, i3, u, w1, w2, w3,
                      g1, g2, g3, p0, p1, p2, p3,
                      rows, pick_t, du_all, d_out, hid, da1, da3, o1, o2, o3, sems):
    e = pl.program_id(0)
    count = pl.num_programs(0)
    me = lax.axis_index('expert')
    tokens = d0.shape[0]
    slot_e = lax.rem(e, 2)
    cols, model = u.shape
    ff = w1.shape[1]
    group = 4
    padded = du_all.shape[1]

    @pl.when(e == 0)
    def _():
        for r, ref in enumerate((d0, d1, d2, d3)):
            rows[r * tokens:(r + 1) * tokens] = ref[...]

    slot_row, gate_row = route_rows((i0, i1, i2, i3), 3, me, me * count + e)
    lane_dev = lax.broadcasted_iota(jnp.int32, slot_row.shape, 1) // tokens
    device = jnp.bitwise_xor(lane_dev, me)
    col_row = jnp.where(slot_row >= 0.0, slot_row.astype(jnp.int32) + device * capacity, -1)
    hot = lax.broadcasted_iota(jnp.int32, (padded, group * tokens), 0) == col_row
    gated = jnp.where(hot, gate_row, 0.0).astype(BF)
    plain = jnp.where(hot, 1.0, 0.0).astype(BF)
    lanes = pl.ds(pl.multiple_of(e * padded, padded), padded)
    pick_t[:, lanes] = jnp.transpose(plain)
    d_out[...] = nn(gated[0:cols], rows[...]).astype(BF)

    def copies(s, idx):
        return [pltpu.make_async_copy(src.at[s], dst.at[idx], sems.at[s, i]) for i, (src, dst) in enumerate(((o1, g1), (o2, g2), (o3, g3)))]

    uv = u[...]
    dov = d_out[...]
    half = 256
    for n in range(ff // half):
        part = slice(n * half, (n + 1) * half)
        pre1 = nn(uv, w1[:, part]).astype(BF).astype(F32)
        pre3 = nn(uv, w3[:, part]).astype(BF).astype(F32)
        grad_hid = nt(dov, w2[part, :]).astype(BF).astype(F32)
        sigma = jax.nn.sigmoid(pre1)
        silu = pre1 * sigma
        hid[:, part] = (silu * pre3).astype(BF)
        da1[:, part] = (grad_hid * pre3 * sigma * (1.0 + pre1 * (1.0 - sigma))).astype(BF)
        da3[:, part] = (grad_hid * silu).astype(BF)

    @pl.when(e >= 2)
    def _():
        for c in copies(slot_e, e - 2):
            c.wait()

    fresh = copies(slot_e, e)
    for m in range(ff // 256):
        part = slice(m * 256, (m + 1) * 256)
        o2[slot_e, part] = tn(hid[:, part], dov)
    fresh[1].start()
    for m in range(model // 256):
        part = slice(m * 256, (m + 1) * 256)
        o1[slot_e, part] = tn(u[:, part], da1[...])
        o3[slot_e, part] = tn(u[:, part], da3[...])
    fresh[0].start()
    fresh[2].start()
    for n in range(model // 256):
        part = slice(n * 256, (n + 1) * 256)
        du_all[e, 0:cols, part] = (nt(da1[...], w1[part]) + nt(da3[...], w3[part])).astype(BF)
    du_all[e, cols:padded] = jnp.zeros((padded - cols, model), BF)

    @pl.when(e == count - 1)
    def _():
        for n in range(model // 256):
            part = slice(n * 256, (n + 1) * 256)
            mixed = nn(pick_t[...], du_all[:, :, part].reshape(pick_t.shape[1], 256))
            for r, ref in enumerate((p0, p1, p2, p3)):
                ref[:, part] = mixed[r * tokens:(r + 1) * tokens]
        for back in (1, 0):
            for c in copies(lax.rem(e + back, 2), e - back):
                c.wait()


def whole(shape):
    return pl.BlockSpec(shape, lambda e: (0,) * len(shape), pipeline_mode=pl.Buffered(1))


def expert_bwd(dys, infos, u, w1, w2, w3):
    tokens, model = dys[0].shape
    count, cols, _ = u.shape
    ff = w1.shape[2]
    padded = 256
    hb = pl.BlockSpec(memory_space=pl.ANY)
    part = jax.ShapeDtypeStruct((tokens, model), F32)
    return pl.pallas_call(
        functools.partial(expert_bwd_kernel, cols // 4),
        grid=(count,),
        out_shape=(jax.ShapeDtypeStruct((count, model, ff), F32), jax.ShapeDtypeStruct((count, ff, model), F32), jax.ShapeDtypeStruct((count, model, ff), F32), part, part, part, part),
        in_specs=[whole(dys[0].shape)] * 4 + [whole(infos[0].shape)] * 4 + [
            pl.BlockSpec((None, cols, model), lambda e: (e, 0, 0)),
            pl.BlockSpec((None, model, ff), lambda e: (e, 0, 0)),
            pl.BlockSpec((None, ff, model), lambda e: (e, 0, 0)),
            pl.BlockSpec((None, model, ff), lambda e: (e, 0, 0)),
        ],
        out_specs=(hb, hb, hb) + (whole((tokens, model)),) * 4,
        scratch_shapes=[
            pltpu.VMEM((4 * tokens, model), BF), pltpu.VMEM((4 * tokens, count * padded), BF), pltpu.VMEM((count, padded, model), BF),
            pltpu.VMEM((cols, model), BF), pltpu.VMEM((cols, ff), BF), pltpu.VMEM((cols, ff), BF), pltpu.VMEM((cols, ff), BF),
            pltpu.VMEM((2, model, ff), F32), pltpu.VMEM((2, ff, model), F32), pltpu.VMEM((2, model, ff), F32),
            pltpu.SemaphoreType.DMA((2, 3)),
        ],
        compiler_params=pltpu.CompilerParams(vmem_limit_bytes=VMEM_LIMIT, dimension_semantics=("arbitrary",)),
        cost_estimate=pl.CostEstimate(flops=50 * 10 ** 9, bytes_accessed=150 * 10 ** 6, transcendentals=0),
        name="expert_bwd",
    )(*dys, *infos, u, w1, w2, w3)


def expert_fwd_kernel(u0, u1, u2, u3, i0, i1, i2, i3, w1, w2, w3, p0, p1, p2, p3, rows, pick_t, out_all, late, late_t):
    e = pl.program_id(0)
    count = pl.num_programs(0)
    me = lax.axis_index('expert')
    tokens, model = u0.shape
    ff = w1.shape[1]
    chunk = 128

    @pl.when(e == 0)
    def _():
        late[...] = jnp.zeros_like(late)
        for r, ref in enumerate((u0, u1, u2, u3)):
            rows[r * tokens:(r + 1) * tokens] = ref[...]

    slot_row, gate_row = route_rows((i0, i1, i2, i3), 0, me, me * count + e)
    kept = jnp.where(slot_row >= 0.0, 1.0, 0.0)
    start = jnp.zeros((1, 1), F32)
    starts = []
    for r in range(4):
        starts.append(jnp.broadcast_to(start, (1, tokens)))
        start = start + jnp.sum(kept[:, r * tokens:(r + 1) * tokens], axis=1, keepdims=True)
    filled = jnp.sum(kept)
    col_row = jnp.where(slot_row >= 0.0, slot_row + jnp.concatenate(starts, axis=1), -1.0).astype(jnp.int32)

    def run(first):
        hot = lax.broadcasted_iota(jnp.int32, (chunk, 4 * tokens), 0) + first == col_row
        plain = jnp.where(hot, 1.0, 0.0).astype(BF)
        gated = jnp.where(hot, gate_row, 0.0).astype(BF)
        v = nn(plain, rows[...]).astype(BF)
        pieces = []
        for n in range(ff // 256):
            part = slice(n * 256, (n + 1) * 256)
            a1 = nn(v, w1[:, part]).astype(BF).astype(F32)
            a3 = nn(v, w3[:, part]).astype(BF).astype(F32)
            pieces.append((a1 * jax.nn.sigmoid(a1) * a3).astype(BF))
        hidden = jnp.concatenate(pieces, axis=1)
        return jnp.transpose(gated), nn(hidden, w2[...]).astype(BF)

    first_t, first_out = run(0)
    pick_t[:, pl.ds(pl.multiple_of(e * chunk, chunk), chunk)] = first_t
    out_all[e] = first_out

    @pl.when(filled > float(chunk))
    def _():
        more_t, more_out = run(chunk)
        late_t[...] = more_t
        for n in range(model // 256):
            part = slice(n * 256, (n + 1) * 256)
            late[:, part] += nn(late_t[...], more_out[:, part])

    @pl.when(e == count - 1)
    def _():
        for n in range(model // 256):
            part = slice(n * 256, (n + 1) * 256)
            mixed = late[:, part] + nn(pick_t[...], out_all[:, :, part].reshape(pick_t.shape[1], 256))
            for r, ref in enumerate((p0, p1, p2, p3)):
                ref[:, part] = mixed[r * tokens:(r + 1) * tokens]


def expert_fwd(us, infos, w1, w2, w3):
    tokens, model = us[0].shape
    count, _, ff = w1.shape
    chunk = 128
    part = jax.ShapeDtypeStruct((tokens, model), F32)
    return pl.pallas_call(
        expert_fwd_kernel,
        grid=(count,),
        out_shape=(part, part, part, part),
        in_specs=[whole(us[0].shape)] * 4 + [whole(infos[0].shape)] * 4 + [
            pl.BlockSpec((None, model, ff), lambda e: (e, 0, 0)),
            pl.BlockSpec((None, ff, model), lambda e: (e, 0, 0)),
            pl.BlockSpec((None, model, ff), lambda e: (e, 0, 0)),
        ],
        out_specs=(whole((tokens, model)),) * 4,
        scratch_shapes=[
            pltpu.VMEM((4 * tokens, model), BF), pltpu.VMEM((4 * tokens, count * chunk), BF), pltpu.VMEM((count, chunk, model), BF),
            pltpu.VMEM((4 * tokens, model), F32), pltpu.VMEM((4 * tokens, chunk), BF),
        ],
        compiler_params=pltpu.CompilerParams(vmem_limit_bytes=VMEM_LIMIT, dimension_semantics=("arbitrary",)),
        cost_estimate=pl.CostEstimate(flops=16 * 10 ** 9, bytes_accessed=50 * 10 ** 6, transcendentals=0),
        name="expert_fwd",
    )(*us, *infos, w1, w2, w3)


def solution(mesh):
    group = mesh.shape['expert']

    def hop(value, bit):
        return lax.ppermute(value, 'expert', [(i, i ^ bit) for i in range(group)])

    def spread(value):
        far = hop(value, 2)
        near = hop(value, 1)
        return value, near, far, hop(far, 1)

    def local_step(x_a, x_b, dy_b, eid_a, slot_a, gate_a, eid_b, slot_b, gate_b, u_b, norm_1, norm_2, w_q, w_k, w_v, w_o, w_1, w_2, w_3):
        model, heads, dim = w_q.shape
        kv_heads = w_k.shape[1]
        reps = heads // kv_heads
        info = jnp.concatenate([a.T.astype(BF) for a in (eid_a, slot_a, gate_a, eid_b, slot_b, gate_b)], axis=0)
        infos = spread(info)
        dys = spread(dy_b)
        n1, n2 = norm_1.reshape(1, model), norm_2.reshape(1, model)
        wq_t, wk_t, wv_t = (w.transpose(1, 2, 0).reshape(-1, model) for w in (w_q, w_k, w_v))
        wo = w_o.reshape(-1, model)
        h_a, u_a, h_b, nb, qkv_b, ctx_b = attn_fwd(x_a, x_b, n1, n2, wq_t, wk_t, wv_t, wo, kv_heads, reps, dim)
        us = spread(u_a)
        g1, g2, g3, b0, b1, b2, b3 = expert_bwd(dys, infos, u_b, w_1, w_2, w_3)
        mine_b = b0 + hop(b1, 1)
        far_b = hop(b2 + hop(b3, 1), 2)
        a0, a1, a2, a3 = expert_fwd(us, infos, w_1, w_2, w_3)
        mine_a = a0 + hop(a1, 1)
        far_a = hop(a2 + hop(a3, 1), 2)
        dx_b, g_q, g_k, g_v, g_o, g_n1, g_n2 = attn_bwd(mine_b, far_b, dy_b, h_b, x_b, nb, qkv_b, ctx_b, n1, n2, wo, wq_t, wk_t, wv_t, kv_heads, reps, dim)
        y_a = (h_a.astype(F32) + (mine_a + far_a)).astype(BF)
        g_q = g_q.reshape(heads, dim, model).transpose(2, 0, 1)
        g_k = g_k.reshape(kv_heads, dim, model).transpose(2, 0, 1)
        g_v = g_v.reshape(kv_heads, dim, model).transpose(2, 0, 1)
        g_o = g_o.reshape(heads, dim, model)
        return (y_a, dx_b, g1, g2, g3, g_q[None], g_k[None], g_v[None], g_o[None], g_n1, g_n2)

    row_spec = P(('data', 'expert'), None)
    cube_spec = P(('data', 'expert'), None, None)
    quad_spec = P(('data', 'expert'), None, None, None)
    expert_spec = P('expert', None, None)
    in_specs = (row_spec, row_spec, row_spec, row_spec, row_spec, row_spec, row_spec, row_spec, row_spec, cube_spec, P(), P(), P(), P(), P(), P(), expert_spec, expert_spec, expert_spec)
    out_specs = (row_spec, row_spec, cube_spec, cube_spec, cube_spec, quad_spec, quad_spec, quad_spec, quad_spec, row_spec, row_spec)
    return jax.shard_map(local_step, mesh=mesh, in_specs=in_specs, out_specs=out_specs, check_vma=False)
```

```python
import functools

import jax
import jax.numpy as jnp
from jax import lax
from jax.experimental import pallas as pl
from jax.experimental.pallas import tpu as pltpu
from jax.sharding import PartitionSpec as P


NORM_EPS = 1e-6
BF = jnp.bfloat16
F32 = jnp.float32
MIB = 1024 * 1024


def nn(a, b):
    return lax.dot_general(a, b, (((1,), (0,)), ((), ())), preferred_element_type=F32)


def nt(a, b):
    return lax.dot_general(a, b, (((1,), (1,)), ((), ())), preferred_element_type=F32)


def tn(a, b):
    return lax.dot_general(a, b, (((0,), (0,)), ((), ())), preferred_element_type=F32)


def row_of(ref):
    return ref[...].astype(F32).reshape(1, ref.shape[0])


def rms_scale(wide):
    return lax.rsqrt(jnp.mean(wide * wide, axis=-1, keepdims=True) + NORM_EPS)


def rms_rows(values, gain):
    wide = values.astype(F32)
    return (wide * rms_scale(wide) * gain).astype(BF)


def rms_pull(wide, gain, cot):
    scale = rms_scale(wide)
    scaled = wide * scale
    grad_gain = jnp.sum(cot * scaled, axis=0, keepdims=True).astype(BF).astype(F32)
    inner = cot * gain
    pull = jnp.mean(inner * wide, axis=-1, keepdims=True)
    grad = scale * inner - scaled * (scale * scale * pull)
    return grad.astype(BF).astype(F32), grad_gain


def probs_of(scores_t):
    rows = lax.broadcasted_iota(jnp.int32, scores_t.shape, 0)
    cols = lax.broadcasted_iota(jnp.int32, scores_t.shape, 1) % scores_t.shape[0]
    masked = jnp.where(rows <= cols, scores_t, -1e30)
    top = jnp.max(masked, axis=0, keepdims=True)
    unnorm = jnp.exp(masked - top)
    return unnorm / jnp.sum(unnorm, axis=0, keepdims=True)


def heads_to_lanes(ref, group, reps, dim, lanes):
    return jnp.concatenate([ref[(group * reps + r) * dim:(group * reps + r + 1) * dim, lanes] for r in range(reps)], axis=1)


def attn_fwd_kernel(kv_heads, reps, dim, x_a, x_b, n1, n2, wq_h, wk_h, wv_h, wo_h,
                    h_a, u_a, h_b, nb, qkv_b, ctx_b,
                    wq, wk, wv, wo, nrm, q_t, k_t, v_t, ctx, sems):
    copies = [pltpu.make_async_copy(s, d, sems.at[i]) for i, (s, d) in enumerate(((wk_h, wk), (wv_h, wv), (wq_h, wq), (wo_h, wo)))]
    for c in copies:
        c.start()
    tokens = x_a.shape[0]
    heads = kv_heads * reps
    gain1 = row_of(n1)
    nrm[0:tokens] = rms_rows(x_a[...], gain1)
    normed_b = rms_rows(x_b[...], gain1)
    nrm[tokens:2 * tokens] = normed_b
    nb[...] = normed_b
    copies[0].wait()
    k_t[...] = nt(wk[...], nrm[...]).astype(BF)
    copies[1].wait()
    v_t[...] = nt(wv[...], nrm[...]).astype(BF)
    copies[2].wait()
    step = heads * dim // 4
    for i in range(4):
        q_t[i * step:(i + 1) * step] = nt(wq[i * step:(i + 1) * step], nrm[...]).astype(BF)
    for b in range(2):
        lanes = slice(b * tokens, (b + 1) * tokens)
        for g in range(kv_heads):
            kg = k_t[g * dim:(g + 1) * dim, lanes]
            vg = v_t[g * dim:(g + 1) * dim, lanes]
            qg = heads_to_lanes(q_t, g, reps, dim, lanes)
            probs = probs_of(tn(kg, qg) * dim ** -0.5).astype(BF)
            out = nn(vg, probs).astype(BF)
            for r in range(reps):
                ctx[(g * reps + r) * dim:(g * reps + r + 1) * dim, lanes] = out[:, r * tokens:(r + 1) * tokens]
    second = slice(tokens, 2 * tokens)
    qkv_b[0:heads * dim] = q_t[:, second]
    qkv_b[heads * dim:(heads + kv_heads) * dim] = k_t[:, second]
    qkv_b[(heads + kv_heads) * dim:] = v_t[:, second]
    ctx_b[...] = ctx[:, second]
    copies[3].wait()
    attn = tn(ctx[...], wo[...]).astype(BF).astype(F32)
    ha = (x_a[...].astype(F32) + attn[0:tokens]).astype(BF)
    h_a[...] = ha
    h_b[...] = (x_b[...].astype(F32) + attn[tokens:2 * tokens]).astype(BF)
    u_a[...] = rms_rows(ha, row_of(n2))


def attn_fwd(x_a, x_b, n1, n2, wq, wk, wv, wo, kv_heads, reps, dim):
    tokens, model = x_a.shape
    q_dim, kv_dim = kv_heads * reps * dim, kv_heads * dim
    vm = pl.BlockSpec(memory_space=pltpu.VMEM)
    hb = pl.BlockSpec(memory_space=pl.ANY)
    row = jax.ShapeDtypeStruct((tokens, model), BF)
    return pl.pallas_call(
        functools.partial(attn_fwd_kernel, kv_heads, reps, dim),
        out_shape=(row, row, row, row, jax.ShapeDtypeStruct((q_dim + 2 * kv_dim, tokens), BF), jax.ShapeDtypeStruct((q_dim, tokens), BF)),
        in_specs=[vm] * 4 + [hb] * 4,
        out_specs=(vm,) * 6,
        scratch_shapes=[
            pltpu.VMEM((q_dim, model), BF), pltpu.VMEM((kv_dim, model), BF), pltpu.VMEM((kv_dim, model), BF), pltpu.VMEM((q_dim, model), BF),
            pltpu.VMEM((2 * tokens, model), BF), pltpu.VMEM((q_dim, 2 * tokens), BF), pltpu.VMEM((kv_dim, 2 * tokens), BF), pltpu.VMEM((kv_dim, 2 * tokens), BF),
            pltpu.VMEM((q_dim, 2 * tokens), BF), pltpu.SemaphoreType.DMA((4,)),
        ],
        compiler_params=pltpu.CompilerParams(vmem_limit_bytes=24 * MIB),
        cost_estimate=pl.CostEstimate(flops=10 ** 10, bytes_accessed=14 * 10 ** 6, transcendentals=0),
        name="attn_fwd",
    )(x_a, x_b, n1, n2, wq, wk, wv, wo)


def attn_bwd_kernel(kv_heads, reps, dim, s0, s1, t0, dy, h_b, x_b, nb, qkv, ctx, n1, n2, wo_h, wq_h, wk_h, wv_h,
                    dx, gq, gk, gv, go, gn1, gn2,
                    wo, wq, wk, wv, oq, ok, ov, oo, dctx, dq, dk, dv, sems, osems):
    copies = [pltpu.make_async_copy(s, d, sems.at[i]) for i, (s, d) in enumerate(((wo_h, wo), (wq_h, wq), (wk_h, wk), (wv_h, wv)))]
    for c in copies:
        c.start()
    tokens = x_b.shape[0]
    q_dim, kv_dim = kv_heads * reps * dim, kv_heads * dim
    du = ((s0[...] + s1[...]) + t0[...]).astype(BF).astype(F32)
    grad_h, g2 = rms_pull(h_b[...].astype(F32), row_of(n2), du)
    gn2[...] = g2
    dh = (dy[...].astype(F32) + grad_h).astype(BF)
    copies[0].wait()
    outs = []

    def flush(src, dst):
        c = pltpu.make_async_copy(src, dst, osems.at[len(outs)])
        c.start()
        outs.append(c)

    step = q_dim // 4
    for i in range(4):
        dctx[i * step:(i + 1) * step] = nt(wo[i * step:(i + 1) * step], dh).astype(BF)
    for i in range(4):
        part = slice(i * step, (i + 1) * step)
        oo[part] = nn(ctx[part], dh).astype(BF).astype(F32)
        flush(oo.at[part], go.at[part])
    every = slice(0, tokens)
    normed = nb[...]
    for g in range(kv_heads):
        kv = slice(g * dim, (g + 1) * dim)
        kg = qkv[q_dim + g * dim:q_dim + (g + 1) * dim]
        vg = qkv[q_dim + kv_dim + g * dim:q_dim + kv_dim + (g + 1) * dim]
        qg = heads_to_lanes(qkv, g, reps, dim, every)
        dg = heads_to_lanes(dctx, g, reps, dim, every)
        probs = probs_of(tn(kg, qg) * dim ** -0.5)
        dprobs = tn(vg, dg).astype(BF).astype(F32)
        weighted = probs * dprobs
        dscores = ((weighted - probs * jnp.sum(weighted, axis=0, keepdims=True)) * dim ** -0.5).astype(BF)
        dv[kv] = nt(dg, probs.astype(BF)).astype(BF)
        dk[kv] = nt(qg, dscores).astype(BF)
        dqg = nn(kg, dscores).astype(BF)
        for r in range(reps):
            dq[(g * reps + r) * dim:(g * reps + r + 1) * dim] = dqg[:, r * tokens:(r + 1) * tokens]
        if g % 2 == 1:
            part = slice((g - 1) * reps * dim, (g + 1) * reps * dim)
            oq[part] = nn(dq[part], normed).astype(BF).astype(F32)
            flush(oq.at[part], gq.at[part])
    ok[...] = nn(dk[...], normed).astype(BF).astype(F32)
    flush(ok, gk)
    ov[...] = nn(dv[...], normed).astype(BF).astype(F32)
    flush(ov, gv)
    for c in copies[1:]:
        c.wait()
    dn = (tn(dq[...], wq[...]) + tn(dk[...], wk[...]) + tn(dv[...], wv[...])).astype(BF).astype(F32)
    grad_x, g1 = rms_pull(x_b[...].astype(F32), row_of(n1), dn)
    gn1[...] = g1
    dx[...] = (dh.astype(F32) + grad_x).astype(BF)
    for c in outs:
        c.wait()


def attn_bwd(s0, s1, t0, dy, h_b, x_b, nb, qkv, ctx, n1, n2, wo, wq, wk, wv, kv_heads, reps, dim):
    tokens, model = x_b.shape
    q_dim, kv_dim = kv_heads * reps * dim, kv_heads * dim
    vm = pl.BlockSpec(memory_space=pltpu.VMEM)
    hb = pl.BlockSpec(memory_space=pl.ANY)
    n_out = 4 + kv_heads // 2 + 2
    return pl.pallas_call(
        functools.partial(attn_bwd_kernel, kv_heads, reps, dim),
        out_shape=(
            jax.ShapeDtypeStruct((tokens, model), BF), jax.ShapeDtypeStruct((q_dim, model), F32), jax.ShapeDtypeStruct((kv_dim, model), F32),
            jax.ShapeDtypeStruct((kv_dim, model), F32), jax.ShapeDtypeStruct((q_dim, model), F32), jax.ShapeDtypeStruct((1, model), F32), jax.ShapeDtypeStruct((1, model), F32),
        ),
        in_specs=[vm] * 11 + [hb] * 4,
        out_specs=(vm, hb, hb, hb, hb, vm, vm),
        scratch_shapes=[
            pltpu.VMEM((q_dim, model), BF), pltpu.VMEM((q_dim, model), BF), pltpu.VMEM((kv_dim, model), BF), pltpu.VMEM((kv_dim, model), BF),
            pltpu.VMEM((q_dim, model), F32), pltpu.VMEM((kv_dim, model), F32), pltpu.VMEM((kv_dim, model), F32), pltpu.VMEM((q_dim, model), F32),
            pltpu.VMEM((q_dim, tokens), BF), pltpu.VMEM((q_dim, tokens), BF), pltpu.VMEM((kv_dim, tokens), BF), pltpu.VMEM((kv_dim, tokens), BF),
            pltpu.SemaphoreType.DMA((4,)), pltpu.SemaphoreType.DMA((n_out,)),
        ],
        compiler_params=pltpu.CompilerParams(vmem_limit_bytes=48 * MIB),
        cost_estimate=pl.CostEstimate(flops=14 * 10 ** 9, bytes_accessed=40 * 10 ** 6, transcendentals=0),
        name="attn_bwd",
    )(s0, s1, t0, dy, h_b, x_b, nb, qkv, ctx, n1, n2, wo, wq, wk, wv)


def route_rows(infos, base, expert):
    wide = [ref[...].astype(F32) for ref in infos]
    top_k = wide[0].shape[0] // 6

    def field(i):
        return jnp.concatenate([w[(base + i) * top_k:(base + i + 1) * top_k] for w in wide], axis=1)

    eid, slot, gate = field(0), field(1), field(2)
    hit = (eid == expert.astype(F32)) & (slot >= 0.0)
    slot_row = jnp.sum(jnp.where(hit, slot + 1.0, 0.0), axis=0, keepdims=True) - 1.0
    gate_row = jnp.sum(jnp.where(hit, gate, 0.0), axis=0, keepdims=True)
    return slot_row, gate_row


def expert_bwd_kernel(capacity, d0, d1, d2, d3, i0, i1, i2, i3, u_h, w1_h, w2_h, w3_h,
                      g1, g2, g3, p0, p1, p2, p3,
                      rows, us, w1s, w2s, w3s, pick_t, du_all, d_out, hid, da1, da3, o1, o2, o3, parts, rsem, wsem, sems, psem):
    e = pl.program_id(0)
    count = pl.num_programs(0)
    me = lax.axis_index('expert')
    tokens = rows.shape[0] // 4
    slot_e = lax.rem(e, 2)
    ring = us.shape[0]
    cols, model = us.shape[1:]
    ff = w1s.shape[2]
    padded = du_all.shape[1]

    def fetch(idx):
        s = lax.rem(idx, ring)
        return [pltpu.make_async_copy(src.at[idx], dst.at[s], wsem.at[s, i]) for i, (src, dst) in enumerate(((u_h, us), (w1_h, w1s), (w3_h, w3s), (w2_h, w2s)))]

    def arrivals():
        return [pltpu.make_async_copy(ref, rows.at[r * tokens:(r + 1) * tokens], rsem.at[r]) for r, ref in enumerate((d0, d1, d2, d3))]

    @pl.when(e == 0)
    def _():
        for c in arrivals() + fetch(0) + fetch(1):
            c.start()
        for c in arrivals():
            c.wait()

    @pl.when(e + 2 < count)
    def _():
        for c in fetch(e + 2):
            c.start()

    slot_row, gate_row = route_rows((i0, i1, i2, i3), 3, me * count + e)
    lane_dev = lax.broadcasted_iota(jnp.int32, slot_row.shape, 1) // tokens
    device = jnp.bitwise_xor(lane_dev, me)
    col_row = jnp.where(slot_row >= 0.0, slot_row.astype(jnp.int32) + device * capacity, -1)
    hot = lax.broadcasted_iota(jnp.int32, (padded, 4 * tokens), 0) == col_row
    gated = jnp.where(hot, gate_row, 0.0).astype(BF)
    plain = jnp.where(hot, 1.0, 0.0).astype(BF)
    pick_t[:, pl.ds(pl.multiple_of(e * padded, padded), padded)] = jnp.transpose(plain)
    d_out[...] = nn(gated[0:cols], rows[...]).astype(BF)

    def copies(s, idx):
        return [pltpu.make_async_copy(src.at[s], dst.at[idx], sems.at[s, i]) for i, (src, dst) in enumerate(((o1, g1), (o2, g2), (o3, g3)))]

    for c in fetch(e):
        c.wait()
    now = lax.rem(e, ring)
    u, w1, w2, w3 = us.at[now], w1s.at[now], w2s.at[now], w3s.at[now]
    uv = u[...]
    dov = d_out[...]
    half = 256
    for n in range(ff // half):
        part = slice(n * half, (n + 1) * half)
        pre1 = nn(uv, w1[:, part]).astype(BF).astype(F32)
        pre3 = nn(uv, w3[:, part]).astype(BF).astype(F32)
        grad_hid = nt(dov, w2[part, :]).astype(BF).astype(F32)
        sigma = jax.nn.sigmoid(pre1)
        silu = pre1 * sigma
        hid[:, part] = (silu * pre3).astype(BF)
        da1[:, part] = (grad_hid * pre3 * sigma * (1.0 + pre1 * (1.0 - sigma))).astype(BF)
        da3[:, part] = (grad_hid * silu).astype(BF)

    @pl.when(e >= 2)
    def _():
        for c in copies(slot_e, e - 2):
            c.wait()

    fresh = copies(slot_e, e)
    for m in range(ff // 256):
        part = slice(m * 256, (m + 1) * 256)
        o2[slot_e, part] = tn(hid[:, part], dov)
    fresh[1].start()
    for m in range(model // 256):
        part = slice(m * 256, (m + 1) * 256)
        o1[slot_e, part] = tn(u[:, part], da1[...])
        o3[slot_e, part] = tn(u[:, part], da3[...])
    fresh[0].start()
    fresh[2].start()
    for n in range(model // 256):
        part = slice(n * 256, (n + 1) * 256)
        du_all[e, 0:cols, part] = (nt(da1[...], w1[part]) + nt(da3[...], w3[part])).astype(BF)
    du_all[e, cols:padded] = jnp.zeros((padded - cols, model), BF)

    @pl.when(e == count - 1)
    def _():
        for n in range(model // 256):
            part = slice(n * 256, (n + 1) * 256)
            parts[:, part] = nn(pick_t[...], du_all[:, :, part].reshape(pick_t.shape[1], 256))
        sends = [pltpu.make_async_copy(parts.at[r * tokens:(r + 1) * tokens], ref, psem.at[r]) for r, ref in enumerate((p0, p1, p2, p3))]
        for c in sends:
            c.start()
        for back in (1, 0):
            for c in copies(lax.rem(e + back, 2), e - back):
                c.wait()
        for c in sends:
            c.wait()


def whole(shape):
    return pl.BlockSpec(shape, lambda e: (0,) * len(shape), pipeline_mode=pl.Buffered(1))


def expert_bwd(dys, infos, u, w1, w2, w3):
    tokens, model = dys[0].shape
    count, cols, _ = u.shape
    ff = w1.shape[2]
    padded, ring = 256, 3
    hb = pl.BlockSpec(memory_space=pl.ANY)
    part = jax.ShapeDtypeStruct((tokens, model), F32)
    return pl.pallas_call(
        functools.partial(expert_bwd_kernel, cols // 4),
        grid=(count,),
        out_shape=(jax.ShapeDtypeStruct((count, model, ff), F32), jax.ShapeDtypeStruct((count, ff, model), F32), jax.ShapeDtypeStruct((count, model, ff), F32), part, part, part, part),
        in_specs=[hb] * 4 + [whole(infos[0].shape)] * 4 + [hb] * 4,
        out_specs=(hb,) * 7,
        scratch_shapes=[
            pltpu.VMEM((4 * tokens, model), BF),
            pltpu.VMEM((ring, cols, model), BF), pltpu.VMEM((ring, model, ff), BF), pltpu.VMEM((ring, ff, model), BF), pltpu.VMEM((ring, model, ff), BF),
            pltpu.VMEM((4 * tokens, count * padded), BF), pltpu.VMEM((count, padded, model), BF),
            pltpu.VMEM((cols, model), BF), pltpu.VMEM((cols, ff), BF), pltpu.VMEM((cols, ff), BF), pltpu.VMEM((cols, ff), BF),
            pltpu.VMEM((2, model, ff), F32), pltpu.VMEM((2, ff, model), F32), pltpu.VMEM((2, model, ff), F32),
            pltpu.VMEM((4 * tokens, model), F32),
            pltpu.SemaphoreType.DMA((4,)), pltpu.SemaphoreType.DMA((ring, 4)), pltpu.SemaphoreType.DMA((2, 3)), pltpu.SemaphoreType.DMA((4,)),
        ],
        compiler_params=pltpu.CompilerParams(vmem_limit_bytes=60 * MIB, dimension_semantics=("arbitrary",)),
        cost_estimate=pl.CostEstimate(flops=50 * 10 ** 9, bytes_accessed=150 * 10 ** 6, transcendentals=0),
        name="expert_bwd",
    )(*dys, *infos, u, w1, w2, w3)


def expert_fwd_kernel(u0, u1, u2, u3, i0, i1, i2, i3, w1_h, w2_h, w3_h, p0, p1, p2, p3,
                      rows, w1s, w2s, w3s, pick_t, out_all, late, late_t, rsem, wsem, psem):
    e = pl.program_id(0)
    count = pl.num_programs(0)
    me = lax.axis_index('expert')
    tokens = rows.shape[0] // 4
    ring, model, ff = w1s.shape
    chunk = 128

    def fetch(idx):
        s = lax.rem(idx, ring)
        return [pltpu.make_async_copy(src.at[idx], dst.at[s], wsem.at[s, i]) for i, (src, dst) in enumerate(((w1_h, w1s), (w3_h, w3s), (w2_h, w2s)))]

    def arrivals():
        return [pltpu.make_async_copy(ref, rows.at[r * tokens:(r + 1) * tokens], rsem.at[r]) for r, ref in enumerate((u0, u1, u2, u3))]

    @pl.when(e == 0)
    def _():
        for c in arrivals() + fetch(0) + fetch(1):
            c.start()
        late[...] = jnp.zeros_like(late)
        for c in arrivals():
            c.wait()

    @pl.when(e + 2 < count)
    def _():
        for c in fetch(e + 2):
            c.start()

    slot_row, gate_row = route_rows((i0, i1, i2, i3), 0, me * count + e)
    kept = jnp.where(slot_row >= 0.0, 1.0, 0.0)
    start = jnp.zeros((1, 1), F32)
    starts = []
    for r in range(4):
        starts.append(jnp.broadcast_to(start, (1, tokens)))
        start = start + jnp.sum(kept[:, r * tokens:(r + 1) * tokens], axis=1, keepdims=True)
    filled = jnp.sum(kept)
    col_row = jnp.where(slot_row >= 0.0, slot_row + jnp.concatenate(starts, axis=1), -1.0).astype(jnp.int32)

    for c in fetch(e):
        c.wait()
    now = lax.rem(e, ring)
    w1, w2, w3 = w1s.at[now], w2s.at[now], w3s.at[now]

    def run(first):
        hot = lax.broadcasted_iota(jnp.int32, (chunk, 4 * tokens), 0) + first == col_row
        plain = jnp.where(hot, 1.0, 0.0).astype(BF)
        gated = jnp.where(hot, gate_row, 0.0).astype(BF)
        v = nn(plain, rows[...]).astype(BF)
        pieces = []
        for n in range(ff // 256):
            part = slice(n * 256, (n + 1) * 256)
            a1 = nn(v, w1[:, part]).astype(BF).astype(F32)
            a3 = nn(v, w3[:, part]).astype(BF).astype(F32)
            pieces.append((a1 * jax.nn.sigmoid(a1) * a3).astype(BF))
        hidden = jnp.concatenate(pieces, axis=1)
        return jnp.transpose(gated), nn(hidden, w2[...]).astype(BF)

    first_t, first_out = run(0)
    pick_t[:, pl.ds(pl.multiple_of(e * chunk, chunk), chunk)] = first_t
    out_all[e] = first_out

    @pl.when(filled > float(chunk))
    def _():
        more_t, more_out = run(chunk)
        late_t[...] = more_t
        for n in range(model // 256):
            part = slice(n * 256, (n + 1) * 256)
            late[:, part] += nn(late_t[...], more_out[:, part])

    @pl.when(e == count - 1)
    def _():
        for n in range(model // 256):
            part = slice(n * 256, (n + 1) * 256)
            late[:, part] += nn(pick_t[...], out_all[:, :, part].reshape(pick_t.shape[1], 256))
        sends = [pltpu.make_async_copy(late.at[r * tokens:(r + 1) * tokens], ref, psem.at[r]) for r, ref in enumerate((p0, p1, p2, p3))]
        for c in sends:
            c.start()
        for c in sends:
            c.wait()


def expert_fwd(us, infos, w1, w2, w3):
    tokens, model = us[0].shape
    count, _, ff = w1.shape
    chunk, ring = 128, 3
    part = jax.ShapeDtypeStruct((tokens, model), F32)
    hb = pl.BlockSpec(memory_space=pl.ANY)
    return pl.pallas_call(
        expert_fwd_kernel,
        grid=(count,),
        out_shape=(part, part, part, part),
        in_specs=[hb] * 4 + [whole(infos[0].shape)] * 4 + [hb] * 3,
        out_specs=(hb,) * 4,
        scratch_shapes=[
            pltpu.VMEM((4 * tokens, model), BF),
            pltpu.VMEM((ring, model, ff), BF), pltpu.VMEM((ring, ff, model), BF), pltpu.VMEM((ring, model, ff), BF),
            pltpu.VMEM((4 * tokens, count * chunk), BF), pltpu.VMEM((count, chunk, model), BF),
            pltpu.VMEM((4 * tokens, model), F32), pltpu.VMEM((4 * tokens, chunk), BF),
            pltpu.SemaphoreType.DMA((4,)), pltpu.SemaphoreType.DMA((ring, 3)), pltpu.SemaphoreType.DMA((4,)),
        ],
        compiler_params=pltpu.CompilerParams(vmem_limit_bytes=36 * MIB, dimension_semantics=("arbitrary",)),
        cost_estimate=pl.CostEstimate(flops=16 * 10 ** 9, bytes_accessed=50 * 10 ** 6, transcendentals=0),
        name="expert_fwd",
    )(*us, *infos, w1, w2, w3)


def pack_kernel(*refs):
    refs[-1][...] = jnp.concatenate([r[...].astype(F32) for r in refs[:-1]], axis=0).astype(BF)


def pack(fields):
    vm = pl.BlockSpec(memory_space=pltpu.VMEM)
    rows = sum(f.shape[0] for f in fields)
    return pl.pallas_call(
        pack_kernel,
        out_shape=jax.ShapeDtypeStruct((rows, fields[0].shape[1]), BF),
        in_specs=[vm] * len(fields), out_specs=vm,
        compiler_params=pltpu.CompilerParams(vmem_limit_bytes=4 * MIB),
        name="pack",
    )(*fields)


def solution(mesh):
    group = mesh.shape['expert']

    def hop(value, bits):
        return lax.ppermute(value, 'expert', [(i, i ^ bits) for i in range(group)])

    def local_step(x_a, x_b, dy_b, eid_a, slot_a, gate_a, eid_b, slot_b, gate_b, u_b, norm_1, norm_2, w_q, w_k, w_v, w_o, w_1, w_2, w_3):
        model, heads, dim = w_q.shape
        kv_heads = w_k.shape[1]
        reps = heads // kv_heads
        info = pack([a.T for a in (eid_a, slot_a, gate_a, eid_b, slot_b, gate_b)])
        dy2 = hop(dy_b, 2)
        dy1 = hop(dy_b, 1)
        infos = (info, hop(info, 1), hop(info, 2), hop(info, 3))
        wq_t, wk_t, wv_t = (w.transpose(1, 2, 0).reshape(-1, model) for w in (w_q, w_k, w_v))
        wo = w_o.reshape(-1, model)
        h_a, u_a, h_b, nb, qkv_b, ctx_b = attn_fwd(x_a, x_b, norm_1, norm_2, wq_t, wk_t, wv_t, wo, kv_heads, reps, dim)
        dy3 = hop(dy2, 1)
        us = (u_a, hop(u_a, 1), hop(u_a, 2), hop(u_a, 3))
        g1, g2, g3, b0, b1, b2, b3 = expert_bwd((dy_b, dy1, dy2, dy3), infos, u_b, w_1, w_2, w_3)
        far_b = hop(b2 + hop(b3, 1), 2)
        near_b = hop(b1, 1)
        a0, a1, a2, a3 = expert_fwd(us, infos, w_1, w_2, w_3)
        far_a = hop(a2 + hop(a3, 1), 2)
        near_a = hop(a1, 1)
        dx_b, g_q, g_k, g_v, g_o, g_n1, g_n2 = attn_bwd(b0, near_b, far_b, dy_b, h_b, x_b, nb, qkv_b, ctx_b, norm_1, norm_2, wo, wq_t, wk_t, wv_t, kv_heads, reps, dim)
        y_a = (h_a.astype(F32) + ((a0 + near_a) + far_a)).astype(BF)
        g_q = g_q.reshape(heads, dim, model).transpose(2, 0, 1)
        g_k = g_k.reshape(kv_heads, dim, model).transpose(2, 0, 1)
        g_v = g_v.reshape(kv_heads, dim, model).transpose(2, 0, 1)
        g_o = g_o.reshape(heads, dim, model)
        return (y_a, dx_b, g1, g2, g3, g_q[None], g_k[None], g_v[None], g_o[None], g_n1, g_n2)

    row_spec = P(('data', 'expert'), None)
    cube_spec = P(('data', 'expert'), None, None)
    quad_spec = P(('data', 'expert'), None, None, None)
    expert_spec = P('expert', None, None)
    in_specs = (row_spec, row_spec, row_spec, row_spec, row_spec, row_spec, row_spec, row_spec, row_spec, cube_spec, P(), P(), P(), P(), P(), P(), expert_spec, expert_spec, expert_spec)
    out_specs = (row_spec, row_spec, cube_spec, cube_spec, cube_spec, quad_spec, quad_spec, quad_spec, quad_spec, row_spec, row_spec)
    return jax.shard_map(local_step, mesh=mesh, in_specs=in_specs, out_specs=out_specs, check_vma=False)
```

```python
import functools

import jax
import jax.numpy as jnp
from jax import lax
from jax.experimental import pallas as pl
from jax.experimental.pallas import tpu as pltpu
from jax.sharding import PartitionSpec as P


NORM_EPS = 1e-6
BF = jnp.bfloat16
F32 = jnp.float32
MIB = 1024 * 1024
CHUNK = 128


def nn(a, b):
    return lax.dot_general(a, b, (((1,), (0,)), ((), ())), preferred_element_type=F32)


def nt(a, b):
    return lax.dot_general(a, b, (((1,), (1,)), ((), ())), preferred_element_type=F32)


def tn(a, b):
    return lax.dot_general(a, b, (((0,), (0,)), ((), ())), preferred_element_type=F32)


def row_of(ref):
    return ref[...].astype(F32).reshape(1, ref.shape[0])


def rms_scale(wide):
    return lax.rsqrt(jnp.mean(wide * wide, axis=-1, keepdims=True) + NORM_EPS)


def rms_rows(values, gain):
    wide = values.astype(F32)
    return (wide * rms_scale(wide) * gain).astype(BF)


def rms_pull(wide, gain, cot):
    scale = rms_scale(wide)
    scaled = wide * scale
    grad_gain = jnp.sum(cot * scaled, axis=0, keepdims=True).astype(BF).astype(F32)
    inner = cot * gain
    pull = jnp.mean(inner * wide, axis=-1, keepdims=True)
    grad = scale * inner - scaled * (scale * scale * pull)
    return grad.astype(BF).astype(F32), grad_gain


def probs_of(scores_t):
    rows = lax.broadcasted_iota(jnp.int32, scores_t.shape, 0)
    cols = lax.broadcasted_iota(jnp.int32, scores_t.shape, 1) % scores_t.shape[0]
    masked = jnp.where(rows <= cols, scores_t, -1e30)
    top = jnp.max(masked, axis=0, keepdims=True)
    unnorm = jnp.exp(masked - top)
    return unnorm / jnp.sum(unnorm, axis=0, keepdims=True)


def heads_to_lanes(ref, group, reps, dim, lanes):
    return jnp.concatenate([ref[(group * reps + r) * dim:(group * reps + r + 1) * dim, lanes] for r in range(reps)], axis=1)


def attn_fwd_kernel(kv_heads, reps, dim, x_a, x_b, n1, n2, wq_h, wk_h, wv_h, wo_h,
                    h_a, u_a, h_b, nb, qkv_b, ctx_b,
                    wq, wk, wv, wo, nrm, q_t, k_t, v_t, ctx, sems):
    copies = [pltpu.make_async_copy(s, d, sems.at[i]) for i, (s, d) in enumerate(((wk_h, wk), (wv_h, wv), (wq_h, wq), (wo_h, wo)))]
    for c in copies:
        c.start()
    tokens = x_a.shape[0]
    heads = kv_heads * reps
    gain1 = row_of(n1)
    nrm[0:tokens] = rms_rows(x_a[...], gain1)
    normed_b = rms_rows(x_b[...], gain1)
    nrm[tokens:2 * tokens] = normed_b
    nb[...] = normed_b
    copies[0].wait()
    k_t[...] = nt(wk[...], nrm[...]).astype(BF)
    copies[1].wait()
    v_t[...] = nt(wv[...], nrm[...]).astype(BF)
    copies[2].wait()
    step = heads * dim // 4
    for i in range(4):
        q_t[i * step:(i + 1) * step] = nt(wq[i * step:(i + 1) * step], nrm[...]).astype(BF)
    for b in range(2):
        lanes = slice(b * tokens, (b + 1) * tokens)
        for g in range(kv_heads):
            kg = k_t[g * dim:(g + 1) * dim, lanes]
            vg = v_t[g * dim:(g + 1) * dim, lanes]
            qg = heads_to_lanes(q_t, g, reps, dim, lanes)
            probs = probs_of(tn(kg, qg) * dim ** -0.5).astype(BF)
            out = nn(vg, probs).astype(BF)
            for r in range(reps):
                ctx[(g * reps + r) * dim:(g * reps + r + 1) * dim, lanes] = out[:, r * tokens:(r + 1) * tokens]
    second = slice(tokens, 2 * tokens)
    qkv_b[0:heads * dim] = q_t[:, second]
    qkv_b[heads * dim:(heads + kv_heads) * dim] = k_t[:, second]
    qkv_b[(heads + kv_heads) * dim:] = v_t[:, second]
    ctx_b[...] = ctx[:, second]
    copies[3].wait()
    attn = tn(ctx[...], wo[...]).astype(BF).astype(F32)
    ha = (x_a[...].astype(F32) + attn[0:tokens]).astype(BF)
    h_a[...] = ha
    h_b[...] = (x_b[...].astype(F32) + attn[tokens:2 * tokens]).astype(BF)
    u_a[...] = rms_rows(ha, row_of(n2))


def attn_fwd(x_a, x_b, n1, n2, wq, wk, wv, wo, kv_heads, reps, dim):
    tokens, model = x_a.shape
    q_dim, kv_dim = kv_heads * reps * dim, kv_heads * dim
    vm = pl.BlockSpec(memory_space=pltpu.VMEM)
    hb = pl.BlockSpec(memory_space=pl.ANY)
    row = jax.ShapeDtypeStruct((tokens, model), BF)
    return pl.pallas_call(
        functools.partial(attn_fwd_kernel, kv_heads, reps, dim),
        out_shape=(row, row, row, row, jax.ShapeDtypeStruct((q_dim + 2 * kv_dim, tokens), BF), jax.ShapeDtypeStruct((q_dim, tokens), BF)),
        in_specs=[vm] * 4 + [hb] * 4,
        out_specs=(vm,) * 6,
        scratch_shapes=[
            pltpu.VMEM((q_dim, model), BF), pltpu.VMEM((kv_dim, model), BF), pltpu.VMEM((kv_dim, model), BF), pltpu.VMEM((q_dim, model), BF),
            pltpu.VMEM((2 * tokens, model), BF), pltpu.VMEM((q_dim, 2 * tokens), BF), pltpu.VMEM((kv_dim, 2 * tokens), BF), pltpu.VMEM((kv_dim, 2 * tokens), BF),
            pltpu.VMEM((q_dim, 2 * tokens), BF), pltpu.SemaphoreType.DMA((4,)),
        ],
        compiler_params=pltpu.CompilerParams(vmem_limit_bytes=60 * MIB),
        cost_estimate=pl.CostEstimate(flops=10 ** 10, bytes_accessed=14 * 10 ** 6, transcendentals=0),
        name="attn_fwd",
    )(x_a, x_b, n1, n2, wq, wk, wv, wo)


def attn_bwd_kernel(kv_heads, reps, dim, s0, s1, t0, dy, h_b, x_b, nb, qkv, ctx, n1, n2, wo_h, wq_h, wk_h, wv_h,
                    dx, gq, gk, gv, go, gn1, gn2,
                    wo, wq, wk, wv, oq, ok, ov, oo, dctx, dq, dk, dv, sems, osems):
    copies = [pltpu.make_async_copy(s, d, sems.at[i]) for i, (s, d) in enumerate(((wo_h, wo), (wq_h, wq), (wk_h, wk), (wv_h, wv)))]
    for c in copies:
        c.start()
    tokens = x_b.shape[0]
    q_dim, kv_dim = kv_heads * reps * dim, kv_heads * dim
    du = ((s0[...] + s1[...]) + t0[...]).astype(BF).astype(F32)
    grad_h, g2 = rms_pull(h_b[...].astype(F32), row_of(n2), du)
    gn2[...] = g2
    dh = (dy[...].astype(F32) + grad_h).astype(BF)
    copies[0].wait()
    outs = []

    def flush(src, dst):
        c = pltpu.make_async_copy(src, dst, osems.at[len(outs)])
        c.start()
        outs.append(c)

    step = q_dim // 4
    for i in range(4):
        dctx[i * step:(i + 1) * step] = nt(wo[i * step:(i + 1) * step], dh).astype(BF)
    for i in range(4):
        part = slice(i * step, (i + 1) * step)
        oo[part] = nn(ctx[part], dh).astype(BF).astype(F32)
        flush(oo.at[part], go.at[part])
    every = slice(0, tokens)
    normed = nb[...]
    for g in range(kv_heads):
        kv = slice(g * dim, (g + 1) * dim)
        kg = qkv[q_dim + g * dim:q_dim + (g + 1) * dim]
        vg = qkv[q_dim + kv_dim + g * dim:q_dim + kv_dim + (g + 1) * dim]
        qg = heads_to_lanes(qkv, g, reps, dim, every)
        dg = heads_to_lanes(dctx, g, reps, dim, every)
        probs = probs_of(tn(kg, qg) * dim ** -0.5)
        dprobs = tn(vg, dg).astype(BF).astype(F32)
        weighted = probs * dprobs
        dscores = ((weighted - probs * jnp.sum(weighted, axis=0, keepdims=True)) * dim ** -0.5).astype(BF)
        dv[kv] = nt(dg, probs.astype(BF)).astype(BF)
        dk[kv] = nt(qg, dscores).astype(BF)
        dqg = nn(kg, dscores).astype(BF)
        for r in range(reps):
            dq[(g * reps + r) * dim:(g * reps + r + 1) * dim] = dqg[:, r * tokens:(r + 1) * tokens]
        if g % 2 == 1:
            part = slice((g - 1) * reps * dim, (g + 1) * reps * dim)
            oq[part] = nn(dq[part], normed).astype(BF).astype(F32)
            flush(oq.at[part], gq.at[part])
    ok[...] = nn(dk[...], normed).astype(BF).astype(F32)
    flush(ok, gk)
    ov[...] = nn(dv[...], normed).astype(BF).astype(F32)
    flush(ov, gv)
    for c in copies[1:]:
        c.wait()
    dn = (tn(dq[...], wq[...]) + tn(dk[...], wk[...]) + tn(dv[...], wv[...])).astype(BF).astype(F32)
    grad_x, g1 = rms_pull(x_b[...].astype(F32), row_of(n1), dn)
    gn1[...] = g1
    dx[...] = (dh.astype(F32) + grad_x).astype(BF)
    for c in outs:
        c.wait()


def attn_bwd(s0, s1, t0, dy, h_b, x_b, nb, qkv, ctx, n1, n2, wo, wq, wk, wv, kv_heads, reps, dim):
    tokens, model = x_b.shape
    q_dim, kv_dim = kv_heads * reps * dim, kv_heads * dim
    vm = pl.BlockSpec(memory_space=pltpu.VMEM)
    hb = pl.BlockSpec(memory_space=pl.ANY)
    n_out = 4 + kv_heads // 2 + 2
    return pl.pallas_call(
        functools.partial(attn_bwd_kernel, kv_heads, reps, dim),
        out_shape=(
            jax.ShapeDtypeStruct((tokens, model), BF), jax.ShapeDtypeStruct((q_dim, model), F32), jax.ShapeDtypeStruct((kv_dim, model), F32),
            jax.ShapeDtypeStruct((kv_dim, model), F32), jax.ShapeDtypeStruct((q_dim, model), F32), jax.ShapeDtypeStruct((1, model), F32), jax.ShapeDtypeStruct((1, model), F32),
        ),
        in_specs=[vm] * 11 + [hb] * 4,
        out_specs=(vm, hb, hb, hb, hb, vm, vm),
        scratch_shapes=[
            pltpu.VMEM((q_dim, model), BF), pltpu.VMEM((q_dim, model), BF), pltpu.VMEM((kv_dim, model), BF), pltpu.VMEM((kv_dim, model), BF),
            pltpu.VMEM((q_dim, model), F32), pltpu.VMEM((kv_dim, model), F32), pltpu.VMEM((kv_dim, model), F32), pltpu.VMEM((q_dim, model), F32),
            pltpu.VMEM((q_dim, tokens), BF), pltpu.VMEM((q_dim, tokens), BF), pltpu.VMEM((kv_dim, tokens), BF), pltpu.VMEM((kv_dim, tokens), BF),
            pltpu.SemaphoreType.DMA((4,)), pltpu.SemaphoreType.DMA((n_out,)),
        ],
        compiler_params=pltpu.CompilerParams(vmem_limit_bytes=60 * MIB),
        cost_estimate=pl.CostEstimate(flops=14 * 10 ** 9, bytes_accessed=40 * 10 ** 6, transcendentals=0),
        name="attn_bwd",
    )(s0, s1, t0, dy, h_b, x_b, nb, qkv, ctx, n1, n2, wo, wq, wk, wv)


def route_rows(infos, base, expert):
    wide = [ref[...].astype(F32) for ref in infos]
    top_k = wide[0].shape[0] // 6
    tokens = wide[0].shape[1]

    def field(i):
        return jnp.concatenate([w[(base + i) * top_k:(base + i + 1) * top_k] for w in wide], axis=1)

    eid, slot, gate = field(0), field(1), field(2)
    hit = (eid == expert.astype(F32)) & (slot >= 0.0)
    slot_row = jnp.sum(jnp.where(hit, slot + 1.0, 0.0), axis=0, keepdims=True) - 1.0
    gate_row = jnp.sum(jnp.where(hit, gate, 0.0), axis=0, keepdims=True)
    kept = jnp.where(slot_row >= 0.0, 1.0, 0.0)
    start = jnp.zeros((1, 1), F32)
    starts = []
    for r in range(len(infos)):
        starts.append(jnp.broadcast_to(start, (1, tokens)))
        start = start + jnp.sum(kept[:, r * tokens:(r + 1) * tokens], axis=1, keepdims=True)
    place_row = jnp.where(slot_row >= 0.0, slot_row + jnp.concatenate(starts, axis=1), -1.0).astype(jnp.int32)
    return slot_row, gate_row, place_row, jnp.sum(kept)


def columns_of(slot_row, me, tokens, capacity):
    device = jnp.bitwise_xor(lax.broadcasted_iota(jnp.int32, slot_row.shape, 1) // tokens, me)
    return slot_row + (device * capacity).astype(F32)


def hits(place_row, first):
    return lax.broadcasted_iota(jnp.int32, (CHUNK, place_row.shape[1]), 0) + first == place_row


def squeeze_rows(hot, col_row, u):
    col = jnp.sum(jnp.where(hot, col_row + 1.0, 0.0), axis=1, keepdims=True) - 1.0
    lane = lax.broadcasted_iota(jnp.int32, (CHUNK, u.shape[0]), 1)
    return nn(jnp.where(lane == col.astype(jnp.int32), 1.0, 0.0).astype(BF), u[...]).astype(BF)


def ring_copies(pairs, sem, idx, ring):
    s = lax.rem(idx, ring)
    return [pltpu.make_async_copy(src.at[idx], dst.at[s], sem.at[s, i]) for i, (src, dst) in enumerate(pairs)]


def row_copies(refs, rows, sem):
    tokens = rows.shape[0] // len(refs)
    return [pltpu.make_async_copy(ref, rows.at[r * tokens:(r + 1) * tokens], sem.at[r]) for r, ref in enumerate(refs)]


def part_copies(acc, refs, sem):
    tokens = acc.shape[0] // len(refs)
    return [pltpu.make_async_copy(acc.at[r * tokens:(r + 1) * tokens], ref, sem.at[r]) for r, ref in enumerate(refs)]


def start_all(copies):
    for c in copies:
        c.start()


def wait_all(copies):
    for c in copies:
        c.wait()


def mix_into(acc, pick, outs):
    for n in range(acc.shape[1] // 256):
        part = slice(n * 256, (n + 1) * 256)
        acc[:, part] += nn(pick, outs[:, part])


def expert_data_kernel(capacity, d0, d1, d2, d3, i0, i1, i2, i3, u_h, w1_h, w2_h, w3_h,
                       acts, p0, p1, p2, p3,
                       rows, us, w1s, w2s, w3s, pick, du_two, act, act_b, late_t, acc, rsem, wsem, asem, lsem, psem):
    e = pl.program_id(0)
    count = pl.num_programs(0)
    me = lax.axis_index('expert')
    tokens = rows.shape[0] // 4
    ring = us.shape[0]
    ff = w1s.shape[2]
    model = rows.shape[1]
    slot_e = lax.rem(e, 2)
    arrivals = row_copies((d0, d1, d2, d3), rows, rsem)
    pairs = ((u_h, us), (w1_h, w1s), (w3_h, w3s), (w2_h, w2s))

    @pl.when(e == 0)
    def _():
        start_all(arrivals + ring_copies(pairs, wsem, 0, ring) + ring_copies(pairs, wsem, 1, ring))
        acc[...] = jnp.zeros_like(acc)
        wait_all(arrivals)

    @pl.when(e + 2 < count)
    def _():
        start_all(ring_copies(pairs, wsem, e + 2, ring))

    slot_row, gate_row, place_row, filled = route_rows((i0, i1, i2, i3), 3, me * count + e)
    col_row = columns_of(slot_row, me, tokens, capacity)

    def save(idx):
        s = lax.rem(idx, 2)
        return pltpu.make_async_copy(act.at[s], acts.at[idx, 0:CHUNK], asem.at[s])

    @pl.when(e >= 2)
    def _():
        save(e - 2).wait()

    wait_all(ring_copies(pairs, wsem, e, ring))
    now = lax.rem(e, ring)
    u, w1, w2, w3 = us.at[now], w1s.at[now], w2s.at[now], w3s.at[now]

    def run(first, keep):
        hot = hits(place_row, first)
        d_out = nn(jnp.where(hot, gate_row, 0.0).astype(BF), rows[...]).astype(BF)
        u_c = squeeze_rows(hot, col_row, u)
        for n in range(ff // 256):
            part = slice(n * 256, (n + 1) * 256)
            pre1 = nn(u_c, w1[:, part]).astype(BF).astype(F32)
            pre3 = nn(u_c, w3[:, part]).astype(BF).astype(F32)
            grad_hid = nt(d_out, w2[part, :]).astype(BF).astype(F32)
            sigma = jax.nn.sigmoid(pre1)
            silu = pre1 * sigma
            keep[:, n * 256:(n + 1) * 256] = (silu * pre3).astype(BF)
            keep[:, ff + n * 256:ff + (n + 1) * 256] = (grad_hid * pre3 * sigma * (1.0 + pre1 * (1.0 - sigma))).astype(BF)
            keep[:, 2 * ff + n * 256:2 * ff + (n + 1) * 256] = (grad_hid * silu).astype(BF)
        du = [(nt(keep[:, ff:2 * ff], w1[n * 256:(n + 1) * 256]) + nt(keep[:, 2 * ff:3 * ff], w3[n * 256:(n + 1) * 256])).astype(BF) for n in range(model // 256)]
        return jnp.transpose(jnp.where(hot, 1.0, 0.0).astype(BF)), du

    chosen, du = run(0, act.at[slot_e])
    save(e).start()
    half = pl.ds(pl.multiple_of(slot_e * CHUNK, CHUNK), CHUNK)
    pick[:, half] = chosen
    for n, piece in enumerate(du):
        du_two[half, n * 256:(n + 1) * 256] = piece

    @pl.when(filled > float(CHUNK))
    def _():
        more, du_more = run(CHUNK, act_b)
        c = pltpu.make_async_copy(act_b, acts.at[e, CHUNK:2 * CHUNK], lsem.at[0])
        c.start()
        late_t[...] = more
        for n, piece in enumerate(du_more):
            acc[:, n * 256:(n + 1) * 256] += nn(late_t[...], piece)
        c.wait()

    @pl.when(slot_e == 1)
    def _():
        mix_into(acc, pick[...], du_two)

    @pl.when(e == count - 1)
    def _():
        sends = part_copies(acc, (p0, p1, p2, p3), psem)
        start_all(sends)
        save(e - 1).wait()
        save(e).wait()
        wait_all(sends)


def whole(shape):
    return pl.BlockSpec(shape, lambda e: (0,) * len(shape), pipeline_mode=pl.Buffered(1))


def expert_data(dys, infos, u, w1, w2, w3):
    tokens, model = dys[0].shape
    count, cols, _ = u.shape
    ff = w1.shape[2]
    ring = 3
    hb = pl.BlockSpec(memory_space=pl.ANY)
    part = jax.ShapeDtypeStruct((tokens, model), F32)
    return pl.pallas_call(
        functools.partial(expert_data_kernel, cols // 4),
        grid=(count,),
        out_shape=(jax.ShapeDtypeStruct((count, 2 * CHUNK, 3 * ff), BF), part, part, part, part),
        in_specs=[hb] * 4 + [whole(infos[0].shape)] * 4 + [hb] * 4,
        out_specs=(hb,) * 5,
        scratch_shapes=[
            pltpu.VMEM((4 * tokens, model), BF),
            pltpu.VMEM((ring, cols, model), BF), pltpu.VMEM((ring, model, ff), BF), pltpu.VMEM((ring, ff, model), BF), pltpu.VMEM((ring, model, ff), BF),
            pltpu.VMEM((4 * tokens, 2 * CHUNK), BF), pltpu.VMEM((2 * CHUNK, model), BF),
            pltpu.VMEM((2, CHUNK, 3 * ff), BF), pltpu.VMEM((CHUNK, 3 * ff), BF), pltpu.VMEM((4 * tokens, CHUNK), BF), pltpu.VMEM((4 * tokens, model), F32),
            pltpu.SemaphoreType.DMA((4,)), pltpu.SemaphoreType.DMA((ring, 4)), pltpu.SemaphoreType.DMA((2,)), pltpu.SemaphoreType.DMA((1,)), pltpu.SemaphoreType.DMA((4,)),
        ],
        compiler_params=pltpu.CompilerParams(vmem_limit_bytes=60 * MIB, dimension_semantics=("arbitrary",)),
        cost_estimate=pl.CostEstimate(flops=20 * 10 ** 9, bytes_accessed=70 * 10 ** 6, transcendentals=0),
        name="expert_data",
    )(*dys, *infos, u, w1, w2, w3)


def expert_grad_kernel(capacity, d0, d1, d2, d3, i0, i1, i2, i3, u_h, act_h,
                       g1, g2, g3,
                       rows, us, acts, act_b, d_out, u_c, o1, o2, o3, rsem, wsem, lsem, sems):
    e = pl.program_id(0)
    count = pl.num_programs(0)
    me = lax.axis_index('expert')
    tokens = rows.shape[0] // 4
    ring = us.shape[0]
    model = rows.shape[1]
    ff = o2.shape[1]
    slot_e = lax.rem(e, 2)
    arrivals = row_copies((d0, d1, d2, d3), rows, rsem)

    def fetch(idx):
        s = lax.rem(idx, ring)
        return [pltpu.make_async_copy(u_h.at[idx], us.at[s], wsem.at[s, 0]), pltpu.make_async_copy(act_h.at[idx, 0:CHUNK], acts.at[s], wsem.at[s, 1])]

    def flush(idx):
        s = lax.rem(idx, 2)
        return [pltpu.make_async_copy(src.at[s], dst.at[idx], sems.at[s, i]) for i, (src, dst) in enumerate(((o1, g1), (o2, g2), (o3, g3)))]

    @pl.when(e == 0)
    def _():
        start_all(arrivals + fetch(0) + fetch(1))
        wait_all(arrivals)

    @pl.when(e + 2 < count)
    def _():
        start_all(fetch(e + 2))

    slot_row, gate_row, place_row, filled = route_rows((i0, i1, i2, i3), 3, me * count + e)
    col_row = columns_of(slot_row, me, tokens, capacity)
    wait_all(fetch(e))
    now = lax.rem(e, ring)

    def rebuild(first):
        hot = hits(place_row, first)
        d_out[...] = nn(jnp.where(hot, gate_row, 0.0).astype(BF), rows[...]).astype(BF)
        u_c[...] = squeeze_rows(hot, col_row, us.at[now])

    rebuild(0)

    @pl.when(e >= 2)
    def _():
        wait_all(flush(e - 2))

    done = flush(e)
    act = acts.at[now]
    for m in range(ff // 256):
        o2[slot_e, m * 256:(m + 1) * 256] = tn(act[:, m * 256:(m + 1) * 256], d_out[...])
    for m in range(model // 256):
        part = slice(m * 256, (m + 1) * 256)
        o1[slot_e, part] = tn(u_c[:, part], act[:, ff:2 * ff])
        o3[slot_e, part] = tn(u_c[:, part], act[:, 2 * ff:3 * ff])

    @pl.when(filled > float(CHUNK))
    def _():
        c = pltpu.make_async_copy(act_h.at[e, CHUNK:2 * CHUNK], act_b, lsem.at[0])
        c.start()
        rebuild(CHUNK)
        c.wait()
        for m in range(ff // 256):
            o2[slot_e, m * 256:(m + 1) * 256] += tn(act_b[:, m * 256:(m + 1) * 256], d_out[...])
        for m in range(model // 256):
            part = slice(m * 256, (m + 1) * 256)
            o1[slot_e, part] += tn(u_c[:, part], act_b[:, ff:2 * ff])
            o3[slot_e, part] += tn(u_c[:, part], act_b[:, 2 * ff:3 * ff])

    start_all(done)

    @pl.when(e == count - 1)
    def _():
        wait_all(flush(e - 1))
        wait_all(flush(e))


def expert_grad(dys, infos, u, acts):
    tokens, model = dys[0].shape
    count, cols, _ = u.shape
    ff = acts.shape[2] // 3
    ring = 3
    hb = pl.BlockSpec(memory_space=pl.ANY)
    return pl.pallas_call(
        functools.partial(expert_grad_kernel, cols // 4),
        grid=(count,),
        out_shape=(jax.ShapeDtypeStruct((count, model, ff), F32), jax.ShapeDtypeStruct((count, ff, model), F32), jax.ShapeDtypeStruct((count, model, ff), F32)),
        in_specs=[hb] * 4 + [whole(infos[0].shape)] * 4 + [hb] * 2,
        out_specs=(hb,) * 3,
        scratch_shapes=[
            pltpu.VMEM((4 * tokens, model), BF), pltpu.VMEM((ring, cols, model), BF), pltpu.VMEM((ring, CHUNK, 3 * ff), BF), pltpu.VMEM((CHUNK, 3 * ff), BF),
            pltpu.VMEM((CHUNK, model), BF), pltpu.VMEM((CHUNK, model), BF),
            pltpu.VMEM((2, model, ff), F32), pltpu.VMEM((2, ff, model), F32), pltpu.VMEM((2, model, ff), F32),
            pltpu.SemaphoreType.DMA((4,)), pltpu.SemaphoreType.DMA((ring, 2)), pltpu.SemaphoreType.DMA((1,)), pltpu.SemaphoreType.DMA((2, 3)),
        ],
        compiler_params=pltpu.CompilerParams(vmem_limit_bytes=60 * MIB, dimension_semantics=("arbitrary",)),
        cost_estimate=pl.CostEstimate(flops=35 * 10 ** 9, bytes_accessed=110 * 10 ** 6, transcendentals=0),
        name="expert_grad",
    )(*dys, *infos, u, acts)


def expert_fwd_kernel(u0, u1, u2, u3, i0, i1, i2, i3, w1_h, w2_h, w3_h, p0, p1, p2, p3,
                      rows, w1s, w2s, w3s, pick, out_two, acc, late_t, rsem, wsem, psem):
    e = pl.program_id(0)
    count = pl.num_programs(0)
    me = lax.axis_index('expert')
    ring, _, ff = w1s.shape
    slot_e = lax.rem(e, 2)
    arrivals = row_copies((u0, u1, u2, u3), rows, rsem)
    pairs = ((w1_h, w1s), (w3_h, w3s), (w2_h, w2s))

    @pl.when(e == 0)
    def _():
        start_all(arrivals + ring_copies(pairs, wsem, 0, ring) + ring_copies(pairs, wsem, 1, ring))
        acc[...] = jnp.zeros_like(acc)
        wait_all(arrivals)

    @pl.when(e + 2 < count)
    def _():
        start_all(ring_copies(pairs, wsem, e + 2, ring))

    _, gate_row, place_row, filled = route_rows((i0, i1, i2, i3), 0, me * count + e)
    wait_all(ring_copies(pairs, wsem, e, ring))
    now = lax.rem(e, ring)
    w1, w2, w3 = w1s.at[now], w2s.at[now], w3s.at[now]

    def run(first):
        hot = hits(place_row, first)
        v = nn(jnp.where(hot, 1.0, 0.0).astype(BF), rows[...]).astype(BF)
        pieces = []
        for n in range(ff // 256):
            part = slice(n * 256, (n + 1) * 256)
            a1 = nn(v, w1[:, part]).astype(BF).astype(F32)
            a3 = nn(v, w3[:, part]).astype(BF).astype(F32)
            pieces.append((a1 * jax.nn.sigmoid(a1) * a3).astype(BF))
        hidden = jnp.concatenate(pieces, axis=1)
        return jnp.transpose(jnp.where(hot, gate_row, 0.0).astype(BF)), nn(hidden, w2[...]).astype(BF)

    chosen, out = run(0)
    half = pl.ds(pl.multiple_of(slot_e * CHUNK, CHUNK), CHUNK)
    pick[:, half] = chosen
    out_two[half, :] = out

    @pl.when(filled > float(CHUNK))
    def _():
        more, out_more = run(CHUNK)
        late_t[...] = more
        mix_into(acc, late_t[...], out_more)

    @pl.when(slot_e == 1)
    def _():
        mix_into(acc, pick[...], out_two)

    @pl.when(e == count - 1)
    def _():
        sends = part_copies(acc, (p0, p1, p2, p3), psem)
        start_all(sends)
        wait_all(sends)


def expert_fwd(us, infos, w1, w2, w3):
    tokens, model = us[0].shape
    count, _, ff = w1.shape
    ring = 3
    part = jax.ShapeDtypeStruct((tokens, model), F32)
    hb = pl.BlockSpec(memory_space=pl.ANY)
    return pl.pallas_call(
        expert_fwd_kernel,
        grid=(count,),
        out_shape=(part, part, part, part),
        in_specs=[hb] * 4 + [whole(infos[0].shape)] * 4 + [hb] * 3,
        out_specs=(hb,) * 4,
        scratch_shapes=[
            pltpu.VMEM((4 * tokens, model), BF),
            pltpu.VMEM((ring, model, ff), BF), pltpu.VMEM((ring, ff, model), BF), pltpu.VMEM((ring, model, ff), BF),
            pltpu.VMEM((4 * tokens, 2 * CHUNK), BF), pltpu.VMEM((2 * CHUNK, model), BF),
            pltpu.VMEM((4 * tokens, model), F32), pltpu.VMEM((4 * tokens, CHUNK), BF),
            pltpu.SemaphoreType.DMA((4,)), pltpu.SemaphoreType.DMA((ring, 3)), pltpu.SemaphoreType.DMA((4,)),
        ],
        compiler_params=pltpu.CompilerParams(vmem_limit_bytes=60 * MIB, dimension_semantics=("arbitrary",)),
        cost_estimate=pl.CostEstimate(flops=16 * 10 ** 9, bytes_accessed=50 * 10 ** 6, transcendentals=0),
        name="expert_fwd",
    )(*us, *infos, w1, w2, w3)


def pack_kernel(*refs):
    refs[-1][...] = jnp.concatenate([r[...].astype(F32) for r in refs[:-1]], axis=0).astype(BF)


def pack(fields):
    vm = pl.BlockSpec(memory_space=pltpu.VMEM)
    rows = sum(f.shape[0] for f in fields)
    return pl.pallas_call(
        pack_kernel,
        out_shape=jax.ShapeDtypeStruct((rows, fields[0].shape[1]), BF),
        in_specs=[vm] * len(fields), out_specs=vm,
        compiler_params=pltpu.CompilerParams(vmem_limit_bytes=60 * MIB),
        name="pack",
    )(*fields)


def solution(mesh):
    group = mesh.shape['expert']

    def hop(value, bits):
        return lax.ppermute(value, 'expert', [(i, i ^ bits) for i in range(group)])

    def local_step(x_a, x_b, dy_b, eid_a, slot_a, gate_a, eid_b, slot_b, gate_b, u_b, norm_1, norm_2, w_q, w_k, w_v, w_o, w_1, w_2, w_3):
        model, heads, dim = w_q.shape
        kv_heads = w_k.shape[1]
        reps = heads // kv_heads
        info = pack([a.T for a in (eid_a, slot_a, gate_a, eid_b, slot_b, gate_b)])
        dy2 = hop(dy_b, 2)
        dy1 = hop(dy_b, 1)
        infos = (info, hop(info, 1), hop(info, 2), hop(info, 3))
        wq_t, wk_t, wv_t = (w.transpose(1, 2, 0).reshape(-1, model) for w in (w_q, w_k, w_v))
        wo = w_o.reshape(-1, model)
        h_a, u_a, h_b, nb, qkv_b, ctx_b = attn_fwd(x_a, x_b, norm_1, norm_2, wq_t, wk_t, wv_t, wo, kv_heads, reps, dim)
        dy3 = hop(dy2, 1)
        us = (u_a, hop(u_a, 1), hop(u_a, 2), hop(u_a, 3))
        dys = (dy_b, dy1, dy2, dy3)
        acts, b0, b1, b2, b3 = expert_data(dys, infos, u_b, w_1, w_2, w_3)
        swap_b = hop(b3, 1)
        near_b = hop(b1, 1)
        a0, a1, a2, a3 = expert_fwd(us, infos, w_1, w_2, w_3)
        far_b = hop(b2 + swap_b, 2)
        far_a = hop(a2 + hop(a3, 1), 2)
        near_a = hop(a1, 1)
        g1, g2, g3 = expert_grad(dys, infos, u_b, acts)
        dx_b, g_q, g_k, g_v, g_o, g_n1, g_n2 = attn_bwd(b0, near_b, far_b, dy_b, h_b, x_b, nb, qkv_b, ctx_b, norm_1, norm_2, wo, wq_t, wk_t, wv_t, kv_heads, reps, dim)
        y_a = (h_a.astype(F32) + ((a0 + near_a) + far_a)).astype(BF)
        g_q = g_q.reshape(heads, dim, model).transpose(2, 0, 1)
        g_k = g_k.reshape(kv_heads, dim, model).transpose(2, 0, 1)
        g_v = g_v.reshape(kv_heads, dim, model).transpose(2, 0, 1)
        g_o = g_o.reshape(heads, dim, model)
        return (y_a, dx_b, g1, g2, g3, g_q[None], g_k[None], g_v[None], g_o[None], g_n1, g_n2)

    row_spec = P(('data', 'expert'), None)
    cube_spec = P(('data', 'expert'), None, None)
    quad_spec = P(('data', 'expert'), None, None, None)
    expert_spec = P('expert', None, None)
    in_specs = (row_spec, row_spec, row_spec, row_spec, row_spec, row_spec, row_spec, row_spec, row_spec, cube_spec, P(), P(), P(), P(), P(), P(), expert_spec, expert_spec, expert_spec)
    out_specs = (row_spec, row_spec, cube_spec, cube_spec, cube_spec, quad_spec, quad_spec, quad_spec, quad_spec, row_spec, row_spec)
    return jax.shard_map(local_step, mesh=mesh, in_specs=in_specs, out_specs=out_specs, check_vma=False)
```

```python
import functools

import jax
import jax.numpy as jnp
from jax import lax
from jax.experimental import pallas as pl
from jax.experimental.pallas import tpu as pltpu
from jax.sharding import PartitionSpec as P


NORM_EPS = 1e-6
BF = jnp.bfloat16
F32 = jnp.float32
MIB = 1024 * 1024
CHUNK = 128


def nn(a, b):
    return lax.dot_general(a, b, (((1,), (0,)), ((), ())), preferred_element_type=F32)


def nt(a, b):
    return lax.dot_general(a, b, (((1,), (1,)), ((), ())), preferred_element_type=F32)


def tn(a, b):
    return lax.dot_general(a, b, (((0,), (0,)), ((), ())), preferred_element_type=F32)


def row_of(ref):
    return ref[...].astype(F32).reshape(1, ref.shape[0])


def rms_scale(wide):
    return lax.rsqrt(jnp.mean(wide * wide, axis=-1, keepdims=True) + NORM_EPS)


def rms_rows(values, gain):
    wide = values.astype(F32)
    return (wide * rms_scale(wide) * gain).astype(BF)


def rms_pull(wide, gain, cot):
    scale = rms_scale(wide)
    scaled = wide * scale
    grad_gain = jnp.sum(cot * scaled, axis=0, keepdims=True).astype(BF).astype(F32)
    inner = cot * gain
    pull = jnp.mean(inner * wide, axis=-1, keepdims=True)
    grad = scale * inner - scaled * (scale * scale * pull)
    return grad.astype(BF).astype(F32), grad_gain


def probs_of(scores_t):
    rows = lax.broadcasted_iota(jnp.int32, scores_t.shape, 0)
    cols = lax.broadcasted_iota(jnp.int32, scores_t.shape, 1) % scores_t.shape[0]
    masked = jnp.where(rows <= cols, scores_t, -1e30)
    top = jnp.max(masked, axis=0, keepdims=True)
    unnorm = jnp.exp(masked - top)
    return unnorm / jnp.sum(unnorm, axis=0, keepdims=True)


def heads_to_lanes(ref, group, reps, dim, lanes):
    return jnp.concatenate([ref[(group * reps + r) * dim:(group * reps + r + 1) * dim, lanes] for r in range(reps)], axis=1)


def attn_fwd_kernel(kv_heads, reps, dim, xa_h, xb_h, n1, n2, wq_h, wk_h, wv_h, wo_h,
                    ha_h, ua_h, hb_h, nb_h, qkv_h, ctx_h,
                    xs, wq, wk, wv, wo, nrm, nrm_t, q_t, k_t, v_t, ctx, q_b, ctx_b, hs, ua, sems, osems):
    tokens = xs.shape[0] // 2
    heads = kv_heads * reps
    first, second = slice(0, tokens), slice(tokens, 2 * tokens)
    half = heads * dim // 2
    moves = ((xa_h, xs.at[first]), (xb_h, xs.at[second]), (wk_h, wk), (wv_h, wv), (wq_h.at[0:half], wq.at[0:half]), (wq_h.at[half:], wq.at[half:]), (wo_h, wo))
    copies = [pltpu.make_async_copy(s, d, sems.at[i]) for i, (s, d) in enumerate(moves)]
    start_all(copies)
    outs = []

    def flush(src, dst):
        c = pltpu.make_async_copy(src, dst, osems.at[len(outs)])
        c.start()
        outs.append(c)

    wait_all(copies[0:2])
    nrm[...] = rms_rows(xs[...], row_of(n1))
    nrm_t[...] = jnp.transpose(nrm[...])
    flush(nrm.at[second], nb_h)
    copies[2].wait()
    k_t[...] = nn(wk[...], nrm_t[...]).astype(BF)
    copies[3].wait()
    v_t[...] = nn(wv[...], nrm_t[...]).astype(BF)
    for i in range(2):
        copies[4 + i].wait()
        part = slice(i * half, (i + 1) * half)
        q_t[part] = nn(wq[part], nrm_t[...]).astype(BF)
    q_b[0:heads * dim] = q_t[:, second]
    q_b[heads * dim:(heads + kv_heads) * dim] = k_t[:, second]
    q_b[(heads + kv_heads) * dim:] = v_t[:, second]
    flush(q_b, qkv_h)
    for lanes in (second, first):
        for g in range(kv_heads):
            kg = k_t[g * dim:(g + 1) * dim, lanes]
            vg = v_t[g * dim:(g + 1) * dim, lanes]
            qg = heads_to_lanes(q_t, g, reps, dim, lanes)
            probs = probs_of(tn(kg, qg) * dim ** -0.5).astype(BF)
            out = nn(vg, probs).astype(BF)
            for r in range(reps):
                ctx[(g * reps + r) * dim:(g * reps + r + 1) * dim, lanes] = out[:, r * tokens:(r + 1) * tokens]
    ctx_b[...] = ctx[:, second]
    flush(ctx_b, ctx_h)
    copies[6].wait()
    hs[...] = (xs[...].astype(F32) + tn(ctx[...], wo[...]).astype(BF).astype(F32)).astype(BF)
    flush(hs.at[first], ha_h)
    flush(hs.at[second], hb_h)
    ua[...] = rms_rows(hs[first], row_of(n2))
    flush(ua, ua_h)
    wait_all(outs)


def attn_fwd(x_a, x_b, n1, n2, wq, wk, wv, wo, kv_heads, reps, dim):
    tokens, model = x_a.shape
    q_dim, kv_dim = kv_heads * reps * dim, kv_heads * dim
    vm = pl.BlockSpec(memory_space=pltpu.VMEM)
    hb = pl.BlockSpec(memory_space=pl.ANY)
    row = jax.ShapeDtypeStruct((tokens, model), BF)
    return pl.pallas_call(
        functools.partial(attn_fwd_kernel, kv_heads, reps, dim),
        out_shape=(row, row, row, row, jax.ShapeDtypeStruct((q_dim + 2 * kv_dim, tokens), BF), jax.ShapeDtypeStruct((q_dim, tokens), BF)),
        in_specs=[hb] * 2 + [vm] * 2 + [hb] * 4,
        out_specs=(hb,) * 6,
        scratch_shapes=[
            pltpu.VMEM((2 * tokens, model), BF),
            pltpu.VMEM((q_dim, model), BF), pltpu.VMEM((kv_dim, model), BF), pltpu.VMEM((kv_dim, model), BF), pltpu.VMEM((q_dim, model), BF),
            pltpu.VMEM((2 * tokens, model), BF), pltpu.VMEM((model, 2 * tokens), BF),
            pltpu.VMEM((q_dim, 2 * tokens), BF), pltpu.VMEM((kv_dim, 2 * tokens), BF), pltpu.VMEM((kv_dim, 2 * tokens), BF), pltpu.VMEM((q_dim, 2 * tokens), BF),
            pltpu.VMEM((q_dim + 2 * kv_dim, tokens), BF), pltpu.VMEM((q_dim, tokens), BF), pltpu.VMEM((2 * tokens, model), BF), pltpu.VMEM((tokens, model), BF),
            pltpu.SemaphoreType.DMA((7,)), pltpu.SemaphoreType.DMA((6,)),
        ],
        compiler_params=pltpu.CompilerParams(vmem_limit_bytes=60 * MIB),
        cost_estimate=pl.CostEstimate(flops=10 ** 10, bytes_accessed=14 * 10 ** 6, transcendentals=0),
        name="attn_fwd",
    )(x_a, x_b, n1, n2, wq, wk, wv, wo)


def attn_bwd_kernel(kv_heads, reps, dim, s0, s1, t0, dy, h_b, x_b, nb, qkv, ctx, n1, n2, wo_h, wq_h, wk_h, wv_h,
                    dx, gq, gk, gv, go, gn1, gn2,
                    wo, wq, wk, wv, oq, ok, ov, oo, dctx, dq, dk, dv, sems, osems):
    copies = [pltpu.make_async_copy(s, d, sems.at[i]) for i, (s, d) in enumerate(((wo_h, wo), (wq_h, wq), (wk_h, wk), (wv_h, wv)))]
    for c in copies:
        c.start()
    tokens = x_b.shape[0]
    q_dim, kv_dim = kv_heads * reps * dim, kv_heads * dim
    du = ((s0[...] + s1[...]) + t0[...]).astype(BF).astype(F32)
    grad_h, g2 = rms_pull(h_b[...].astype(F32), row_of(n2), du)
    gn2[...] = g2
    dh = (dy[...].astype(F32) + grad_h).astype(BF)
    copies[0].wait()
    outs = []

    def flush(src, dst):
        c = pltpu.make_async_copy(src, dst, osems.at[len(outs)])
        c.start()
        outs.append(c)

    step = q_dim // 4
    for i in range(4):
        dctx[i * step:(i + 1) * step] = nt(wo[i * step:(i + 1) * step], dh).astype(BF)
    for i in range(4):
        part = slice(i * step, (i + 1) * step)
        oo[part] = nn(ctx[part], dh).astype(BF).astype(F32)
        flush(oo.at[part], go.at[part])
    every = slice(0, tokens)
    normed = nb[...]
    for g in range(kv_heads):
        kv = slice(g * dim, (g + 1) * dim)
        kg = qkv[q_dim + g * dim:q_dim + (g + 1) * dim]
        vg = qkv[q_dim + kv_dim + g * dim:q_dim + kv_dim + (g + 1) * dim]
        qg = heads_to_lanes(qkv, g, reps, dim, every)
        dg = heads_to_lanes(dctx, g, reps, dim, every)
        probs = probs_of(tn(kg, qg) * dim ** -0.5)
        dprobs = tn(vg, dg).astype(BF).astype(F32)
        weighted = probs * dprobs
        dscores = ((weighted - probs * jnp.sum(weighted, axis=0, keepdims=True)) * dim ** -0.5).astype(BF)
        dv[kv] = nt(dg, probs.astype(BF)).astype(BF)
        dk[kv] = nt(qg, dscores).astype(BF)
        dqg = nn(kg, dscores).astype(BF)
        for r in range(reps):
            dq[(g * reps + r) * dim:(g * reps + r + 1) * dim] = dqg[:, r * tokens:(r + 1) * tokens]
        if g % 2 == 1:
            part = slice((g - 1) * reps * dim, (g + 1) * reps * dim)
            oq[part] = nn(dq[part], normed).astype(BF).astype(F32)
            flush(oq.at[part], gq.at[part])
    ok[...] = nn(dk[...], normed).astype(BF).astype(F32)
    flush(ok, gk)
    ov[...] = nn(dv[...], normed).astype(BF).astype(F32)
    flush(ov, gv)
    for c in copies[1:]:
        c.wait()
    dn = (tn(dq[...], wq[...]) + tn(dk[...], wk[...]) + tn(dv[...], wv[...])).astype(BF).astype(F32)
    grad_x, g1 = rms_pull(x_b[...].astype(F32), row_of(n1), dn)
    gn1[...] = g1
    dx[...] = (dh.astype(F32) + grad_x).astype(BF)
    for c in outs:
        c.wait()


def attn_bwd(s0, s1, t0, dy, h_b, x_b, nb, qkv, ctx, n1, n2, wo, wq, wk, wv, kv_heads, reps, dim):
    tokens, model = x_b.shape
    q_dim, kv_dim = kv_heads * reps * dim, kv_heads * dim
    vm = pl.BlockSpec(memory_space=pltpu.VMEM)
    hb = pl.BlockSpec(memory_space=pl.ANY)
    n_out = 4 + kv_heads // 2 + 2
    return pl.pallas_call(
        functools.partial(attn_bwd_kernel, kv_heads, reps, dim),
        out_shape=(
            jax.ShapeDtypeStruct((tokens, model), BF), jax.ShapeDtypeStruct((q_dim, model), F32), jax.ShapeDtypeStruct((kv_dim, model), F32),
            jax.ShapeDtypeStruct((kv_dim, model), F32), jax.ShapeDtypeStruct((q_dim, model), F32), jax.ShapeDtypeStruct((1, model), F32), jax.ShapeDtypeStruct((1, model), F32),
        ),
        in_specs=[vm] * 11 + [hb] * 4,
        out_specs=(vm, hb, hb, hb, hb, vm, vm),
        scratch_shapes=[
            pltpu.VMEM((q_dim, model), BF), pltpu.VMEM((q_dim, model), BF), pltpu.VMEM((kv_dim, model), BF), pltpu.VMEM((kv_dim, model), BF),
            pltpu.VMEM((q_dim, model), F32), pltpu.VMEM((kv_dim, model), F32), pltpu.VMEM((kv_dim, model), F32), pltpu.VMEM((q_dim, model), F32),
            pltpu.VMEM((q_dim, tokens), BF), pltpu.VMEM((q_dim, tokens), BF), pltpu.VMEM((kv_dim, tokens), BF), pltpu.VMEM((kv_dim, tokens), BF),
            pltpu.SemaphoreType.DMA((4,)), pltpu.SemaphoreType.DMA((n_out,)),
        ],
        compiler_params=pltpu.CompilerParams(vmem_limit_bytes=60 * MIB),
        cost_estimate=pl.CostEstimate(flops=14 * 10 ** 9, bytes_accessed=40 * 10 ** 6, transcendentals=0),
        name="attn_bwd",
    )(s0, s1, t0, dy, h_b, x_b, nb, qkv, ctx, n1, n2, wo, wq, wk, wv)


def route_rows(info, base, expert):
    group, _, width = info.shape
    tokens = width // 3
    top_k = info.shape[1] // 2
    wide = [info[r].astype(F32)[base * top_k:(base + 1) * top_k] for r in range(group)]

    def field(i):
        return jnp.concatenate([w[:, i * tokens:(i + 1) * tokens] for w in wide], axis=1)

    eid, slot, gate = field(0), field(1), field(2)
    hit = (eid == expert.astype(F32)) & (slot >= 0.0)
    slot_row = jnp.sum(jnp.where(hit, slot + 1.0, 0.0), axis=0, keepdims=True) - 1.0
    gate_row = jnp.sum(jnp.where(hit, gate, 0.0), axis=0, keepdims=True)
    return slot_row, gate_row


def places(slot_row, group):
    tokens = slot_row.shape[1] // group
    kept = jnp.where(slot_row >= 0.0, 1.0, 0.0)
    start = jnp.zeros((1, 1), F32)
    starts = []
    for r in range(group):
        starts.append(jnp.broadcast_to(start, (1, tokens)))
        start = start + jnp.sum(kept[:, r * tokens:(r + 1) * tokens], axis=1, keepdims=True)
    place_row = jnp.where(slot_row >= 0.0, slot_row + jnp.concatenate(starts, axis=1), -1.0).astype(jnp.int32)
    return place_row, jnp.sum(kept)


def hits(place_row, first):
    return lax.broadcasted_iota(jnp.int32, (CHUNK, place_row.shape[1]), 0) + first == place_row


def ring_copies(pairs, sem, idx, ring):
    s = lax.rem(idx, ring)
    return [pltpu.make_async_copy(src.at[idx], dst.at[s], sem.at[s, i]) for i, (src, dst) in enumerate(pairs)]


def row_copies(refs, rows, sem):
    tokens = rows.shape[0] // len(refs)
    return [pltpu.make_async_copy(ref.at[0:tokens], rows.at[r * tokens:(r + 1) * tokens], sem.at[r]) for r, ref in enumerate(refs)]


def info_copies(refs, info, sem):
    _, depth, width = info.shape
    first = refs[0].shape[0] - depth
    return [pltpu.make_async_copy(ref.at[first:first + depth, 0:width], info.at[r], sem.at[len(refs) + r]) for r, ref in enumerate(refs)]


def part_copies(acc, refs, sem):
    tokens = acc.shape[0] // len(refs)
    return [pltpu.make_async_copy(acc.at[r * tokens:(r + 1) * tokens], ref, sem.at[r]) for r, ref in enumerate(refs)]


def start_all(copies):
    for c in copies:
        c.start()


def wait_all(copies):
    for c in copies:
        c.wait()


def mix_into(acc, pick, outs):
    for n in range(acc.shape[1] // 256):
        part = slice(n * 256, (n + 1) * 256)
        acc[:, part] += nn(pick, outs[:, part])


def expert_bwd_kernel(capacity, d0, d1, d2, d3, u_h, w1_h, w2_h, w3_h,
                      g1, g2, g3, p0, p1, p2, p3,
                      rows, info, us, w1s, w2s, w3s, pick, du_two, d_out, hid, da1, da3, o1, o2, o3, acc, rsem, wsem, sems, psem):
    e = pl.program_id(0)
    count = pl.num_programs(0)
    me = lax.axis_index('expert')
    slot_e = lax.rem(e, 2)
    ring, cols, model = us.shape
    tokens = rows.shape[0] // 4
    ff = w1s.shape[2]
    padded = du_two.shape[0] // 2
    heads = (d0, d1, d2, d3)
    arrivals = info_copies(heads, info, rsem) + row_copies(heads, rows, rsem)
    pairs = ((u_h, us), (w1_h, w1s), (w3_h, w3s), (w2_h, w2s))

    @pl.when(e == 0)
    def _():
        start_all(arrivals + ring_copies(pairs, wsem, 0, ring) + ring_copies(pairs, wsem, 1, ring))
        acc[...] = jnp.zeros_like(acc)
        du_two[...] = jnp.zeros_like(du_two)
        wait_all(arrivals)

    @pl.when(e + 2 < count)
    def _():
        start_all(ring_copies(pairs, wsem, e + 2, ring))

    slot_row, gate_row = route_rows(info, 1, me * count + e)
    device = jnp.bitwise_xor(lax.broadcasted_iota(jnp.int32, slot_row.shape, 1) // tokens, me)
    col_row = jnp.where(slot_row >= 0.0, slot_row.astype(jnp.int32) + device * capacity, -1)
    hot = lax.broadcasted_iota(jnp.int32, (padded, 4 * tokens), 0) == col_row
    pick[:, pl.ds(pl.multiple_of(slot_e * padded, padded), padded)] = jnp.transpose(jnp.where(hot, 1.0, 0.0).astype(BF))
    d_out[...] = nn(jnp.where(hot, gate_row, 0.0).astype(BF)[0:cols], rows[...]).astype(BF)

    def flush(idx):
        s = lax.rem(idx, 2)
        return [pltpu.make_async_copy(src.at[s], dst.at[idx], sems.at[s, i]) for i, (src, dst) in enumerate(((o1, g1), (o2, g2), (o3, g3)))]

    wait_all(ring_copies(pairs, wsem, e, ring))
    now = lax.rem(e, ring)
    u, w1, w2, w3 = us.at[now], w1s.at[now], w2s.at[now], w3s.at[now]
    uv = u[...]
    dov = d_out[...]
    for n in range(ff // 256):
        part = slice(n * 256, (n + 1) * 256)
        pre1 = nn(uv, w1[:, part]).astype(BF).astype(F32)
        pre3 = nn(uv, w3[:, part]).astype(BF).astype(F32)
        grad_hid = nt(dov, w2[part, :]).astype(BF).astype(F32)
        sigma = jax.nn.sigmoid(pre1)
        silu = pre1 * sigma
        hid[:, part] = (silu * pre3).astype(BF)
        da1[:, part] = (grad_hid * pre3 * sigma * (1.0 + pre1 * (1.0 - sigma))).astype(BF)
        da3[:, part] = (grad_hid * silu).astype(BF)

    @pl.when(e >= 2)
    def _():
        wait_all(flush(e - 2))

    fresh = flush(e)
    for m in range(ff // 256):
        part = slice(m * 256, (m + 1) * 256)
        o2[slot_e, part] = tn(hid[:, part], dov)
    fresh[1].start()
    for m in range(model // 256):
        part = slice(m * 256, (m + 1) * 256)
        o1[slot_e, part] = tn(u[:, part], da1[...])
        o3[slot_e, part] = tn(u[:, part], da3[...])
    fresh[0].start()
    fresh[2].start()
    live = pl.ds(pl.multiple_of(slot_e * padded, padded), cols)
    for n in range(model // 256):
        part = slice(n * 256, (n + 1) * 256)
        du_two[live, part] = (nt(da1[...], w1[part]) + nt(da3[...], w3[part])).astype(BF)

    @pl.when(slot_e == 1)
    def _():
        mix_into(acc, pick[...], du_two)

    @pl.when(e == count - 1)
    def _():
        sends = part_copies(acc, (p0, p1, p2, p3), psem)
        start_all(sends)
        wait_all(flush(e - 1))
        wait_all(flush(e))
        wait_all(sends)


def expert_bwd(dys, u, w1, w2, w3, tokens):
    model = dys[0].shape[1]
    count, cols, _ = u.shape
    ff = w1.shape[2]
    padded, ring = 256, 3
    hb = pl.BlockSpec(memory_space=pl.ANY)
    part = jax.ShapeDtypeStruct((tokens, model), F32)
    return pl.pallas_call(
        functools.partial(expert_bwd_kernel, cols // 4),
        grid=(count,),
        out_shape=(jax.ShapeDtypeStruct((count, model, ff), F32), jax.ShapeDtypeStruct((count, ff, model), F32), jax.ShapeDtypeStruct((count, model, ff), F32), part, part, part, part),
        in_specs=[hb] * 8,
        out_specs=(hb,) * 7,
        scratch_shapes=[
            pltpu.VMEM((4 * tokens, model), BF), pltpu.VMEM((4, dys[0].shape[0] - tokens, 3 * tokens), BF),
            pltpu.VMEM((ring, cols, model), BF), pltpu.VMEM((ring, model, ff), BF), pltpu.VMEM((ring, ff, model), BF), pltpu.VMEM((ring, model, ff), BF),
            pltpu.VMEM((4 * tokens, 2 * padded), BF), pltpu.VMEM((2 * padded, model), BF),
            pltpu.VMEM((cols, model), BF), pltpu.VMEM((cols, ff), BF), pltpu.VMEM((cols, ff), BF), pltpu.VMEM((cols, ff), BF),
            pltpu.VMEM((2, model, ff), F32), pltpu.VMEM((2, ff, model), F32), pltpu.VMEM((2, model, ff), F32),
            pltpu.VMEM((4 * tokens, model), F32),
            pltpu.SemaphoreType.DMA((8,)), pltpu.SemaphoreType.DMA((ring, 4)), pltpu.SemaphoreType.DMA((2, 3)), pltpu.SemaphoreType.DMA((4,)),
        ],
        compiler_params=pltpu.CompilerParams(vmem_limit_bytes=60 * MIB, dimension_semantics=("arbitrary",)),
        cost_estimate=pl.CostEstimate(flops=50 * 10 ** 9, bytes_accessed=150 * 10 ** 6, transcendentals=0),
        name="expert_bwd",
    )(*dys, u, w1, w2, w3)


def expert_fwd_kernel(u0, u1, u2, u3, d0, d1, d2, d3, w1_h, w2_h, w3_h, p0, p1, p2, p3,
                      rows, info, w1s, w2s, w3s, pick, out_two, acc, late_t, rsem, wsem, psem):
    e = pl.program_id(0)
    count = pl.num_programs(0)
    me = lax.axis_index('expert')
    ring, _, ff = w1s.shape
    slot_e = lax.rem(e, 2)
    arrivals = info_copies((d0, d1, d2, d3), info, rsem) + row_copies((u0, u1, u2, u3), rows, rsem)
    pairs = ((w1_h, w1s), (w3_h, w3s), (w2_h, w2s))

    @pl.when(e == 0)
    def _():
        start_all(arrivals + ring_copies(pairs, wsem, 0, ring) + ring_copies(pairs, wsem, 1, ring))
        acc[...] = jnp.zeros_like(acc)
        wait_all(arrivals)

    @pl.when(e + 2 < count)
    def _():
        start_all(ring_copies(pairs, wsem, e + 2, ring))

    slot_row, gate_row = route_rows(info, 0, me * count + e)
    place_row, filled = places(slot_row, 4)
    wait_all(ring_copies(pairs, wsem, e, ring))
    now = lax.rem(e, ring)
    w1, w2, w3 = w1s.at[now], w2s.at[now], w3s.at[now]

    def run(first):
        hot = hits(place_row, first)
        v = nn(jnp.where(hot, 1.0, 0.0).astype(BF), rows[...]).astype(BF)
        pieces = []
        for n in range(ff // 256):
            part = slice(n * 256, (n + 1) * 256)
            a1 = nn(v, w1[:, part]).astype(BF).astype(F32)
            a3 = nn(v, w3[:, part]).astype(BF).astype(F32)
            pieces.append((a1 * jax.nn.sigmoid(a1) * a3).astype(BF))
        hidden = jnp.concatenate(pieces, axis=1)
        return jnp.transpose(jnp.where(hot, gate_row, 0.0).astype(BF)), nn(hidden, w2[...]).astype(BF)

    chosen, out = run(0)
    half = pl.ds(pl.multiple_of(slot_e * CHUNK, CHUNK), CHUNK)
    pick[:, half] = chosen
    out_two[half, :] = out

    @pl.when(filled > float(CHUNK))
    def _():
        more, out_more = run(CHUNK)
        late_t[...] = more
        mix_into(acc, late_t[...], out_more)

    @pl.when(slot_e == 1)
    def _():
        mix_into(acc, pick[...], out_two)

    @pl.when(e == count - 1)
    def _():
        sends = part_copies(acc, (p0, p1, p2, p3), psem)
        start_all(sends)
        wait_all(sends)


def expert_fwd(us, dys, w1, w2, w3):
    tokens, model = us[0].shape
    count, _, ff = w1.shape
    ring = 3
    part = jax.ShapeDtypeStruct((tokens, model), F32)
    hb = pl.BlockSpec(memory_space=pl.ANY)
    return pl.pallas_call(
        expert_fwd_kernel,
        grid=(count,),
        out_shape=(part, part, part, part),
        in_specs=[hb] * 11,
        out_specs=(hb,) * 4,
        scratch_shapes=[
            pltpu.VMEM((4 * tokens, model), BF), pltpu.VMEM((4, dys[0].shape[0] - tokens, 3 * tokens), BF),
            pltpu.VMEM((ring, model, ff), BF), pltpu.VMEM((ring, ff, model), BF), pltpu.VMEM((ring, model, ff), BF),
            pltpu.VMEM((4 * tokens, 2 * CHUNK), BF), pltpu.VMEM((2 * CHUNK, model), BF),
            pltpu.VMEM((4 * tokens, model), F32), pltpu.VMEM((4 * tokens, CHUNK), BF),
            pltpu.SemaphoreType.DMA((8,)), pltpu.SemaphoreType.DMA((ring, 3)), pltpu.SemaphoreType.DMA((4,)),
        ],
        compiler_params=pltpu.CompilerParams(vmem_limit_bytes=60 * MIB, dimension_semantics=("arbitrary",)),
        cost_estimate=pl.CostEstimate(flops=16 * 10 ** 9, bytes_accessed=50 * 10 ** 6, transcendentals=0),
        name="expert_fwd",
    )(*us, *dys, w1, w2, w3)


def pack_kernel(dy, *refs):
    out = refs[-1]
    tokens = dy.shape[0]
    fields = [r[...].astype(F32) for r in refs[:-1]]
    both = jnp.concatenate([jnp.concatenate(fields[0:3], axis=1), jnp.concatenate(fields[3:6], axis=1)], axis=0)
    out[0:tokens] = dy[...]
    out[tokens:] = jnp.concatenate([both, jnp.zeros((both.shape[0], dy.shape[1] - both.shape[1]), F32)], axis=1).astype(BF)


def pack(dy, fields):
    vm = pl.BlockSpec(memory_space=pltpu.VMEM)
    depth = 2 * fields[0].shape[0]
    return pl.pallas_call(
        pack_kernel,
        out_shape=jax.ShapeDtypeStruct((dy.shape[0] + depth, dy.shape[1]), BF),
        in_specs=[vm] * 7, out_specs=vm,
        compiler_params=pltpu.CompilerParams(vmem_limit_bytes=60 * MIB),
        name="pack",
    )(dy, *fields)


def solution(mesh):
    group = mesh.shape['expert']

    def hop(value, bits):
        return lax.ppermute(value, 'expert', [(i, i ^ bits) for i in range(group)])

    def local_step(x_a, x_b, dy_b, eid_a, slot_a, gate_a, eid_b, slot_b, gate_b, u_b, norm_1, norm_2, w_q, w_k, w_v, w_o, w_1, w_2, w_3):
        model, heads, dim = w_q.shape
        kv_heads = w_k.shape[1]
        reps = heads // kv_heads
        load = pack(dy_b, [a.T for a in (eid_a, slot_a, gate_a, eid_b, slot_b, gate_b)])
        dy2 = hop(load, 2)
        dy1 = hop(load, 1)
        wq_t, wk_t, wv_t = (w.transpose(1, 2, 0).reshape(-1, model) for w in (w_q, w_k, w_v))
        wo = w_o.reshape(-1, model)
        h_a, u_a, h_b, nb, qkv_b, ctx_b = attn_fwd(x_a, x_b, norm_1, norm_2, wq_t, wk_t, wv_t, wo, kv_heads, reps, dim)
        dys = (load, dy1, dy2, hop(dy2, 1))
        us = (u_a, hop(u_a, 1), hop(u_a, 2), hop(u_a, 3))
        g1, g2, g3, b0, b1, b2, b3 = expert_bwd(dys, u_b, w_1, w_2, w_3, x_a.shape[0])
        far_b = hop(b2 + hop(b3, 1), 2)
        near_b = hop(b1, 1)
        a0, a1, a2, a3 = expert_fwd(us, dys, w_1, w_2, w_3)
        far_a = hop(a2 + hop(a3, 1), 2)
        near_a = hop(a1, 1)
        dx_b, g_q, g_k, g_v, g_o, g_n1, g_n2 = attn_bwd(b0, near_b, far_b, dy_b, h_b, x_b, nb, qkv_b, ctx_b, norm_1, norm_2, wo, wq_t, wk_t, wv_t, kv_heads, reps, dim)
        y_a = (h_a.astype(F32) + ((a0 + near_a) + far_a)).astype(BF)
        g_q = g_q.reshape(heads, dim, model).transpose(2, 0, 1)
        g_k = g_k.reshape(kv_heads, dim, model).transpose(2, 0, 1)
        g_v = g_v.reshape(kv_heads, dim, model).transpose(2, 0, 1)
        g_o = g_o.reshape(heads, dim, model)
        return (y_a, dx_b, g1, g2, g3, g_q[None], g_k[None], g_v[None], g_o[None], g_n1, g_n2)

    row_spec = P(('data', 'expert'), None)
    cube_spec = P(('data', 'expert'), None, None)
    quad_spec = P(('data', 'expert'), None, None, None)
    expert_spec = P('expert', None, None)
    in_specs = (row_spec, row_spec, row_spec, row_spec, row_spec, row_spec, row_spec, row_spec, row_spec, cube_spec, P(), P(), P(), P(), P(), P(), expert_spec, expert_spec, expert_spec)
    out_specs = (row_spec, row_spec, cube_spec, cube_spec, cube_spec, quad_spec, quad_spec, quad_spec, quad_spec, row_spec, row_spec)
    return jax.shard_map(local_step, mesh=mesh, in_specs=in_specs, out_specs=out_specs, check_vma=False)
```

```python
import functools

import jax
import jax.numpy as jnp
from jax import lax
from jax.experimental import pallas as pl
from jax.experimental.pallas import tpu as pltpu
from jax.sharding import PartitionSpec as P


NORM_EPS = 1e-6
BF = jnp.bfloat16
F32 = jnp.float32
MIB = 1024 * 1024


def nn(a, b):
    return lax.dot_general(a, b, (((1,), (0,)), ((), ())), preferred_element_type=F32)


def nt(a, b):
    return lax.dot_general(a, b, (((1,), (1,)), ((), ())), preferred_element_type=F32)


def tn(a, b):
    return lax.dot_general(a, b, (((0,), (0,)), ((), ())), preferred_element_type=F32)


def row_of(ref):
    return ref[...].astype(F32).reshape(1, ref.shape[0])


def rms_scale(wide):
    return lax.rsqrt(jnp.mean(wide * wide, axis=-1, keepdims=True) + NORM_EPS)


def rms_rows(values, gain):
    wide = values.astype(F32)
    return (wide * rms_scale(wide) * gain).astype(BF)


def rms_pull(wide, gain, cot):
    scale = rms_scale(wide)
    scaled = wide * scale
    grad_gain = jnp.sum(cot * scaled, axis=0, keepdims=True).astype(BF).astype(F32)
    inner = cot * gain
    pull = jnp.mean(inner * wide, axis=-1, keepdims=True)
    grad = scale * inner - scaled * (scale * scale * pull)
    return grad.astype(BF).astype(F32), grad_gain


def probs_of(scores_t):
    rows = lax.broadcasted_iota(jnp.int32, scores_t.shape, 0)
    cols = lax.broadcasted_iota(jnp.int32, scores_t.shape, 1) % scores_t.shape[0]
    masked = jnp.where(rows <= cols, scores_t, -1e30)
    top = jnp.max(masked, axis=0, keepdims=True)
    unnorm = jnp.exp(masked - top)
    return unnorm / jnp.sum(unnorm, axis=0, keepdims=True)


def heads_to_lanes(ref, group, reps, dim, lanes):
    return jnp.concatenate([ref[(group * reps + r) * dim:(group * reps + r + 1) * dim, lanes] for r in range(reps)], axis=1)


def neighbours():
    me = lax.axis_index('expert')
    return me + 1 - 2 * (me % 2), (me + 2) % 4


def greet(peers):
    barrier = pltpu.get_barrier_semaphore()
    for peer in peers:
        pl.semaphore_signal(barrier, inc=1, device_id={'expert': peer}, device_id_type=pl.DeviceIdType.MESH)
    pl.semaphore_wait(barrier, len(peers))


def remote(src, dst, send, recv, peer):
    return pltpu.make_async_remote_copy(src_ref=src, dst_ref=dst, send_sem=send, recv_sem=recv, device_id={'expert': peer}, device_id_type=pl.DeviceIdType.MESH)


def attn_fwd_kernel(kv_heads, reps, dim, xa_h, xb_h, dy_h, ea, sa, ga, eb, sb, gb, n1, n2, wq_h, wk_h, wv_h, wo_h,
                    ha_h, ua_h, hb_h, nb_h, qkv_h, ctx_h, load_h,
                    xs, wq, wk, wv, wo, nrm, nrm_t, q_t, k_t, v_t, ctx, q_b, ctx_b, hs, ua, mine, far_in, sems, osems, ssem, rsem):
    near, far = neighbours()
    tokens = xs.shape[0] // 2
    heads = kv_heads * reps
    first, second = slice(0, tokens), slice(tokens, 2 * tokens)
    half = heads * dim // 2
    moves = ((dy_h, mine.at[0:tokens]), (xa_h, xs.at[first]), (xb_h, xs.at[second]), (wk_h, wk), (wv_h, wv), (wq_h.at[0:half], wq.at[0:half]), (wq_h.at[half:], wq.at[half:]), (wo_h, wo))
    copies = [pltpu.make_async_copy(s, d, sems.at[i]) for i, (s, d) in enumerate(moves)]
    start_all(copies)
    outs = []

    def flush(src, dst):
        c = pltpu.make_async_copy(src, dst, osems.at[len(outs)])
        c.start()
        outs.append(c)

    fields = [r[...].astype(F32) for r in (ea, sa, ga, eb, sb, gb)]
    both = jnp.concatenate([jnp.concatenate(fields[0:3], axis=1), jnp.concatenate(fields[3:6], axis=1)], axis=0)
    mine[tokens:] = jnp.concatenate([both, jnp.zeros((both.shape[0], mine.shape[1] - both.shape[1]), F32)], axis=1).astype(BF)
    greet((near, far))
    copies[0].wait()
    to_far = remote(mine, far_in, ssem.at[0], rsem.at[0], far)
    to_near = remote(mine, load_h.at[1], ssem.at[1], rsem.at[1], near)
    relay = remote(far_in, load_h.at[3], ssem.at[2], rsem.at[2], near)
    to_far.start()
    to_near.start()
    flush(mine, load_h.at[0])

    wait_all(copies[1:3])
    nrm[...] = rms_rows(xs[...], row_of(n1))
    nrm_t[...] = jnp.transpose(nrm[...])
    flush(nrm.at[second], nb_h)
    copies[3].wait()
    k_t[...] = nn(wk[...], nrm_t[...]).astype(BF)
    copies[4].wait()
    v_t[...] = nn(wv[...], nrm_t[...]).astype(BF)
    for i in range(2):
        copies[5 + i].wait()
        part = slice(i * half, (i + 1) * half)
        q_t[part] = nn(wq[part], nrm_t[...]).astype(BF)
    q_b[0:heads * dim] = q_t[:, second]
    q_b[heads * dim:(heads + kv_heads) * dim] = k_t[:, second]
    q_b[(heads + kv_heads) * dim:] = v_t[:, second]
    flush(q_b, qkv_h)
    for lanes in (second, first):
        for g in range(kv_heads):
            kg = k_t[g * dim:(g + 1) * dim, lanes]
            vg = v_t[g * dim:(g + 1) * dim, lanes]
            qg = heads_to_lanes(q_t, g, reps, dim, lanes)
            probs = probs_of(tn(kg, qg) * dim ** -0.5).astype(BF)
            out = nn(vg, probs).astype(BF)
            for r in range(reps):
                ctx[(g * reps + r) * dim:(g * reps + r + 1) * dim, lanes] = out[:, r * tokens:(r + 1) * tokens]
    ctx_b[...] = ctx[:, second]
    flush(ctx_b, ctx_h)
    to_far.wait_recv()
    relay.start()
    flush(far_in, load_h.at[2])
    copies[7].wait()
    hs[...] = (xs[...].astype(F32) + tn(ctx[...], wo[...]).astype(BF).astype(F32)).astype(BF)
    flush(hs.at[first], ha_h)
    flush(hs.at[second], hb_h)
    ua[...] = rms_rows(hs[first], row_of(n2))
    flush(ua, ua_h)
    to_far.wait_send()
    to_near.wait()
    relay.wait()
    wait_all(outs)


def attn_fwd(x_a, x_b, dy, fields, n1, n2, wq, wk, wv, wo, kv_heads, reps, dim):
    tokens, model = x_a.shape
    q_dim, kv_dim = kv_heads * reps * dim, kv_heads * dim
    depth = 2 * fields[0].shape[0]
    vm = pl.BlockSpec(memory_space=pltpu.VMEM)
    hb = pl.BlockSpec(memory_space=pl.ANY)
    row = jax.ShapeDtypeStruct((tokens, model), BF)
    return pl.pallas_call(
        functools.partial(attn_fwd_kernel, kv_heads, reps, dim),
        out_shape=(row, row, row, row, jax.ShapeDtypeStruct((q_dim + 2 * kv_dim, tokens), BF), jax.ShapeDtypeStruct((q_dim, tokens), BF), jax.ShapeDtypeStruct((4, tokens + depth, model), BF)),
        in_specs=[hb] * 3 + [vm] * 8 + [hb] * 4,
        out_specs=(hb,) * 7,
        scratch_shapes=[
            pltpu.VMEM((2 * tokens, model), BF),
            pltpu.VMEM((q_dim, model), BF), pltpu.VMEM((kv_dim, model), BF), pltpu.VMEM((kv_dim, model), BF), pltpu.VMEM((q_dim, model), BF),
            pltpu.VMEM((2 * tokens, model), BF), pltpu.VMEM((model, 2 * tokens), BF),
            pltpu.VMEM((q_dim, 2 * tokens), BF), pltpu.VMEM((kv_dim, 2 * tokens), BF), pltpu.VMEM((kv_dim, 2 * tokens), BF), pltpu.VMEM((q_dim, 2 * tokens), BF),
            pltpu.VMEM((q_dim + 2 * kv_dim, tokens), BF), pltpu.VMEM((q_dim, tokens), BF), pltpu.VMEM((2 * tokens, model), BF), pltpu.VMEM((tokens, model), BF),
            pltpu.VMEM((tokens + depth, model), BF), pltpu.VMEM((tokens + depth, model), BF),
            pltpu.SemaphoreType.DMA((8,)), pltpu.SemaphoreType.DMA((8,)), pltpu.SemaphoreType.DMA((3,)), pltpu.SemaphoreType.DMA((3,)),
        ],
        compiler_params=pltpu.CompilerParams(vmem_limit_bytes=60 * MIB, collective_id=0, has_side_effects=True),
        cost_estimate=pl.CostEstimate(flops=10 ** 10, bytes_accessed=14 * 10 ** 6, transcendentals=0),
        name="attn_fwd",
    )(x_a, x_b, dy, *fields, n1, n2, wq, wk, wv, wo)


def attn_bwd_kernel(kv_heads, reps, dim, du_in, dy, h_b, x_b, nb, qkv, ctx, n1, n2, wo_h, wq_h, wk_h, wv_h,
                    dx, gq, gk, gv, go, gn1, gn2,
                    wo, wq, wk, wv, oq, ok, ov, oo, dctx, dq, dk, dv, sems, osems):
    copies = [pltpu.make_async_copy(s, d, sems.at[i]) for i, (s, d) in enumerate(((wo_h, wo), (wq_h, wq), (wk_h, wk), (wv_h, wv)))]
    for c in copies:
        c.start()
    tokens = x_b.shape[0]
    q_dim, kv_dim = kv_heads * reps * dim, kv_heads * dim
    du = du_in[...].astype(F32)
    grad_h, g2 = rms_pull(h_b[...].astype(F32), row_of(n2), du)
    gn2[...] = g2
    dh = (dy[...].astype(F32) + grad_h).astype(BF)
    copies[0].wait()
    outs = []

    def flush(src, dst):
        c = pltpu.make_async_copy(src, dst, osems.at[len(outs)])
        c.start()
        outs.append(c)

    step = q_dim // 4
    for i in range(4):
        dctx[i * step:(i + 1) * step] = nt(wo[i * step:(i + 1) * step], dh).astype(BF)
    for i in range(4):
        part = slice(i * step, (i + 1) * step)
        oo[part] = nn(ctx[part], dh).astype(BF).astype(F32)
        flush(oo.at[part], go.at[part])
    every = slice(0, tokens)
    normed = nb[...]
    for g in range(kv_heads):
        kv = slice(g * dim, (g + 1) * dim)
        kg = qkv[q_dim + g * dim:q_dim + (g + 1) * dim]
        vg = qkv[q_dim + kv_dim + g * dim:q_dim + kv_dim + (g + 1) * dim]
        qg = heads_to_lanes(qkv, g, reps, dim, every)
        dg = heads_to_lanes(dctx, g, reps, dim, every)
        probs = probs_of(tn(kg, qg) * dim ** -0.5)
        dprobs = tn(vg, dg).astype(BF).astype(F32)
        weighted = probs * dprobs
        dscores = ((weighted - probs * jnp.sum(weighted, axis=0, keepdims=True)) * dim ** -0.5).astype(BF)
        dv[kv] = nt(dg, probs.astype(BF)).astype(BF)
        dk[kv] = nt(qg, dscores).astype(BF)
        dqg = nn(kg, dscores).astype(BF)
        for r in range(reps):
            dq[(g * reps + r) * dim:(g * reps + r + 1) * dim] = dqg[:, r * tokens:(r + 1) * tokens]
        if g % 2 == 1:
            part = slice((g - 1) * reps * dim, (g + 1) * reps * dim)
            oq[part] = nn(dq[part], normed).astype(BF).astype(F32)
            flush(oq.at[part], gq.at[part])
    ok[...] = nn(dk[...], normed).astype(BF).astype(F32)
    flush(ok, gk)
    ov[...] = nn(dv[...], normed).astype(BF).astype(F32)
    flush(ov, gv)
    for c in copies[1:]:
        c.wait()
    dn = (tn(dq[...], wq[...]) + tn(dk[...], wk[...]) + tn(dv[...], wv[...])).astype(BF).astype(F32)
    grad_x, g1 = rms_pull(x_b[...].astype(F32), row_of(n1), dn)
    gn1[...] = g1
    dx[...] = (dh.astype(F32) + grad_x).astype(BF)
    for c in outs:
        c.wait()


def attn_bwd(du, dy, h_b, x_b, nb, qkv, ctx, n1, n2, wo, wq, wk, wv, kv_heads, reps, dim):
    tokens, model = x_b.shape
    q_dim, kv_dim = kv_heads * reps * dim, kv_heads * dim
    vm = pl.BlockSpec(memory_space=pltpu.VMEM)
    hb = pl.BlockSpec(memory_space=pl.ANY)
    n_out = 4 + kv_heads // 2 + 2
    return pl.pallas_call(
        functools.partial(attn_bwd_kernel, kv_heads, reps, dim),
        out_shape=(
            jax.ShapeDtypeStruct((tokens, model), BF), jax.ShapeDtypeStruct((q_dim, model), F32), jax.ShapeDtypeStruct((kv_dim, model), F32),
            jax.ShapeDtypeStruct((kv_dim, model), F32), jax.ShapeDtypeStruct((q_dim, model), F32), jax.ShapeDtypeStruct((1, model), F32), jax.ShapeDtypeStruct((1, model), F32),
        ),
        in_specs=[vm] * 9 + [hb] * 4,
        out_specs=(vm, hb, hb, hb, hb, vm, vm),
        scratch_shapes=[
            pltpu.VMEM((q_dim, model), BF), pltpu.VMEM((q_dim, model), BF), pltpu.VMEM((kv_dim, model), BF), pltpu.VMEM((kv_dim, model), BF),
            pltpu.VMEM((q_dim, model), F32), pltpu.VMEM((kv_dim, model), F32), pltpu.VMEM((kv_dim, model), F32), pltpu.VMEM((q_dim, model), F32),
            pltpu.VMEM((q_dim, tokens), BF), pltpu.VMEM((q_dim, tokens), BF), pltpu.VMEM((kv_dim, tokens), BF), pltpu.VMEM((kv_dim, tokens), BF),
            pltpu.SemaphoreType.DMA((4,)), pltpu.SemaphoreType.DMA((n_out,)),
        ],
        compiler_params=pltpu.CompilerParams(vmem_limit_bytes=60 * MIB),
        cost_estimate=pl.CostEstimate(flops=14 * 10 ** 9, bytes_accessed=40 * 10 ** 6, transcendentals=0),
        name="attn_bwd",
    )(du, dy, h_b, x_b, nb, qkv, ctx, n1, n2, wo, wq, wk, wv)


def route_rows(info, base, expert):
    group, _, width = info.shape
    tokens = width // 3
    top_k = info.shape[1] // 2
    wide = [info[r].astype(F32)[base * top_k:(base + 1) * top_k] for r in range(group)]

    def field(i):
        return jnp.concatenate([w[:, i * tokens:(i + 1) * tokens] for w in wide], axis=1)

    eid, slot, gate = field(0), field(1), field(2)
    hit = (eid == expert.astype(F32)) & (slot >= 0.0)
    slot_row = jnp.sum(jnp.where(hit, slot + 1.0, 0.0), axis=0, keepdims=True) - 1.0
    gate_row = jnp.sum(jnp.where(hit, gate, 0.0), axis=0, keepdims=True)
    return slot_row, gate_row


def ring_copies(pairs, sem, idx, ring):
    s = lax.rem(idx, ring)
    return [pltpu.make_async_copy(src.at[idx], dst.at[s], sem.at[s, i]) for i, (src, dst) in enumerate(pairs)]


def row_copies(refs, rows, sem):
    tokens = rows.shape[0] // len(refs)
    return [pltpu.make_async_copy(ref.at[0:tokens], rows.at[r * tokens:(r + 1) * tokens], sem.at[r]) for r, ref in enumerate(refs)]


def info_copy(loads, info, sem):
    _, depth, width = info.shape
    first = loads.shape[1] - depth
    return [pltpu.make_async_copy(loads.at[:, first:first + depth, 0:width], info, sem.at[4])]


def part_copies(acc, refs, sem):
    tokens = acc.shape[0] // len(refs)
    return [pltpu.make_async_copy(acc.at[r * tokens:(r + 1) * tokens], ref, sem.at[r]) for r, ref in enumerate(refs)]


def start_all(copies):
    for c in copies:
        c.start()


def wait_all(copies):
    for c in copies:
        c.wait()


def mix_into(acc, pick, outs):
    for n in range(acc.shape[1] // 256):
        part = slice(n * 256, (n + 1) * 256)
        acc[:, part] += nn(pick, outs[:, part])


def expert_bwd_kernel(capacity, loads, u_h, w1_h, w2_h, w3_h,
                      g1, g2, g3, p0, p1, p2, p3,
                      rows, info, us, w1s, w2s, w3s, pick, du_two, d_out, hid, da1, da3, o1, o2, o3, acc, rsem, wsem, sems, psem):
    e = pl.program_id(0)
    count = pl.num_programs(0)
    me = lax.axis_index('expert')
    slot_e = lax.rem(e, 2)
    ring, cols, model = us.shape
    tokens = rows.shape[0] // 4
    ff = w1s.shape[2]
    padded = du_two.shape[0] // 2
    arrivals = info_copy(loads, info, rsem) + row_copies([loads.at[r] for r in range(4)], rows, rsem)
    pairs = ((u_h, us), (w1_h, w1s), (w3_h, w3s), (w2_h, w2s))

    @pl.when(e == 0)
    def _():
        start_all(arrivals + ring_copies(pairs, wsem, 0, ring) + ring_copies(pairs, wsem, 1, ring))
        acc[...] = jnp.zeros_like(acc)
        du_two[...] = jnp.zeros_like(du_two)
        wait_all(arrivals)

    @pl.when(e + 2 < count)
    def _():
        start_all(ring_copies(pairs, wsem, e + 2, ring))

    slot_row, gate_row = route_rows(info, 1, me * count + e)
    device = jnp.bitwise_xor(lax.broadcasted_iota(jnp.int32, slot_row.shape, 1) // tokens, me)
    col_row = jnp.where(slot_row >= 0.0, slot_row.astype(jnp.int32) + device * capacity, -1)
    hot = lax.broadcasted_iota(jnp.int32, (padded, 4 * tokens), 0) == col_row
    pick[:, pl.ds(pl.multiple_of(slot_e * padded, padded), padded)] = jnp.transpose(jnp.where(hot, 1.0, 0.0).astype(BF))
    d_out[...] = nn(jnp.where(hot, gate_row, 0.0).astype(BF)[0:cols], rows[...]).astype(BF)

    def flush(idx):
        s = lax.rem(idx, 2)
        return [pltpu.make_async_copy(src.at[s], dst.at[idx], sems.at[s, i]) for i, (src, dst) in enumerate(((o1, g1), (o2, g2), (o3, g3)))]

    wait_all(ring_copies(pairs, wsem, e, ring))
    now = lax.rem(e, ring)
    u, w1, w2, w3 = us.at[now], w1s.at[now], w2s.at[now], w3s.at[now]
    uv = u[...]
    dov = d_out[...]
    for n in range(ff // 256):
        part = slice(n * 256, (n + 1) * 256)
        pre1 = nn(uv, w1[:, part]).astype(BF).astype(F32)
        pre3 = nn(uv, w3[:, part]).astype(BF).astype(F32)
        grad_hid = nt(dov, w2[part, :]).astype(BF).astype(F32)
        sigma = jax.nn.sigmoid(pre1)
        silu = pre1 * sigma
        hid[:, part] = (silu * pre3).astype(BF)
        da1[:, part] = (grad_hid * pre3 * sigma * (1.0 + pre1 * (1.0 - sigma))).astype(BF)
        da3[:, part] = (grad_hid * silu).astype(BF)

    @pl.when(e >= 2)
    def _():
        wait_all(flush(e - 2))

    fresh = flush(e)
    for m in range(ff // 256):
        part = slice(m * 256, (m + 1) * 256)
        o2[slot_e, part] = tn(hid[:, part], dov)
    fresh[1].start()
    for m in range(model // 256):
        part = slice(m * 256, (m + 1) * 256)
        o1[slot_e, part] = tn(u[:, part], da1[...])
        o3[slot_e, part] = tn(u[:, part], da3[...])
    fresh[0].start()
    fresh[2].start()
    live = pl.ds(pl.multiple_of(slot_e * padded, padded), cols)
    for n in range(model // 256):
        part = slice(n * 256, (n + 1) * 256)
        du_two[live, part] = (nt(da1[...], w1[part]) + nt(da3[...], w3[part])).astype(BF)

    @pl.when(slot_e == 1)
    def _():
        mix_into(acc, pick[...], du_two)

    @pl.when(e == count - 1)
    def _():
        sends = part_copies(acc, (p0, p1, p2, p3), psem)
        start_all(sends)
        wait_all(flush(e - 1))
        wait_all(flush(e))
        wait_all(sends)


def expert_bwd(loads, u, w1, w2, w3, tokens):
    model = loads.shape[2]
    count, cols, _ = u.shape
    ff = w1.shape[2]
    padded, ring = 256, 3
    hb = pl.BlockSpec(memory_space=pl.ANY)
    part = jax.ShapeDtypeStruct((tokens, model), F32)
    return pl.pallas_call(
        functools.partial(expert_bwd_kernel, cols // 4),
        grid=(count,),
        out_shape=(jax.ShapeDtypeStruct((count, model, ff), F32), jax.ShapeDtypeStruct((count, ff, model), F32), jax.ShapeDtypeStruct((count, model, ff), F32), part, part, part, part),
        in_specs=[hb] * 5,
        out_specs=(hb,) * 7,
        scratch_shapes=[
            pltpu.VMEM((4 * tokens, model), BF), pltpu.VMEM((4, loads.shape[1] - tokens, 3 * tokens), BF),
            pltpu.VMEM((ring, cols, model), BF), pltpu.VMEM((ring, model, ff), BF), pltpu.VMEM((ring, ff, model), BF), pltpu.VMEM((ring, model, ff), BF),
            pltpu.VMEM((4 * tokens, 2 * padded), BF), pltpu.VMEM((2 * padded, model), BF),
            pltpu.VMEM((cols, model), BF), pltpu.VMEM((cols, ff), BF), pltpu.VMEM((cols, ff), BF), pltpu.VMEM((cols, ff), BF),
            pltpu.VMEM((2, model, ff), F32), pltpu.VMEM((2, ff, model), F32), pltpu.VMEM((2, model, ff), F32),
            pltpu.VMEM((4 * tokens, model), F32),
            pltpu.SemaphoreType.DMA((5,)), pltpu.SemaphoreType.DMA((ring, 4)), pltpu.SemaphoreType.DMA((2, 3)), pltpu.SemaphoreType.DMA((4,)),
        ],
        compiler_params=pltpu.CompilerParams(vmem_limit_bytes=60 * MIB, dimension_semantics=("arbitrary",)),
        cost_estimate=pl.CostEstimate(flops=50 * 10 ** 9, bytes_accessed=150 * 10 ** 6, transcendentals=0),
        name="expert_bwd",
    )(loads, u, w1, w2, w3)


def expert_fwd_kernel(capacity, u0, u1, u2, u3, loads, b0, b1, b2, b3, w1_h, w2_h, w3_h, du_o, mine_o, out_o,
                      rows, info, w1s, w2s, w3s, pick, out_two, acc, loc0, loc2, rx1, rx3, rxf, ra1, ra3, rsem, wsem, bsem, ssem, xsem):
    e = pl.program_id(0)
    count = pl.num_programs(0)
    me = lax.axis_index('expert')
    near, far = neighbours()
    ring, _, ff = w1s.shape
    slot_e = e % 2
    tokens = rows.shape[0] // 4
    cols = 4 * capacity
    padded = out_two.shape[0] // 2
    arrivals = info_copy(loads, info, rsem) + row_copies((u0, u1, u2, u3), rows, rsem)
    pairs = ((w1_h, w1s), (w3_h, w3s), (w2_h, w2s))
    local = [pltpu.make_async_copy(b0, loc0, bsem.at[0]), pltpu.make_async_copy(b2, loc2, bsem.at[1])]
    swap3 = remote(b3, rx3, ssem.at[0], xsem.at[0], near)
    swap1 = remote(b1, rx1, ssem.at[1], xsem.at[1], near)
    over = remote(loc2, rxf, ssem.at[2], xsem.at[2], far)
    part = [slice(r * tokens, (r + 1) * tokens) for r in range(4)]
    late3 = remote(acc.at[part[3]], ra3, ssem.at[3], xsem.at[3], near)
    late1 = remote(acc.at[part[1]], ra1, ssem.at[4], xsem.at[4], near)

    @pl.when(e == 0)
    def _():
        start_all(arrivals + ring_copies(pairs, wsem, 0, ring) + ring_copies(pairs, wsem, 1, ring) + local)
        greet((near, far))
        swap3.start()
        swap1.start()
        acc[...] = jnp.zeros_like(acc)
        out_two[...] = jnp.zeros_like(out_two)
        wait_all(arrivals)

    @pl.when(e == 1)
    def _():
        wait_all(local)
        swap3.wait()
        loc2[...] += rx3[...]
        over.start()

    @pl.when(e + 2 < count)
    def _():
        start_all(ring_copies(pairs, wsem, e + 2, ring))

    slot_row, gate_row = route_rows(info, 0, me * count + e)
    group = lax.broadcasted_iota(jnp.int32, slot_row.shape, 1) // tokens
    col_row = jnp.where(slot_row >= 0.0, slot_row.astype(jnp.int32) + group * capacity, -1)
    hot = lax.broadcasted_iota(jnp.int32, (padded, 4 * tokens), 0) == col_row
    pick[:, pl.ds(pl.multiple_of(slot_e * padded, padded), padded)] = jnp.transpose(jnp.where(hot, gate_row, 0.0).astype(BF))
    v = nn(jnp.where(hot, 1.0, 0.0).astype(BF)[0:cols], rows[...]).astype(BF)
    wait_all(ring_copies(pairs, wsem, e, ring))
    now = e % ring
    w1, w2, w3 = w1s.at[now], w2s.at[now], w3s.at[now]
    pieces = []
    for n in range(ff // 256):
        lanes = slice(n * 256, (n + 1) * 256)
        a1 = nn(v, w1[:, lanes]).astype(BF).astype(F32)
        a3 = nn(v, w3[:, lanes]).astype(BF).astype(F32)
        pieces.append((a1 * jax.nn.sigmoid(a1) * a3).astype(BF))
    out_two[pl.ds(pl.multiple_of(slot_e * padded, padded), cols), :] = nn(jnp.concatenate(pieces, axis=1), w2[...]).astype(BF)

    @pl.when(slot_e == 1)
    def _():
        mix_into(acc, pick[...], out_two)

    @pl.when(e == count - 1)
    def _():
        late3.start()
        late1.start()
        swap1.wait()
        over.wait()
        du_o[...] = ((loc0[...] + rx1[...]) + rxf[...]).astype(BF)
        late3.wait()
        out_o[...] = acc[part[2]] + ra3[...]
        late1.wait()
        mine_o[...] = acc[part[0]] + ra1[...]


def whole(shape):
    return pl.BlockSpec(shape, lambda e: (0,) * len(shape), pipeline_mode=pl.Buffered(1))


def expert_fwd(us, loads, sums, w1, w2, w3, capacity):
    tokens, model = us[0].shape
    count, _, ff = w1.shape
    padded, ring = 256, 3
    part = jax.ShapeDtypeStruct((tokens, model), F32)
    hb = pl.BlockSpec(memory_space=pl.ANY)
    tile = pltpu.VMEM((tokens, model), F32)
    return pl.pallas_call(
        functools.partial(expert_fwd_kernel, capacity),
        grid=(count,),
        out_shape=(jax.ShapeDtypeStruct((tokens, model), BF), part, part),
        in_specs=[hb] * 12,
        out_specs=(whole((tokens, model)),) * 3,
        scratch_shapes=[
            pltpu.VMEM((4 * tokens, model), BF), pltpu.VMEM((4, loads.shape[1] - tokens, 3 * tokens), BF),
            pltpu.VMEM((ring, model, ff), BF), pltpu.VMEM((ring, ff, model), BF), pltpu.VMEM((ring, model, ff), BF),
            pltpu.VMEM((4 * tokens, 2 * padded), BF), pltpu.VMEM((2 * padded, model), BF), pltpu.VMEM((4 * tokens, model), F32),
            tile, tile, tile, tile, tile, tile, tile,
            pltpu.SemaphoreType.DMA((5,)), pltpu.SemaphoreType.DMA((ring, 3)), pltpu.SemaphoreType.DMA((2,)), pltpu.SemaphoreType.DMA((5,)), pltpu.SemaphoreType.DMA((5,)),
        ],
        compiler_params=pltpu.CompilerParams(vmem_limit_bytes=60 * MIB, dimension_semantics=("arbitrary",), collective_id=1, has_side_effects=True),
        cost_estimate=pl.CostEstimate(flops=16 * 10 ** 9, bytes_accessed=50 * 10 ** 6, transcendentals=0),
        name="expert_fwd",
    )(*us, loads, *sums, w1, w2, w3)


def solution(mesh):
    group = mesh.shape['expert']

    def hop(value, bits):
        return lax.ppermute(value, 'expert', [(i, i ^ bits) for i in range(group)])

    def local_step(x_a, x_b, dy_b, eid_a, slot_a, gate_a, eid_b, slot_b, gate_b, u_b, norm_1, norm_2, w_q, w_k, w_v, w_o, w_1, w_2, w_3):
        model, heads, dim = w_q.shape
        kv_heads = w_k.shape[1]
        reps = heads // kv_heads
        wq_t, wk_t, wv_t = (w.transpose(1, 2, 0).reshape(-1, model) for w in (w_q, w_k, w_v))
        wo = w_o.reshape(-1, model)
        fields = [a.T for a in (eid_a, slot_a, gate_a, eid_b, slot_b, gate_b)]
        h_a, u_a, h_b, nb, qkv_b, ctx_b, loads = attn_fwd(x_a, x_b, dy_b, fields, norm_1, norm_2, wq_t, wk_t, wv_t, wo, kv_heads, reps, dim)
        us = (u_a, hop(u_a, 1), hop(u_a, 2), hop(u_a, 3))
        g1, g2, g3, *sums = expert_bwd(loads, u_b, w_1, w_2, w_3, x_a.shape[0])
        du, mine_a, out_a = expert_fwd(us, loads, sums, w_1, w_2, w_3, u_b.shape[1] // group)
        far_a = hop(out_a, 2)
        dx_b, g_q, g_k, g_v, g_o, g_n1, g_n2 = attn_bwd(du, dy_b, h_b, x_b, nb, qkv_b, ctx_b, norm_1, norm_2, wo, wq_t, wk_t, wv_t, kv_heads, reps, dim)
        y_a = (h_a.astype(F32) + (mine_a + far_a)).astype(BF)
        g_q = g_q.reshape(heads, dim, model).transpose(2, 0, 1)
        g_k = g_k.reshape(kv_heads, dim, model).transpose(2, 0, 1)
        g_v = g_v.reshape(kv_heads, dim, model).transpose(2, 0, 1)
        g_o = g_o.reshape(heads, dim, model)
        return (y_a, dx_b, g1, g2, g3, g_q[None], g_k[None], g_v[None], g_o[None], g_n1, g_n2)

    row_spec = P(('data', 'expert'), None)
    cube_spec = P(('data', 'expert'), None, None)
    quad_spec = P(('data', 'expert'), None, None, None)
    expert_spec = P('expert', None, None)
    in_specs = (row_spec, row_spec, row_spec, row_spec, row_spec, row_spec, row_spec, row_spec, row_spec, cube_spec, P(), P(), P(), P(), P(), P(), expert_spec, expert_spec, expert_spec)
    out_specs = (row_spec, row_spec, cube_spec, cube_spec, cube_spec, quad_spec, quad_spec, quad_spec, quad_spec, row_spec, row_spec)
    return jax.shard_map(local_step, mesh=mesh, in_specs=in_specs, out_specs=out_specs, check_vma=False)
```

```python
import functools

import jax
import jax.numpy as jnp
from jax import lax
from jax.experimental import pallas as pl
from jax.experimental.pallas import tpu as pltpu
from jax.sharding import PartitionSpec as P


NORM_EPS = 1e-6
BF = jnp.bfloat16
F32 = jnp.float32
VMEM_BYTES = 67043328
QUAD = 4
BLOCK = 64


def nn(a, b):
    return lax.dot_general(a, b, (((1,), (0,)), ((), ())), preferred_element_type=F32)


def nt(a, b):
    return lax.dot_general(a, b, (((1,), (1,)), ((), ())), preferred_element_type=F32)


def tn(a, b):
    return lax.dot_general(a, b, (((0,), (0,)), ((), ())), preferred_element_type=F32)


def row_of(ref):
    return ref[...].astype(F32).reshape(1, ref.shape[0])


def rms_scale(wide):
    return lax.rsqrt(jnp.mean(wide * wide, axis=-1, keepdims=True) + NORM_EPS)


def rms_rows(values, gain):
    wide = values.astype(F32)
    return (wide * rms_scale(wide) * gain).astype(BF)


def rms_pull(wide, gain, cot):
    scale = rms_scale(wide)
    scaled = wide * scale
    grad_gain = jnp.sum(cot * scaled, axis=0, keepdims=True).astype(BF).astype(F32)
    inner = cot * gain
    pull = jnp.mean(inner * wide, axis=-1, keepdims=True)
    grad = scale * inner - scaled * (scale * scale * pull)
    return grad.astype(BF).astype(F32), grad_gain


def probs_of(scores_t):
    rows = lax.broadcasted_iota(jnp.int32, scores_t.shape, 0)
    cols = lax.broadcasted_iota(jnp.int32, scores_t.shape, 1) % scores_t.shape[0]
    masked = jnp.where(rows <= cols, scores_t, -1e30)
    top = jnp.max(masked, axis=0, keepdims=True)
    unnorm = jnp.exp(masked - top)
    return unnorm / jnp.sum(unnorm, axis=0, keepdims=True)


def heads_to_lanes(ref, group, reps, dim, lanes):
    return jnp.concatenate([ref[(group * reps + r) * dim:(group * reps + r + 1) * dim, lanes] for r in range(reps)], axis=1)


def neighbours():
    me = lax.axis_index('expert')
    return me + 1 - 2 * (me % 2), (me + 2) % 4


def greet(peers):
    barrier = pltpu.get_barrier_semaphore()
    for peer in peers:
        pl.semaphore_signal(barrier, inc=1, device_id={'expert': peer}, device_id_type=pl.DeviceIdType.MESH)
    pl.semaphore_wait(barrier, len(peers))


def remote(src, dst, send, recv, peer):
    return pltpu.make_async_remote_copy(src_ref=src, dst_ref=dst, send_sem=send, recv_sem=recv, device_id={'expert': peer}, device_id_type=pl.DeviceIdType.MESH)


def attn_fwd_kernel(kv_heads, reps, dim, xa_h, xb_h, dy_h, ea, sa, ga, eb, sb, gb, n1, n2, wq_h, wk_h, wv_h, wo_h,
                    ha_h, ua_h, hb_h, nb_h, qkv_h, ctx_h, load_h,
                    xs, wq, wk, wv, wo, nrm, nrm_t, q_t, k_t, v_t, ctx, q_b, ctx_b, hs, ua, mine, far_in, sems, osems, ssem, rsem):
    near, far = neighbours()
    tokens = xs.shape[0] // 2
    heads = kv_heads * reps
    first, second = slice(0, tokens), slice(tokens, 2 * tokens)
    half = heads * dim // 2
    moves = ((dy_h, mine.at[0:tokens]), (xa_h, xs.at[first]), (xb_h, xs.at[second]), (wk_h, wk), (wv_h, wv), (wq_h.at[0:half], wq.at[0:half]), (wq_h.at[half:], wq.at[half:]), (wo_h, wo))
    copies = [pltpu.make_async_copy(s, d, sems.at[i]) for i, (s, d) in enumerate(moves)]
    start_all(copies)
    outs = []

    def flush(src, dst):
        c = pltpu.make_async_copy(src, dst, osems.at[len(outs)])
        c.start()
        outs.append(c)

    fields = [r[...].astype(F32) for r in (ea, sa, ga, eb, sb, gb)]
    both = jnp.concatenate([jnp.concatenate(fields[0:3], axis=1), jnp.concatenate(fields[3:6], axis=1)], axis=0)
    mine[tokens:] = jnp.concatenate([both, jnp.zeros((both.shape[0], mine.shape[1] - both.shape[1]), F32)], axis=1).astype(BF)
    greet((near, far))
    copies[0].wait()
    to_far = remote(mine, far_in, ssem.at[0], rsem.at[0], far)
    to_near = remote(mine, load_h.at[1], ssem.at[1], rsem.at[1], near)
    relay = remote(far_in, load_h.at[3], ssem.at[2], rsem.at[2], near)
    to_far.start()
    to_near.start()
    flush(mine, load_h.at[0])

    wait_all(copies[1:3])
    nrm[...] = rms_rows(xs[...], row_of(n1))
    nrm_t[...] = jnp.transpose(nrm[...])
    flush(nrm.at[second], nb_h)
    copies[3].wait()
    k_t[...] = nn(wk[...], nrm_t[...]).astype(BF)
    copies[4].wait()
    v_t[...] = nn(wv[...], nrm_t[...]).astype(BF)
    for i in range(2):
        copies[5 + i].wait()
        part = slice(i * half, (i + 1) * half)
        q_t[part] = nn(wq[part], nrm_t[...]).astype(BF)
    q_b[0:heads * dim] = q_t[:, second]
    q_b[heads * dim:(heads + kv_heads) * dim] = k_t[:, second]
    q_b[(heads + kv_heads) * dim:] = v_t[:, second]
    flush(q_b, qkv_h)
    for lanes in (second, first):
        for g in range(kv_heads):
            kg = k_t[g * dim:(g + 1) * dim, lanes]
            vg = v_t[g * dim:(g + 1) * dim, lanes]
            qg = heads_to_lanes(q_t, g, reps, dim, lanes)
            probs = probs_of(tn(kg, qg) * dim ** -0.5).astype(BF)
            out = nn(vg, probs).astype(BF)
            for r in range(reps):
                ctx[(g * reps + r) * dim:(g * reps + r + 1) * dim, lanes] = out[:, r * tokens:(r + 1) * tokens]
    ctx_b[...] = ctx[:, second]
    flush(ctx_b, ctx_h)
    copies[7].wait()
    hs[...] = (xs[...].astype(F32) + tn(ctx[...], wo[...]).astype(BF).astype(F32)).astype(BF)
    to_far.wait_recv()
    relay.start()
    flush(far_in, load_h.at[2])
    flush(hs.at[first], ha_h)
    flush(hs.at[second], hb_h)
    ua[...] = rms_rows(hs[first], row_of(n2))
    flush(ua, ua_h)
    to_far.wait_send()
    to_near.wait()
    relay.wait()
    wait_all(outs)


def attn_fwd(x_a, x_b, dy, fields, n1, n2, wq, wk, wv, wo, kv_heads, reps, dim):
    tokens, model = x_a.shape
    q_dim, kv_dim = kv_heads * reps * dim, kv_heads * dim
    depth = 2 * fields[0].shape[0]
    vm = pl.BlockSpec(memory_space=pltpu.VMEM)
    hb = pl.BlockSpec(memory_space=pl.ANY)
    row = jax.ShapeDtypeStruct((tokens, model), BF)
    return pl.pallas_call(
        functools.partial(attn_fwd_kernel, kv_heads, reps, dim),
        out_shape=(row, row, row, row, jax.ShapeDtypeStruct((q_dim + 2 * kv_dim, tokens), BF), jax.ShapeDtypeStruct((q_dim, tokens), BF), jax.ShapeDtypeStruct((4, tokens + depth, model), BF)),
        in_specs=[hb] * 3 + [vm] * 8 + [hb] * 4,
        out_specs=(hb,) * 7,
        scratch_shapes=[
            pltpu.VMEM((2 * tokens, model), BF),
            pltpu.VMEM((q_dim, model), BF), pltpu.VMEM((kv_dim, model), BF), pltpu.VMEM((kv_dim, model), BF), pltpu.VMEM((q_dim, model), BF),
            pltpu.VMEM((2 * tokens, model), BF), pltpu.VMEM((model, 2 * tokens), BF),
            pltpu.VMEM((q_dim, 2 * tokens), BF), pltpu.VMEM((kv_dim, 2 * tokens), BF), pltpu.VMEM((kv_dim, 2 * tokens), BF), pltpu.VMEM((q_dim, 2 * tokens), BF),
            pltpu.VMEM((q_dim + 2 * kv_dim, tokens), BF), pltpu.VMEM((q_dim, tokens), BF), pltpu.VMEM((2 * tokens, model), BF), pltpu.VMEM((tokens, model), BF),
            pltpu.VMEM((tokens + depth, model), BF), pltpu.VMEM((tokens + depth, model), BF),
            pltpu.SemaphoreType.DMA((8,)), pltpu.SemaphoreType.DMA((8,)), pltpu.SemaphoreType.DMA((3,)), pltpu.SemaphoreType.DMA((3,)),
        ],
        compiler_params=pltpu.CompilerParams(vmem_limit_bytes=VMEM_BYTES, collective_id=0, has_side_effects=True),
        cost_estimate=pl.CostEstimate(flops=10 ** 10, bytes_accessed=14 * 10 ** 6, transcendentals=0),
        name="attn_fwd",
    )(x_a, x_b, dy, *fields, n1, n2, wq, wk, wv, wo)


def attn_bwd_kernel(kv_heads, reps, dim, du_in, dy, h_b, x_b, nb, qkv, ctx, n1, n2, wo_h, wq_h, wk_h, wv_h,
                    dx, gq, gk, gv, go, gn1, gn2,
                    wo, wq, wk, wv, oq, ok, ov, oo, dctx, dq, dk, dv, sems, osems):
    copies = [pltpu.make_async_copy(s, d, sems.at[i]) for i, (s, d) in enumerate(((wo_h, wo), (wq_h, wq), (wk_h, wk), (wv_h, wv)))]
    for c in copies:
        c.start()
    tokens = x_b.shape[0]
    q_dim, kv_dim = kv_heads * reps * dim, kv_heads * dim
    du = du_in[...].astype(F32)
    grad_h, g2 = rms_pull(h_b[...].astype(F32), row_of(n2), du)
    gn2[...] = g2
    dh = (dy[...].astype(F32) + grad_h).astype(BF)
    copies[0].wait()
    outs = []

    def flush(src, dst):
        c = pltpu.make_async_copy(src, dst, osems.at[len(outs)])
        c.start()
        outs.append(c)

    step = q_dim // 4
    for i in range(4):
        dctx[i * step:(i + 1) * step] = nt(wo[i * step:(i + 1) * step], dh).astype(BF)
    for i in range(4):
        part = slice(i * step, (i + 1) * step)
        oo[part] = nn(ctx[part], dh).astype(BF).astype(F32)
        flush(oo.at[part], go.at[part])
    every = slice(0, tokens)
    normed = nb[...]
    for g in range(kv_heads):
        kv = slice(g * dim, (g + 1) * dim)
        kg = qkv[q_dim + g * dim:q_dim + (g + 1) * dim]
        vg = qkv[q_dim + kv_dim + g * dim:q_dim + kv_dim + (g + 1) * dim]
        qg = heads_to_lanes(qkv, g, reps, dim, every)
        dg = heads_to_lanes(dctx, g, reps, dim, every)
        probs = probs_of(tn(kg, qg) * dim ** -0.5)
        dprobs = tn(vg, dg).astype(BF).astype(F32)
        weighted = probs * dprobs
        dscores = ((weighted - probs * jnp.sum(weighted, axis=0, keepdims=True)) * dim ** -0.5).astype(BF)
        dv[kv] = nt(dg, probs.astype(BF)).astype(BF)
        dk[kv] = nt(qg, dscores).astype(BF)
        dqg = nn(kg, dscores).astype(BF)
        for r in range(reps):
            dq[(g * reps + r) * dim:(g * reps + r + 1) * dim] = dqg[:, r * tokens:(r + 1) * tokens]
        if g % 2 == 1:
            part = slice((g - 1) * reps * dim, (g + 1) * reps * dim)
            oq[part] = nn(dq[part], normed).astype(BF).astype(F32)
            flush(oq.at[part], gq.at[part])
    ok[...] = nn(dk[...], normed).astype(BF).astype(F32)
    flush(ok, gk)
    ov[...] = nn(dv[...], normed).astype(BF).astype(F32)
    flush(ov, gv)
    for c in copies[1:]:
        c.wait()
    dn = (tn(dq[...], wq[...]) + tn(dk[...], wk[...]) + tn(dv[...], wv[...])).astype(BF).astype(F32)
    grad_x, g1 = rms_pull(x_b[...].astype(F32), row_of(n1), dn)
    gn1[...] = g1
    dx[...] = (dh.astype(F32) + grad_x).astype(BF)
    for c in outs:
        c.wait()


def attn_bwd(du, dy, h_b, x_b, nb, qkv, ctx, n1, n2, wo, wq, wk, wv, kv_heads, reps, dim):
    tokens, model = x_b.shape
    q_dim, kv_dim = kv_heads * reps * dim, kv_heads * dim
    vm = pl.BlockSpec(memory_space=pltpu.VMEM)
    hb = pl.BlockSpec(memory_space=pl.ANY)
    n_out = 4 + kv_heads // 2 + 2
    return pl.pallas_call(
        functools.partial(attn_bwd_kernel, kv_heads, reps, dim),
        out_shape=(
            jax.ShapeDtypeStruct((tokens, model), BF), jax.ShapeDtypeStruct((q_dim, model), F32), jax.ShapeDtypeStruct((kv_dim, model), F32),
            jax.ShapeDtypeStruct((kv_dim, model), F32), jax.ShapeDtypeStruct((q_dim, model), F32), jax.ShapeDtypeStruct((1, model), F32), jax.ShapeDtypeStruct((1, model), F32),
        ),
        in_specs=[vm] * 9 + [hb] * 4,
        out_specs=(vm, hb, hb, hb, hb, vm, vm),
        scratch_shapes=[
            pltpu.VMEM((q_dim, model), BF), pltpu.VMEM((q_dim, model), BF), pltpu.VMEM((kv_dim, model), BF), pltpu.VMEM((kv_dim, model), BF),
            pltpu.VMEM((q_dim, model), F32), pltpu.VMEM((kv_dim, model), F32), pltpu.VMEM((kv_dim, model), F32), pltpu.VMEM((q_dim, model), F32),
            pltpu.VMEM((q_dim, tokens), BF), pltpu.VMEM((q_dim, tokens), BF), pltpu.VMEM((kv_dim, tokens), BF), pltpu.VMEM((kv_dim, tokens), BF),
            pltpu.SemaphoreType.DMA((4,)), pltpu.SemaphoreType.DMA((n_out,)),
        ],
        compiler_params=pltpu.CompilerParams(vmem_limit_bytes=VMEM_BYTES),
        cost_estimate=pl.CostEstimate(flops=14 * 10 ** 9, bytes_accessed=40 * 10 ** 6, transcendentals=0),
        name="attn_bwd",
    )(du, dy, h_b, x_b, nb, qkv, ctx, n1, n2, wo, wq, wk, wv)


def route_rows(info, base, expert):
    group, _, width = info.shape
    tokens = width // 3
    top_k = info.shape[1] // 2
    wide = [info[r].astype(F32)[base * top_k:(base + 1) * top_k] for r in range(group)]

    def field(i):
        return jnp.concatenate([w[:, i * tokens:(i + 1) * tokens] for w in wide], axis=1)

    eid, slot, gate = field(0), field(1), field(2)
    hit = (eid == expert.astype(F32)) & (slot >= 0.0)
    slot_row = jnp.sum(jnp.where(hit, slot + 1.0, 0.0), axis=0, keepdims=True) - 1.0
    gate_row = jnp.sum(jnp.where(hit, gate, 0.0), axis=0, keepdims=True)
    return slot_row, gate_row


def ring_copies(pairs, sem, idx, ring):
    s = lax.rem(idx, ring)
    return [pltpu.make_async_copy(src.at[idx], dst.at[s], sem.at[s, i]) for i, (src, dst) in enumerate(pairs)]


def row_copies(refs, rows, sem):
    tokens = rows.shape[0] // len(refs)
    return [pltpu.make_async_copy(ref.at[0:tokens], rows.at[r * tokens:(r + 1) * tokens], sem.at[r]) for r, ref in enumerate(refs)]


def info_copy(load, info, sem):
    depth, width = info.shape
    first = load.shape[0] - depth
    return pltpu.make_async_copy(load.at[first:first + depth, 0:width], info, sem)


def hits(slot_row, tokens, capacity):
    source = lax.broadcasted_iota(jnp.int32, slot_row.shape, 1) // tokens
    col_row = jnp.where(slot_row >= 0.0, slot_row.astype(jnp.int32) + source * capacity, -1)
    return lax.broadcasted_iota(jnp.int32, (4 * capacity, slot_row.shape[1]), 0) == col_row


def start_all(copies):
    for c in copies:
        c.start()


def wait_all(copies):
    for c in copies:
        c.wait()


def keep_routes(slots, gates, q, slot_row, gate_row):
    slots[pl.ds(q, 1), :] = slot_row
    gates[pl.ds(q, 1), :] = gate_row


def stash(outs, q, capacity, lanes, res):
    for r in range(outs.shape[0]):
        outs[r, pl.ds(pl.multiple_of(q * BLOCK, BLOCK), capacity), lanes] = res[r * capacity:(r + 1) * capacity].astype(BF)


def mix_into(acc, outs, slots, gates, q, weighted):
    tokens = acc.shape[0] // outs.shape[0]
    depth = lax.broadcasted_iota(jnp.int32, (BLOCK, tokens), 0).astype(F32)
    for r in range(outs.shape[0]):
        lanes = slice(r * tokens, (r + 1) * tokens)
        blocks = []
        for k in range(QUAD):
            weight = gates[k:k + 1, lanes] if weighted else 1.0
            slot = jnp.where(q >= k, slots[k:k + 1, lanes], -1.0)
            blocks.append(jnp.where(depth == slot, weight, 0.0))
        pick = jnp.transpose(jnp.concatenate(blocks, axis=0).astype(BF))
        for n in range(acc.shape[1] // 512):
            part = slice(n * 512, (n + 1) * 512)
            acc[lanes, part] += nn(pick, outs[r, :, part])


def expert_bwd_kernel(capacity, loads, u_h, w1_h, w2_h, w3_h,
                      g1, g2, g3, p0, p1, p2, p3,
                      rows, info, us, w1s, w2s, w3s, slots, gates, du_all, d_out, hid, da1, da3, o1, o2, o3, acc, rsem, wsem, sems, psem):
    e = pl.program_id(0)
    count = pl.num_programs(0)
    me = lax.axis_index('expert')
    slot_e = lax.rem(e, 2)
    ring, _, model = us.shape
    tokens = rows.shape[0] // 4
    ff = w1s.shape[2]
    order = [jnp.bitwise_xor(me, r) for r in range(4)]
    arrivals = row_copies([loads.at[p] for p in order], rows, rsem) + [info_copy(loads.at[p], info.at[r], rsem.at[4 + r]) for r, p in enumerate(order)]
    pairs = ((u_h, us), (w1_h, w1s), (w3_h, w3s), (w2_h, w2s))

    @pl.when(e == 0)
    def _():
        start_all(arrivals + ring_copies(pairs, wsem, 0, ring) + ring_copies(pairs, wsem, 1, ring))
        acc[...] = jnp.zeros_like(acc)
        du_all[...] = jnp.zeros_like(du_all)
        wait_all(arrivals)

    @pl.when(e + 2 < count)
    def _():
        start_all(ring_copies(pairs, wsem, e + 2, ring))

    slot_row, gate_row = route_rows(info, 1, me * count + e)
    q = lax.rem(e, QUAD)
    keep_routes(slots, gates, q, slot_row, gate_row)
    hot = hits(slot_row, tokens, capacity)
    d_out[...] = nn(jnp.where(hot, gate_row, 0.0).astype(BF), rows[...]).astype(BF)

    def flush(idx):
        s = lax.rem(idx, 2)
        return [pltpu.make_async_copy(src.at[s], dst.at[idx], sems.at[s, i]) for i, (src, dst) in enumerate(((o1, g1), (o2, g2), (o3, g3)))]

    wait_all(ring_copies(pairs, wsem, e, ring))
    now = lax.rem(e, ring)
    u, w1, w2, w3 = us.at[now], w1s.at[now], w2s.at[now], w3s.at[now]
    uv = u[...]
    dov = d_out[...]
    for n in range(ff // 256):
        part = slice(n * 256, (n + 1) * 256)
        pre1 = nn(uv, w1[:, part]).astype(BF).astype(F32)
        pre3 = nn(uv, w3[:, part]).astype(BF).astype(F32)
        grad_hid = nt(dov, w2[part, :]).astype(BF).astype(F32)
        sigma = jax.nn.sigmoid(pre1)
        silu = pre1 * sigma
        hid[:, part] = (silu * pre3).astype(BF)
        da1[:, part] = (grad_hid * pre3 * sigma * (1.0 + pre1 * (1.0 - sigma))).astype(BF)
        da3[:, part] = (grad_hid * silu).astype(BF)

    @pl.when(e >= 2)
    def _():
        wait_all(flush(e - 2))

    fresh = flush(e)
    for m in range(ff // 256):
        part = slice(m * 256, (m + 1) * 256)
        o2[slot_e, part] = tn(hid[:, part], dov)
    fresh[1].start()
    for m in range(model // 256):
        part = slice(m * 256, (m + 1) * 256)
        o1[slot_e, part] = tn(u[:, part], da1[...])
        o3[slot_e, part] = tn(u[:, part], da3[...])
    fresh[0].start()
    fresh[2].start()
    for n in range(model // 256):
        part = slice(n * 256, (n + 1) * 256)
        stash(du_all, q, capacity, part, nt(da1[...], w1[part]) + nt(da3[...], w3[part]))

    @pl.when((q == QUAD - 1) | (e == count - 1))
    def _():
        mix_into(acc, du_all, slots, gates, q, False)

    @pl.when(e == count - 1)
    def _():
        sends = [pltpu.make_async_copy(acc.at[pl.ds(pl.multiple_of(p * tokens, tokens), tokens)], ref, psem.at[r]) for r, (p, ref) in enumerate(zip(order, (p0, p1, p2, p3)))]
        start_all(sends)
        wait_all(flush(e - 1))
        wait_all(flush(e))
        wait_all(sends)


def expert_bwd(loads, u, w1, w2, w3, tokens):
    model = loads.shape[2]
    count, cols, _ = u.shape
    ff = w1.shape[2]
    ring = 3
    hb = pl.BlockSpec(memory_space=pl.ANY)
    part = jax.ShapeDtypeStruct((tokens, model), F32)
    return pl.pallas_call(
        functools.partial(expert_bwd_kernel, cols // 4),
        grid=(count,),
        out_shape=(jax.ShapeDtypeStruct((count, model, ff), F32), jax.ShapeDtypeStruct((count, ff, model), F32), jax.ShapeDtypeStruct((count, model, ff), F32), part, part, part, part),
        in_specs=[hb] * 5,
        out_specs=(hb,) * 7,
        scratch_shapes=[
            pltpu.VMEM((4 * tokens, model), BF), pltpu.VMEM((4, loads.shape[1] - tokens, 3 * tokens), BF),
            pltpu.VMEM((ring, cols, model), BF), pltpu.VMEM((ring, model, ff), BF), pltpu.VMEM((ring, ff, model), BF), pltpu.VMEM((ring, model, ff), BF),
            pltpu.VMEM((8, 4 * tokens), F32), pltpu.VMEM((8, 4 * tokens), F32), pltpu.VMEM((4, QUAD * BLOCK, model), BF),
            pltpu.VMEM((cols, model), BF), pltpu.VMEM((cols, ff), BF), pltpu.VMEM((cols, ff), BF), pltpu.VMEM((cols, ff), BF),
            pltpu.VMEM((2, model, ff), F32), pltpu.VMEM((2, ff, model), F32), pltpu.VMEM((2, model, ff), F32),
            pltpu.VMEM((4 * tokens, model), F32),
            pltpu.SemaphoreType.DMA((8,)), pltpu.SemaphoreType.DMA((ring, 4)), pltpu.SemaphoreType.DMA((2, 3)), pltpu.SemaphoreType.DMA((4,)),
        ],
        compiler_params=pltpu.CompilerParams(vmem_limit_bytes=VMEM_BYTES, dimension_semantics=("arbitrary",)),
        cost_estimate=pl.CostEstimate(flops=50 * 10 ** 9, bytes_accessed=150 * 10 ** 6, transcendentals=0),
        name="expert_bwd",
    )(loads, u, w1, w2, w3)


def expert_fwd_kernel(capacity, u0, u1, u2, u3, loads, b0, b1, b2, b3, w1_h, w2_h, w3_h, du_o, mine_o, out_o,
                      rows, info, w1s, w2s, w3s, slots, gates, out_all, acc, loc0, loc2, rx1, rx3, rxf, ra1, ra3, rsem, wsem, bsem, ssem, xsem):
    e = pl.program_id(0)
    count = pl.num_programs(0)
    me = lax.axis_index('expert')
    near, far = neighbours()
    ring, model, ff = w1s.shape
    q = e % QUAD
    tokens = rows.shape[0] // 4
    arrivals = row_copies((u0, u1, u2, u3), rows, rsem) + [info_copy(loads.at[r], info.at[r], rsem.at[4 + r]) for r in range(4)]
    pairs = ((w1_h, w1s), (w3_h, w3s), (w2_h, w2s))
    local = [pltpu.make_async_copy(b0, loc0, bsem.at[0]), pltpu.make_async_copy(b2, loc2, bsem.at[1])]
    swap3 = remote(b3, rx3, ssem.at[0], xsem.at[0], near)
    swap1 = remote(b1, rx1, ssem.at[1], xsem.at[1], near)
    over = remote(loc2, rxf, ssem.at[2], xsem.at[2], far)
    part = [slice(r * tokens, (r + 1) * tokens) for r in range(4)]
    late3 = remote(acc.at[part[3]], ra3, ssem.at[3], xsem.at[3], near)
    late1 = remote(acc.at[part[1]], ra1, ssem.at[4], xsem.at[4], near)

    @pl.when(e == 0)
    def _():
        start_all(arrivals + ring_copies(pairs, wsem, 0, ring) + ring_copies(pairs, wsem, 1, ring) + local)
        greet((near, far))
        swap3.start()
        swap1.start()
        acc[...] = jnp.zeros_like(acc)
        out_all[...] = jnp.zeros_like(out_all)
        wait_all(arrivals)

    @pl.when(e == 3)
    def _():
        wait_all(local)
        swap3.wait()
        loc2[...] += rx3[...]
        over.start()

    @pl.when(e + 2 < count)
    def _():
        start_all(ring_copies(pairs, wsem, e + 2, ring))

    slot_row, gate_row = route_rows(info, 0, me * count + e)
    keep_routes(slots, gates, q, slot_row, gate_row)
    v = nn(jnp.where(hits(slot_row, tokens, capacity), 1.0, 0.0).astype(BF), rows[...]).astype(BF)
    wait_all(ring_copies(pairs, wsem, e, ring))
    now = e % ring
    w1, w2, w3 = w1s.at[now], w2s.at[now], w3s.at[now]
    pieces = []
    for n in range(ff // 256):
        lanes = slice(n * 256, (n + 1) * 256)
        a1 = nn(v, w1[:, lanes]).astype(BF).astype(F32)
        a3 = nn(v, w3[:, lanes]).astype(BF).astype(F32)
        pieces.append((a1 * jax.nn.sigmoid(a1) * a3).astype(BF))
    hidden = jnp.concatenate(pieces, axis=1)
    for n in range(model // 256):
        lanes = slice(n * 256, (n + 1) * 256)
        stash(out_all, q, capacity, lanes, nn(hidden, w2[:, lanes]))

    @pl.when((q == QUAD - 1) | (e == count - 1))
    def _():
        mix_into(acc, out_all, slots, gates, q, True)

    @pl.when(e == count - 1)
    def _():
        late3.start()
        late1.start()
        swap1.wait()
        over.wait()
        du_o[...] = ((loc0[...] + rx1[...]) + rxf[...]).astype(BF)
        late3.wait()
        out_o[...] = acc[part[2]] + ra3[...]
        late1.wait()
        mine_o[...] = acc[part[0]] + ra1[...]


def whole(shape):
    return pl.BlockSpec(shape, lambda e: (0,) * len(shape), pipeline_mode=pl.Buffered(1))


def expert_fwd(us, loads, sums, w1, w2, w3, capacity):
    tokens, model = us[0].shape
    count, _, ff = w1.shape
    ring = 3
    part = jax.ShapeDtypeStruct((tokens, model), F32)
    hb = pl.BlockSpec(memory_space=pl.ANY)
    tile = pltpu.VMEM((tokens, model), F32)
    return pl.pallas_call(
        functools.partial(expert_fwd_kernel, capacity),
        grid=(count,),
        out_shape=(jax.ShapeDtypeStruct((tokens, model), BF), part, part),
        in_specs=[hb] * 12,
        out_specs=(whole((tokens, model)),) * 3,
        scratch_shapes=[
            pltpu.VMEM((4 * tokens, model), BF), pltpu.VMEM((4, loads.shape[1] - tokens, 3 * tokens), BF),
            pltpu.VMEM((ring, model, ff), BF), pltpu.VMEM((ring, ff, model), BF), pltpu.VMEM((ring, model, ff), BF),
            pltpu.VMEM((8, 4 * tokens), F32), pltpu.VMEM((8, 4 * tokens), F32), pltpu.VMEM((4, QUAD * BLOCK, model), BF), pltpu.VMEM((4 * tokens, model), F32),
            tile, tile, tile, tile, tile, tile, tile,
            pltpu.SemaphoreType.DMA((8,)), pltpu.SemaphoreType.DMA((ring, 3)), pltpu.SemaphoreType.DMA((2,)), pltpu.SemaphoreType.DMA((5,)), pltpu.SemaphoreType.DMA((5,)),
        ],
        compiler_params=pltpu.CompilerParams(vmem_limit_bytes=VMEM_BYTES, dimension_semantics=("arbitrary",), collective_id=1, has_side_effects=True),
        cost_estimate=pl.CostEstimate(flops=16 * 10 ** 9, bytes_accessed=50 * 10 ** 6, transcendentals=0),
        name="expert_fwd",
    )(*us, loads, *sums, w1, w2, w3)


def solution(mesh):
    group = mesh.shape['expert']

    def hop(value, bits):
        return lax.ppermute(value, 'expert', [(i, i ^ bits) for i in range(group)])

    def local_step(x_a, x_b, dy_b, eid_a, slot_a, gate_a, eid_b, slot_b, gate_b, u_b, norm_1, norm_2, w_q, w_k, w_v, w_o, w_1, w_2, w_3):
        model, heads, dim = w_q.shape
        kv_heads = w_k.shape[1]
        reps = heads // kv_heads
        wq_t, wk_t, wv_t = (w.transpose(1, 2, 0).reshape(-1, model) for w in (w_q, w_k, w_v))
        wo = w_o.reshape(-1, model)
        fields = [a.T for a in (eid_a, slot_a, gate_a, eid_b, slot_b, gate_b)]
        h_a, u_a, h_b, nb, qkv_b, ctx_b, loads = attn_fwd(x_a, x_b, dy_b, fields, norm_1, norm_2, wq_t, wk_t, wv_t, wo, kv_heads, reps, dim)
        us = (u_a, hop(u_a, 1), hop(u_a, 2), hop(u_a, 3))
        g1, g2, g3, *sums = expert_bwd(loads, u_b, w_1, w_2, w_3, x_a.shape[0])
        du, mine_a, out_a = expert_fwd(us, loads, sums, w_1, w_2, w_3, u_b.shape[1] // group)
        far_a = hop(out_a, 2)
        dx_b, g_q, g_k, g_v, g_o, g_n1, g_n2 = attn_bwd(du, dy_b, h_b, x_b, nb, qkv_b, ctx_b, norm_1, norm_2, wo, wq_t, wk_t, wv_t, kv_heads, reps, dim)
        y_a = (h_a.astype(F32) + (mine_a + far_a)).astype(BF)
        g_q = g_q.reshape(heads, dim, model).transpose(2, 0, 1)
        g_k = g_k.reshape(kv_heads, dim, model).transpose(2, 0, 1)
        g_v = g_v.reshape(kv_heads, dim, model).transpose(2, 0, 1)
        g_o = g_o.reshape(heads, dim, model)
        return (y_a, dx_b, g1, g2, g3, g_q[None], g_k[None], g_v[None], g_o[None], g_n1, g_n2)

    row_spec = P(('data', 'expert'), None)
    cube_spec = P(('data', 'expert'), None, None)
    quad_spec = P(('data', 'expert'), None, None, None)
    expert_spec = P('expert', None, None)
    in_specs = (row_spec, row_spec, row_spec, row_spec, row_spec, row_spec, row_spec, row_spec, row_spec, cube_spec, P(), P(), P(), P(), P(), P(), expert_spec, expert_spec, expert_spec)
    out_specs = (row_spec, row_spec, cube_spec, cube_spec, cube_spec, quad_spec, quad_spec, quad_spec, quad_spec, row_spec, row_spec)
    return jax.shard_map(local_step, mesh=mesh, in_specs=in_specs, out_specs=out_specs, check_vma=False)
```

```python
import functools

import jax
import jax.numpy as jnp
from jax import lax
from jax.experimental import pallas as pl
from jax.experimental.pallas import tpu as pltpu
from jax.sharding import PartitionSpec as P


NORM_EPS = 1e-6
BF = jnp.bfloat16
F32 = jnp.float32
VMEM_BYTES = 67043328
QUAD = 4
BLOCK = 64


def nn(a, b):
    return lax.dot_general(a, b, (((1,), (0,)), ((), ())), preferred_element_type=F32)


def nt(a, b):
    return lax.dot_general(a, b, (((1,), (1,)), ((), ())), preferred_element_type=F32)


def tn(a, b):
    return lax.dot_general(a, b, (((0,), (0,)), ((), ())), preferred_element_type=F32)


def row_of(ref):
    return ref[...].astype(F32).reshape(1, ref.shape[0])


def rms_scale(wide):
    return lax.rsqrt(jnp.mean(wide * wide, axis=-1, keepdims=True) + NORM_EPS)


def rms_rows(values, gain):
    wide = values.astype(F32)
    return (wide * rms_scale(wide) * gain).astype(BF)


def rms_pull(wide, gain, cot):
    scale = rms_scale(wide)
    scaled = wide * scale
    grad_gain = jnp.sum(cot * scaled, axis=0, keepdims=True).astype(BF).astype(F32)
    inner = cot * gain
    pull = jnp.mean(inner * wide, axis=-1, keepdims=True)
    grad = scale * inner - scaled * (scale * scale * pull)
    return grad.astype(BF).astype(F32), grad_gain


def probs_of(scores_t):
    rows = lax.broadcasted_iota(jnp.int32, scores_t.shape, 0)
    cols = lax.broadcasted_iota(jnp.int32, scores_t.shape, 1) % scores_t.shape[0]
    masked = jnp.where(rows <= cols, scores_t, -1e30)
    top = jnp.max(masked, axis=0, keepdims=True)
    unnorm = jnp.exp(masked - top)
    return unnorm / jnp.sum(unnorm, axis=0, keepdims=True)


def heads_to_lanes(ref, group, reps, dim, lanes):
    return jnp.concatenate([ref[(group * reps + r) * dim:(group * reps + r + 1) * dim, lanes] for r in range(reps)], axis=1)


def neighbours():
    me = lax.axis_index('expert')
    return me + 1 - 2 * (me % 2), (me + 2) % 4


def greet(peers):
    barrier = pltpu.get_barrier_semaphore()
    for peer in peers:
        pl.semaphore_signal(barrier, inc=1, device_id={'expert': peer}, device_id_type=pl.DeviceIdType.MESH)
    pl.semaphore_wait(barrier, len(peers))


def remote(src, dst, send, recv, peer):
    return pltpu.make_async_remote_copy(src_ref=src, dst_ref=dst, send_sem=send, recv_sem=recv, device_id={'expert': peer}, device_id_type=pl.DeviceIdType.MESH)


def attn_fwd_kernel(kv_heads, reps, dim, xa_h, xb_h, dy_h, ea, sa, ga, eb, sb, gb, n1, n2, wq_h, wk_h, wv_h, wo_h,
                    ha_h, ua_h, hb_h, nb_h, qkv_h, ctx_h, load_h,
                    xs, wq, wk, wv, wo, nrm, nrm_t, q_t, k_t, v_t, ctx, q_b, ctx_b, hs, ua, mine, far_in, ints, gates, sems, osems, ssem, rsem, tsem):
    near, far = neighbours()
    tokens = xs.shape[0] // 2
    small = ((ea, ints.at[0]), (sa, ints.at[1]), (eb, ints.at[2]), (sb, ints.at[3]), (ga, gates.at[0]), (gb, gates.at[1]))
    tiny = [pltpu.make_async_copy(s, d, tsem.at[i]) for i, (s, d) in enumerate(small)]
    heads = kv_heads * reps
    first, second = slice(0, tokens), slice(tokens, 2 * tokens)
    half = heads * dim // 2
    moves = ((dy_h, mine.at[0:tokens]), (xa_h, xs.at[first]), (xb_h, xs.at[second]), (wk_h, wk), (wv_h, wv), (wq_h.at[0:half], wq.at[0:half]), (wq_h.at[half:], wq.at[half:]), (wo_h, wo))
    copies = [pltpu.make_async_copy(s, d, sems.at[i]) for i, (s, d) in enumerate(moves)]
    start_all(copies[0:1] + tiny + copies[1:])
    outs = []

    def flush(src, dst):
        c = pltpu.make_async_copy(src, dst, osems.at[len(outs)])
        c.start()
        outs.append(c)

    greet((near, far))
    wait_all(tiny)
    fields = [v.astype(F32) for v in (ints[0], ints[1], gates[0], ints[2], ints[3], gates[1])]
    both = jnp.concatenate([jnp.concatenate(fields[0:3], axis=1), jnp.concatenate(fields[3:6], axis=1)], axis=0)
    mine[tokens:] = jnp.concatenate([both, jnp.zeros((both.shape[0], mine.shape[1] - both.shape[1]), F32)], axis=1).astype(BF)
    copies[0].wait()
    to_far = remote(mine, far_in, ssem.at[0], rsem.at[0], far)
    to_near = remote(mine, load_h.at[1], ssem.at[1], rsem.at[1], near)
    relay = remote(far_in, load_h.at[3], ssem.at[2], rsem.at[2], near)
    to_far.start()
    to_near.start()
    flush(mine, load_h.at[0])

    wait_all(copies[1:3])
    nrm[...] = rms_rows(xs[...], row_of(n1))
    nrm_t[...] = jnp.transpose(nrm[...])
    flush(nrm.at[second], nb_h)
    copies[3].wait()
    k_t[...] = nn(wk[...], nrm_t[...]).astype(BF)
    copies[4].wait()
    v_t[...] = nn(wv[...], nrm_t[...]).astype(BF)
    for i in range(2):
        copies[5 + i].wait()
        part = slice(i * half, (i + 1) * half)
        q_t[part] = nn(wq[part], nrm_t[...]).astype(BF)
    q_b[0:heads * dim] = q_t[:, second]
    q_b[heads * dim:(heads + kv_heads) * dim] = k_t[:, second]
    q_b[(heads + kv_heads) * dim:] = v_t[:, second]
    flush(q_b, qkv_h)
    for lanes in (second, first):
        for g in range(kv_heads):
            kg = k_t[g * dim:(g + 1) * dim, lanes]
            vg = v_t[g * dim:(g + 1) * dim, lanes]
            qg = heads_to_lanes(q_t, g, reps, dim, lanes)
            probs = probs_of(tn(kg, qg) * dim ** -0.5).astype(BF)
            out = nn(vg, probs).astype(BF)
            for r in range(reps):
                ctx[(g * reps + r) * dim:(g * reps + r + 1) * dim, lanes] = out[:, r * tokens:(r + 1) * tokens]
    ctx_b[...] = ctx[:, second]
    flush(ctx_b, ctx_h)
    copies[7].wait()
    hs[...] = (xs[...].astype(F32) + tn(ctx[...], wo[...]).astype(BF).astype(F32)).astype(BF)
    to_far.wait_recv()
    relay.start()
    flush(far_in, load_h.at[2])
    flush(hs.at[first], ha_h)
    flush(hs.at[second], hb_h)
    ua[...] = rms_rows(hs[first], row_of(n2))
    flush(ua, ua_h)
    to_far.wait_send()
    to_near.wait()
    relay.wait()
    wait_all(outs)


def attn_fwd(x_a, x_b, dy, fields, n1, n2, wq, wk, wv, wo, kv_heads, reps, dim):
    tokens, model = x_a.shape
    q_dim, kv_dim = kv_heads * reps * dim, kv_heads * dim
    depth = 2 * fields[0].shape[0]
    vm = pl.BlockSpec(memory_space=pltpu.VMEM)
    hb = pl.BlockSpec(memory_space=pl.ANY)
    row = jax.ShapeDtypeStruct((tokens, model), BF)
    return pl.pallas_call(
        functools.partial(attn_fwd_kernel, kv_heads, reps, dim),
        out_shape=(row, row, row, row, jax.ShapeDtypeStruct((q_dim + 2 * kv_dim, tokens), BF), jax.ShapeDtypeStruct((q_dim, tokens), BF), jax.ShapeDtypeStruct((4, tokens + depth, model), BF)),
        in_specs=[hb] * 9 + [vm] * 2 + [hb] * 4,
        out_specs=(hb,) * 7,
        scratch_shapes=[
            pltpu.VMEM((2 * tokens, model), BF),
            pltpu.VMEM((q_dim, model), BF), pltpu.VMEM((kv_dim, model), BF), pltpu.VMEM((kv_dim, model), BF), pltpu.VMEM((q_dim, model), BF),
            pltpu.VMEM((2 * tokens, model), BF), pltpu.VMEM((model, 2 * tokens), BF),
            pltpu.VMEM((q_dim, 2 * tokens), BF), pltpu.VMEM((kv_dim, 2 * tokens), BF), pltpu.VMEM((kv_dim, 2 * tokens), BF), pltpu.VMEM((q_dim, 2 * tokens), BF),
            pltpu.VMEM((q_dim + 2 * kv_dim, tokens), BF), pltpu.VMEM((q_dim, tokens), BF), pltpu.VMEM((2 * tokens, model), BF), pltpu.VMEM((tokens, model), BF),
            pltpu.VMEM((tokens + depth, model), BF), pltpu.VMEM((tokens + depth, model), BF),
            pltpu.VMEM((4,) + fields[0].shape, jnp.int32), pltpu.VMEM((2,) + fields[2].shape, BF),
            pltpu.SemaphoreType.DMA((8,)), pltpu.SemaphoreType.DMA((8,)), pltpu.SemaphoreType.DMA((3,)), pltpu.SemaphoreType.DMA((3,)), pltpu.SemaphoreType.DMA((6,)),
        ],
        compiler_params=pltpu.CompilerParams(vmem_limit_bytes=VMEM_BYTES, collective_id=0, has_side_effects=True),
        cost_estimate=pl.CostEstimate(flops=10 ** 10, bytes_accessed=14 * 10 ** 6, transcendentals=0),
        name="attn_fwd",
    )(x_a, x_b, dy, *fields, n1, n2, wq, wk, wv, wo)


def attn_bwd_kernel(kv_heads, reps, dim, du_in, dy, h_b, x_b, nb, qkv, ctx, n1, n2, wo_h, wq_h, wk_h, wv_h,
                    dx, gq, gk, gv, go, gn1, gn2,
                    wo, wq, wk, wv, oq, ok, ov, oo, dctx, dq, dk, dv, sems, osems):
    copies = [pltpu.make_async_copy(s, d, sems.at[i]) for i, (s, d) in enumerate(((wo_h, wo), (wq_h, wq), (wk_h, wk), (wv_h, wv)))]
    for c in copies:
        c.start()
    tokens = x_b.shape[0]
    q_dim, kv_dim = kv_heads * reps * dim, kv_heads * dim
    du = du_in[...].astype(F32)
    grad_h, g2 = rms_pull(h_b[...].astype(F32), row_of(n2), du)
    gn2[...] = g2
    dh = (dy[...].astype(F32) + grad_h).astype(BF)
    copies[0].wait()
    outs = []

    def flush(src, dst):
        c = pltpu.make_async_copy(src, dst, osems.at[len(outs)])
        c.start()
        outs.append(c)

    step = q_dim // 4
    for i in range(4):
        dctx[i * step:(i + 1) * step] = nt(wo[i * step:(i + 1) * step], dh).astype(BF)
    for i in range(4):
        part = slice(i * step, (i + 1) * step)
        oo[part] = nn(ctx[part], dh).astype(BF).astype(F32)
        flush(oo.at[part], go.at[part])
    every = slice(0, tokens)
    normed = nb[...]
    for g in range(kv_heads):
        kv = slice(g * dim, (g + 1) * dim)
        kg = qkv[q_dim + g * dim:q_dim + (g + 1) * dim]
        vg = qkv[q_dim + kv_dim + g * dim:q_dim + kv_dim + (g + 1) * dim]
        qg = heads_to_lanes(qkv, g, reps, dim, every)
        dg = heads_to_lanes(dctx, g, reps, dim, every)
        probs = probs_of(tn(kg, qg) * dim ** -0.5)
        dprobs = tn(vg, dg).astype(BF).astype(F32)
        weighted = probs * dprobs
        dscores = ((weighted - probs * jnp.sum(weighted, axis=0, keepdims=True)) * dim ** -0.5).astype(BF)
        dv[kv] = nt(dg, probs.astype(BF)).astype(BF)
        dk[kv] = nt(qg, dscores).astype(BF)
        dqg = nn(kg, dscores).astype(BF)
        for r in range(reps):
            dq[(g * reps + r) * dim:(g * reps + r + 1) * dim] = dqg[:, r * tokens:(r + 1) * tokens]
        if g % 2 == 1:
            part = slice((g - 1) * reps * dim, (g + 1) * reps * dim)
            oq[part] = nn(dq[part], normed).astype(BF).astype(F32)
            flush(oq.at[part], gq.at[part])
    ok[...] = nn(dk[...], normed).astype(BF).astype(F32)
    flush(ok, gk)
    ov[...] = nn(dv[...], normed).astype(BF).astype(F32)
    flush(ov, gv)
    for c in copies[1:]:
        c.wait()
    dn = (tn(dq[...], wq[...]) + tn(dk[...], wk[...]) + tn(dv[...], wv[...])).astype(BF).astype(F32)
    grad_x, g1 = rms_pull(x_b[...].astype(F32), row_of(n1), dn)
    gn1[...] = g1
    dx[...] = (dh.astype(F32) + grad_x).astype(BF)
    for c in outs:
        c.wait()


def attn_bwd(du, dy, h_b, x_b, nb, qkv, ctx, n1, n2, wo, wq, wk, wv, kv_heads, reps, dim):
    tokens, model = x_b.shape
    q_dim, kv_dim = kv_heads * reps * dim, kv_heads * dim
    vm = pl.BlockSpec(memory_space=pltpu.VMEM)
    hb = pl.BlockSpec(memory_space=pl.ANY)
    n_out = 4 + kv_heads // 2 + 2
    return pl.pallas_call(
        functools.partial(attn_bwd_kernel, kv_heads, reps, dim),
        out_shape=(
            jax.ShapeDtypeStruct((tokens, model), BF), jax.ShapeDtypeStruct((q_dim, model), F32), jax.ShapeDtypeStruct((kv_dim, model), F32),
            jax.ShapeDtypeStruct((kv_dim, model), F32), jax.ShapeDtypeStruct((q_dim, model), F32), jax.ShapeDtypeStruct((1, model), F32), jax.ShapeDtypeStruct((1, model), F32),
        ),
        in_specs=[vm] * 9 + [hb] * 4,
        out_specs=(vm, hb, hb, hb, hb, vm, vm),
        scratch_shapes=[
            pltpu.VMEM((q_dim, model), BF), pltpu.VMEM((q_dim, model), BF), pltpu.VMEM((kv_dim, model), BF), pltpu.VMEM((kv_dim, model), BF),
            pltpu.VMEM((q_dim, model), F32), pltpu.VMEM((kv_dim, model), F32), pltpu.VMEM((kv_dim, model), F32), pltpu.VMEM((q_dim, model), F32),
            pltpu.VMEM((q_dim, tokens), BF), pltpu.VMEM((q_dim, tokens), BF), pltpu.VMEM((kv_dim, tokens), BF), pltpu.VMEM((kv_dim, tokens), BF),
            pltpu.SemaphoreType.DMA((4,)), pltpu.SemaphoreType.DMA((n_out,)),
        ],
        compiler_params=pltpu.CompilerParams(vmem_limit_bytes=60 * 1024 * 1024),
        cost_estimate=pl.CostEstimate(flops=14 * 10 ** 9, bytes_accessed=40 * 10 ** 6, transcendentals=0),
        name="attn_bwd",
    )(du, dy, h_b, x_b, nb, qkv, ctx, n1, n2, wo, wq, wk, wv)


def route_rows(info, base, expert):
    group, _, width = info.shape
    tokens = width // 3
    top_k = info.shape[1] // 2
    wide = [info[r].astype(F32)[base * top_k:(base + 1) * top_k] for r in range(group)]

    def field(i):
        return jnp.concatenate([w[:, i * tokens:(i + 1) * tokens] for w in wide], axis=1)

    eid, slot, gate = field(0), field(1), field(2)
    hit = (eid == expert.astype(F32)) & (slot >= 0.0)
    slot_row = jnp.sum(jnp.where(hit, slot + 1.0, 0.0), axis=0, keepdims=True) - 1.0
    gate_row = jnp.sum(jnp.where(hit, gate, 0.0), axis=0, keepdims=True)
    return slot_row, gate_row


def ring_copies(pairs, sem, idx, ring):
    s = lax.rem(idx, ring)
    return [pltpu.make_async_copy(src.at[idx], dst.at[s], sem.at[s, i]) for i, (src, dst) in enumerate(pairs)]


def row_copies(refs, rows, sem):
    tokens = rows.shape[0] // len(refs)
    return [pltpu.make_async_copy(ref.at[0:tokens], rows.at[r * tokens:(r + 1) * tokens], sem.at[r]) for r, ref in enumerate(refs)]


def info_copy(load, info, sem):
    depth, width = info.shape
    first = load.shape[0] - depth
    return pltpu.make_async_copy(load.at[first:first + depth, 0:width], info, sem)


def hits(slot_row, tokens, capacity):
    source = lax.broadcasted_iota(jnp.int32, slot_row.shape, 1) // tokens
    col_row = jnp.where(slot_row >= 0.0, slot_row.astype(jnp.int32) + source * capacity, -1)
    return lax.broadcasted_iota(jnp.int32, (4 * capacity, slot_row.shape[1]), 0) == col_row


def start_all(copies):
    for c in copies:
        c.start()


def wait_all(copies):
    for c in copies:
        c.wait()


def keep_routes(slots, gates, q, slot_row, gate_row):
    slots[pl.ds(q, 1), :] = slot_row
    gates[pl.ds(q, 1), :] = gate_row


def stash(outs, q, capacity, lanes, res):
    for r in range(outs.shape[0]):
        outs[r, pl.ds(pl.multiple_of(q * BLOCK, BLOCK), capacity), lanes] = res[r * capacity:(r + 1) * capacity].astype(BF)


def mix_into(acc, outs, slots, gates, q, weighted):
    tokens = acc.shape[0] // outs.shape[0]
    depth = lax.broadcasted_iota(jnp.int32, (BLOCK, tokens), 0).astype(F32)
    for r in range(outs.shape[0]):
        lanes = slice(r * tokens, (r + 1) * tokens)
        blocks = []
        for k in range(QUAD):
            weight = gates[k:k + 1, lanes] if weighted else 1.0
            slot = jnp.where(q >= k, slots[k:k + 1, lanes], -1.0)
            blocks.append(jnp.where(depth == slot, weight, 0.0))
        pick = jnp.transpose(jnp.concatenate(blocks, axis=0).astype(BF))
        for n in range(acc.shape[1] // 512):
            part = slice(n * 512, (n + 1) * 512)
            acc[lanes, part] += nn(pick, outs[r, :, part])


def expert_bwd_kernel(capacity, loads, u_h, w1_h, w2_h, w3_h,
                      g1, g2, g3, p0, p1, p2, p3,
                      rows, info, us, w1s, w2s, w3s, slots, gates, du_all, d_out, hid, da1, da3, o1, o2, o3, acc, rsem, wsem, sems, psem):
    e = pl.program_id(0)
    count = pl.num_programs(0)
    me = lax.axis_index('expert')
    slot_e = lax.rem(e, 2)
    ring, _, model = us.shape
    tokens = rows.shape[0] // 4
    ff = w1s.shape[2]
    order = [jnp.bitwise_xor(me, r) for r in range(4)]
    arrivals = row_copies([loads.at[p] for p in order], rows, rsem) + [info_copy(loads.at[p], info.at[r], rsem.at[4 + r]) for r, p in enumerate(order)]
    pairs = ((u_h, us), (w1_h, w1s), (w3_h, w3s), (w2_h, w2s))

    @pl.when(e == 0)
    def _():
        start_all(arrivals + ring_copies(pairs, wsem, 0, ring) + ring_copies(pairs, wsem, 1, ring))
        acc[...] = jnp.zeros_like(acc)
        du_all[...] = jnp.zeros_like(du_all)
        wait_all(arrivals)

    @pl.when(e + 2 < count)
    def _():
        start_all(ring_copies(pairs, wsem, e + 2, ring))

    slot_row, gate_row = route_rows(info, 1, me * count + e)
    q = lax.rem(e, QUAD)
    keep_routes(slots, gates, q, slot_row, gate_row)
    hot = hits(slot_row, tokens, capacity)
    d_out[...] = nn(jnp.where(hot, gate_row, 0.0).astype(BF), rows[...]).astype(BF)

    def flush(idx):
        s = lax.rem(idx, 2)
        return [pltpu.make_async_copy(src.at[s], dst.at[idx], sems.at[s, i]) for i, (src, dst) in enumerate(((o1, g1), (o2, g2), (o3, g3)))]

    wait_all(ring_copies(pairs, wsem, e, ring))
    now = lax.rem(e, ring)
    u, w1, w2, w3 = us.at[now], w1s.at[now], w2s.at[now], w3s.at[now]
    uv = u[...]
    dov = d_out[...]
    for n in range(ff // 256):
        part = slice(n * 256, (n + 1) * 256)
        pre1 = nn(uv, w1[:, part]).astype(BF).astype(F32)
        pre3 = nn(uv, w3[:, part]).astype(BF).astype(F32)
        grad_hid = nt(dov, w2[part, :]).astype(BF).astype(F32)
        sigma = jax.nn.sigmoid(pre1)
        silu = pre1 * sigma
        hid[:, part] = (silu * pre3).astype(BF)
        da1[:, part] = (grad_hid * pre3 * sigma * (1.0 + pre1 * (1.0 - sigma))).astype(BF)
        da3[:, part] = (grad_hid * silu).astype(BF)

    @pl.when(e >= 2)
    def _():
        wait_all(flush(e - 2))

    fresh = flush(e)
    for m in range(ff // 256):
        part = slice(m * 256, (m + 1) * 256)
        o2[slot_e, part] = tn(hid[:, part], dov)
    fresh[1].start()
    for m in range(model // 256):
        part = slice(m * 256, (m + 1) * 256)
        o1[slot_e, part] = tn(u[:, part], da1[...])
        o3[slot_e, part] = tn(u[:, part], da3[...])
    fresh[0].start()
    fresh[2].start()
    for n in range(model // 256):
        part = slice(n * 256, (n + 1) * 256)
        stash(du_all, q, capacity, part, nt(da1[...], w1[part]) + nt(da3[...], w3[part]))

    @pl.when((q == QUAD - 1) | (e == count - 1))
    def _():
        mix_into(acc, du_all, slots, gates, q, False)

    @pl.when(e == count - 1)
    def _():
        sends = [pltpu.make_async_copy(acc.at[pl.ds(pl.multiple_of(p * tokens, tokens), tokens)], ref, psem.at[r]) for r, (p, ref) in enumerate(zip(order, (p0, p1, p2, p3)))]
        start_all(sends)
        wait_all(flush(e - 1))
        wait_all(flush(e))
        wait_all(sends)


def expert_bwd(loads, u, w1, w2, w3, tokens):
    model = loads.shape[2]
    count, cols, _ = u.shape
    ff = w1.shape[2]
    ring = 3
    hb = pl.BlockSpec(memory_space=pl.ANY)
    part = jax.ShapeDtypeStruct((tokens, model), F32)
    return pl.pallas_call(
        functools.partial(expert_bwd_kernel, cols // 4),
        grid=(count,),
        out_shape=(jax.ShapeDtypeStruct((count, model, ff), F32), jax.ShapeDtypeStruct((count, ff, model), F32), jax.ShapeDtypeStruct((count, model, ff), F32), part, part, part, part),
        in_specs=[hb] * 5,
        out_specs=(hb,) * 7,
        scratch_shapes=[
            pltpu.VMEM((4 * tokens, model), BF), pltpu.VMEM((4, loads.shape[1] - tokens, 3 * tokens), BF),
            pltpu.VMEM((ring, cols, model), BF), pltpu.VMEM((ring, model, ff), BF), pltpu.VMEM((ring, ff, model), BF), pltpu.VMEM((ring, model, ff), BF),
            pltpu.VMEM((8, 4 * tokens), F32), pltpu.VMEM((8, 4 * tokens), F32), pltpu.VMEM((4, QUAD * BLOCK, model), BF),
            pltpu.VMEM((cols, model), BF), pltpu.VMEM((cols, ff), BF), pltpu.VMEM((cols, ff), BF), pltpu.VMEM((cols, ff), BF),
            pltpu.VMEM((2, model, ff), F32), pltpu.VMEM((2, ff, model), F32), pltpu.VMEM((2, model, ff), F32),
            pltpu.VMEM((4 * tokens, model), F32),
            pltpu.SemaphoreType.DMA((8,)), pltpu.SemaphoreType.DMA((ring, 4)), pltpu.SemaphoreType.DMA((2, 3)), pltpu.SemaphoreType.DMA((4,)),
        ],
        compiler_params=pltpu.CompilerParams(vmem_limit_bytes=VMEM_BYTES, dimension_semantics=("arbitrary",)),
        cost_estimate=pl.CostEstimate(flops=50 * 10 ** 9, bytes_accessed=150 * 10 ** 6, transcendentals=0),
        name="expert_bwd",
    )(loads, u, w1, w2, w3)


def expert_fwd_kernel(capacity, u0, u1, u2, u3, loads, b0, b1, b2, b3, w1_h, w2_h, w3_h, du_o, mine_o, out_o,
                      rows, info, w1s, w2s, w3s, slots, gates, out_all, acc, loc0, loc2, rx1, rx3, rxf, ra1, ra3, rsem, wsem, bsem, ssem, xsem):
    e = pl.program_id(0)
    count = pl.num_programs(0)
    me = lax.axis_index('expert')
    near, far = neighbours()
    ring, model, ff = w1s.shape
    q = e % QUAD
    tokens = rows.shape[0] // 4
    arrivals = row_copies((u0, u1, u2, u3), rows, rsem) + [info_copy(loads.at[r], info.at[r], rsem.at[4 + r]) for r in range(4)]
    pairs = ((w1_h, w1s), (w3_h, w3s), (w2_h, w2s))
    local = [pltpu.make_async_copy(b0, loc0, bsem.at[0]), pltpu.make_async_copy(b2, loc2, bsem.at[1])]
    swap3 = remote(b3, rx3, ssem.at[0], xsem.at[0], near)
    swap1 = remote(b1, rx1, ssem.at[1], xsem.at[1], near)
    over = remote(loc2, rxf, ssem.at[2], xsem.at[2], far)
    part = [slice(r * tokens, (r + 1) * tokens) for r in range(4)]
    late3 = remote(acc.at[part[3]], ra3, ssem.at[3], xsem.at[3], near)
    late1 = remote(acc.at[part[1]], ra1, ssem.at[4], xsem.at[4], near)

    @pl.when(e == 0)
    def _():
        start_all(arrivals + ring_copies(pairs, wsem, 0, ring) + ring_copies(pairs, wsem, 1, ring) + local)
        greet((near, far))
        swap3.start()
        acc[...] = jnp.zeros_like(acc)
        out_all[...] = jnp.zeros_like(out_all)
        wait_all(arrivals)

    @pl.when(e == 1)
    def _():
        wait_all(local)
        swap3.wait()
        loc2[...] += rx3[...]
        over.start()
        swap1.start()

    @pl.when(e + 2 < count)
    def _():
        start_all(ring_copies(pairs, wsem, e + 2, ring))

    slot_row, gate_row = route_rows(info, 0, me * count + e)
    keep_routes(slots, gates, q, slot_row, gate_row)
    v = nn(jnp.where(hits(slot_row, tokens, capacity), 1.0, 0.0).astype(BF), rows[...]).astype(BF)
    wait_all(ring_copies(pairs, wsem, e, ring))
    now = e % ring
    w1, w2, w3 = w1s.at[now], w2s.at[now], w3s.at[now]
    pieces = []
    for n in range(ff // 256):
        lanes = slice(n * 256, (n + 1) * 256)
        a1 = nn(v, w1[:, lanes]).astype(BF).astype(F32)
        a3 = nn(v, w3[:, lanes]).astype(BF).astype(F32)
        pieces.append((a1 * jax.nn.sigmoid(a1) * a3).astype(BF))
    hidden = jnp.concatenate(pieces, axis=1)
    for n in range(model // 256):
        lanes = slice(n * 256, (n + 1) * 256)
        stash(out_all, q, capacity, lanes, nn(hidden, w2[:, lanes]))

    @pl.when((q == QUAD - 1) | (e == count - 1))
    def _():
        mix_into(acc, out_all, slots, gates, q, True)

    @pl.when(e == count - 1)
    def _():
        late3.start()
        late1.start()
        swap1.wait()
        over.wait()
        du_o[...] = ((loc0[...] + rx1[...]) + rxf[...]).astype(BF)
        late3.wait()
        out_o[...] = acc[part[2]] + ra3[...]
        late1.wait()
        mine_o[...] = acc[part[0]] + ra1[...]


def whole(shape):
    return pl.BlockSpec(shape, lambda e: (0,) * len(shape), pipeline_mode=pl.Buffered(1))


def expert_fwd(us, loads, sums, w1, w2, w3, capacity):
    tokens, model = us[0].shape
    count, _, ff = w1.shape
    ring = 3
    part = jax.ShapeDtypeStruct((tokens, model), F32)
    hb = pl.BlockSpec(memory_space=pl.ANY)
    tile = pltpu.VMEM((tokens, model), F32)
    return pl.pallas_call(
        functools.partial(expert_fwd_kernel, capacity),
        grid=(count,),
        out_shape=(jax.ShapeDtypeStruct((tokens, model), BF), part, part),
        in_specs=[hb] * 12,
        out_specs=(whole((tokens, model)),) * 3,
        scratch_shapes=[
            pltpu.VMEM((4 * tokens, model), BF), pltpu.VMEM((4, loads.shape[1] - tokens, 3 * tokens), BF),
            pltpu.VMEM((ring, model, ff), BF), pltpu.VMEM((ring, ff, model), BF), pltpu.VMEM((ring, model, ff), BF),
            pltpu.VMEM((8, 4 * tokens), F32), pltpu.VMEM((8, 4 * tokens), F32), pltpu.VMEM((4, QUAD * BLOCK, model), BF), pltpu.VMEM((4 * tokens, model), F32),
            tile, tile, tile, tile, tile, tile, tile,
            pltpu.SemaphoreType.DMA((8,)), pltpu.SemaphoreType.DMA((ring, 3)), pltpu.SemaphoreType.DMA((2,)), pltpu.SemaphoreType.DMA((5,)), pltpu.SemaphoreType.DMA((5,)),
        ],
        compiler_params=pltpu.CompilerParams(vmem_limit_bytes=VMEM_BYTES, dimension_semantics=("arbitrary",), collective_id=1, has_side_effects=True),
        cost_estimate=pl.CostEstimate(flops=16 * 10 ** 9, bytes_accessed=50 * 10 ** 6, transcendentals=0),
        name="expert_fwd",
    )(*us, loads, *sums, w1, w2, w3)


def solution(mesh):
    group = mesh.shape['expert']

    def hop(value, bits):
        return lax.ppermute(value, 'expert', [(i, i ^ bits) for i in range(group)])

    def local_step(x_a, x_b, dy_b, eid_a, slot_a, gate_a, eid_b, slot_b, gate_b, u_b, norm_1, norm_2, w_q, w_k, w_v, w_o, w_1, w_2, w_3):
        model, heads, dim = w_q.shape
        kv_heads = w_k.shape[1]
        reps = heads // kv_heads
        wq_t, wk_t, wv_t = (w.transpose(1, 2, 0).reshape(-1, model) for w in (w_q, w_k, w_v))
        wo = w_o.reshape(-1, model)
        fields = [a.T for a in (eid_a, slot_a, gate_a, eid_b, slot_b, gate_b)]
        h_a, u_a, h_b, nb, qkv_b, ctx_b, loads = attn_fwd(x_a, x_b, dy_b, fields, norm_1, norm_2, wq_t, wk_t, wv_t, wo, kv_heads, reps, dim)
        us = (u_a, hop(u_a, 1), hop(u_a, 2), hop(u_a, 3))
        g1, g2, g3, *sums = expert_bwd(loads, u_b, w_1, w_2, w_3, x_a.shape[0])
        du, mine_a, out_a = expert_fwd(us, loads, sums, w_1, w_2, w_3, u_b.shape[1] // group)
        far_a = hop(out_a, 2)
        dx_b, g_q, g_k, g_v, g_o, g_n1, g_n2 = attn_bwd(du, dy_b, h_b, x_b, nb, qkv_b, ctx_b, norm_1, norm_2, wo, wq_t, wk_t, wv_t, kv_heads, reps, dim)
        y_a = (h_a.astype(F32) + (mine_a + far_a)).astype(BF)
        g_q = g_q.reshape(heads, dim, model).transpose(2, 0, 1)
        g_k = g_k.reshape(kv_heads, dim, model).transpose(2, 0, 1)
        g_v = g_v.reshape(kv_heads, dim, model).transpose(2, 0, 1)
        g_o = g_o.reshape(heads, dim, model)
        return (y_a, dx_b, g1, g2, g3, g_q[None], g_k[None], g_v[None], g_o[None], g_n1, g_n2)

    row_spec = P(('data', 'expert'), None)
    cube_spec = P(('data', 'expert'), None, None)
    quad_spec = P(('data', 'expert'), None, None, None)
    expert_spec = P('expert', None, None)
    in_specs = (row_spec, row_spec, row_spec, row_spec, row_spec, row_spec, row_spec, row_spec, row_spec, cube_spec, P(), P(), P(), P(), P(), P(), expert_spec, expert_spec, expert_spec)
    out_specs = (row_spec, row_spec, cube_spec, cube_spec, cube_spec, quad_spec, quad_spec, quad_spec, quad_spec, row_spec, row_spec)
    return jax.shard_map(local_step, mesh=mesh, in_specs=in_specs, out_specs=out_specs, check_vma=False)
```

```python
import functools

import jax
import jax.numpy as jnp
from jax import lax
from jax.experimental import pallas as pl
from jax.experimental.pallas import tpu as pltpu
from jax.sharding import PartitionSpec as P


NORM_EPS = 1e-6
BF = jnp.bfloat16
F32 = jnp.float32
VMEM_BYTES = 67043328
QUAD = 4
BLOCK = 64


def nn(a, b):
    return lax.dot_general(a, b, (((1,), (0,)), ((), ())), preferred_element_type=F32)


def nt(a, b):
    return lax.dot_general(a, b, (((1,), (1,)), ((), ())), preferred_element_type=F32)


def tn(a, b):
    return lax.dot_general(a, b, (((0,), (0,)), ((), ())), preferred_element_type=F32)


def row_of(ref):
    return ref[...].astype(F32).reshape(1, ref.shape[0])


def rms_scale(wide):
    return lax.rsqrt(jnp.mean(wide * wide, axis=-1, keepdims=True) + NORM_EPS)


def rms_rows(values, gain):
    wide = values.astype(F32)
    return (wide * rms_scale(wide) * gain).astype(BF)


def rms_pull(wide, gain, cot):
    scale = rms_scale(wide)
    scaled = wide * scale
    grad_gain = jnp.sum(cot * scaled, axis=0, keepdims=True).astype(BF).astype(F32)
    inner = cot * gain
    pull = jnp.mean(inner * wide, axis=-1, keepdims=True)
    grad = scale * inner - scaled * (scale * scale * pull)
    return grad.astype(BF).astype(F32), grad_gain


def probs_of(scores_t):
    rows = lax.broadcasted_iota(jnp.int32, scores_t.shape, 0)
    cols = lax.broadcasted_iota(jnp.int32, scores_t.shape, 1) % scores_t.shape[0]
    masked = jnp.where(rows <= cols, scores_t, -1e30)
    top = jnp.max(masked, axis=0, keepdims=True)
    unnorm = jnp.exp(masked - top)
    return unnorm / jnp.sum(unnorm, axis=0, keepdims=True)


def heads_to_lanes(ref, group, reps, dim, lanes):
    return jnp.concatenate([ref[(group * reps + r) * dim:(group * reps + r + 1) * dim, lanes] for r in range(reps)], axis=1)


def neighbours():
    me = lax.axis_index('expert')
    return me + 1 - 2 * (me % 2), (me + 2) % 4


def greet(peers):
    barrier = pltpu.get_barrier_semaphore()
    for peer in peers:
        pl.semaphore_signal(barrier, inc=1, device_id={'expert': peer}, device_id_type=pl.DeviceIdType.MESH)
    pl.semaphore_wait(barrier, len(peers))


def remote(src, dst, send, recv, peer):
    return pltpu.make_async_remote_copy(src_ref=src, dst_ref=dst, send_sem=send, recv_sem=recv, device_id={'expert': peer}, device_id_type=pl.DeviceIdType.MESH)


def attn_fwd_kernel(kv_heads, reps, dim, xa_h, xb_h, dy_h, ea, sa, ga, eb, sb, gb, n1, n2, wq_h, wk_h, wv_h, wo_h,
                    ha_h, ua_h, hb_h, nb_h, qkv_h, ctx_h, load_h,
                    xs, wq, wk, wv, wo, nrm, nrm_t, q_t, k_t, v_t, ctx, q_b, ctx_b, hs, ua, mine, far_in, ints, gates, sems, osems, ssem, rsem, tsem):
    near, far = neighbours()
    tokens = xs.shape[0] // 2
    small = ((ea, ints.at[0]), (sa, ints.at[1]), (eb, ints.at[2]), (sb, ints.at[3]), (ga, gates.at[0]), (gb, gates.at[1]))
    tiny = [pltpu.make_async_copy(s, d, tsem.at[i]) for i, (s, d) in enumerate(small)]
    heads = kv_heads * reps
    first, second = slice(0, tokens), slice(tokens, 2 * tokens)
    half = heads * dim // 2
    moves = ((dy_h, mine.at[0:tokens]), (xa_h, xs.at[first]), (xb_h, xs.at[second]), (wk_h, wk), (wv_h, wv), (wq_h.at[0:half], wq.at[0:half]), (wq_h.at[half:], wq.at[half:]), (wo_h, wo))
    copies = [pltpu.make_async_copy(s, d, sems.at[i]) for i, (s, d) in enumerate(moves)]
    start_all(copies[0:1] + tiny + copies[1:3])
    start_all(copies[3:], 1)
    outs = []

    def flush(src, dst):
        c = pltpu.make_async_copy(src, dst, osems.at[len(outs)])
        c.start()
        outs.append(c)

    greet((near, far))
    wait_all(tiny)
    fields = [v.astype(F32) for v in (ints[0], ints[1], gates[0], ints[2], ints[3], gates[1])]
    both = jnp.concatenate([jnp.concatenate(fields[0:3], axis=1), jnp.concatenate(fields[3:6], axis=1)], axis=0)
    mine[tokens:] = jnp.concatenate([both, jnp.zeros((both.shape[0], mine.shape[1] - both.shape[1]), F32)], axis=1).astype(BF)
    copies[0].wait()
    to_far = remote(mine, far_in, ssem.at[0], rsem.at[0], far)
    to_near = remote(mine, load_h.at[1], ssem.at[1], rsem.at[1], near)
    relay = remote(far_in, load_h.at[3], ssem.at[2], rsem.at[2], near)
    to_far.start()
    to_near.start()
    flush(mine, load_h.at[0])

    wait_all(copies[1:3])
    nrm[...] = rms_rows(xs[...], row_of(n1))
    nrm_t[...] = jnp.transpose(nrm[...])
    flush(nrm.at[second], nb_h)
    copies[3].wait()
    k_t[...] = nn(wk[...], nrm_t[...]).astype(BF)
    copies[4].wait()
    v_t[...] = nn(wv[...], nrm_t[...]).astype(BF)
    for i in range(2):
        copies[5 + i].wait()
        part = slice(i * half, (i + 1) * half)
        q_t[part] = nn(wq[part], nrm_t[...]).astype(BF)
    q_b[0:heads * dim] = q_t[:, second]
    q_b[heads * dim:(heads + kv_heads) * dim] = k_t[:, second]
    q_b[(heads + kv_heads) * dim:] = v_t[:, second]
    flush(q_b, qkv_h)
    for lanes in (second, first):
        for g in range(kv_heads):
            kg = k_t[g * dim:(g + 1) * dim, lanes]
            vg = v_t[g * dim:(g + 1) * dim, lanes]
            qg = heads_to_lanes(q_t, g, reps, dim, lanes)
            probs = probs_of(tn(kg, qg) * dim ** -0.5).astype(BF)
            out = nn(vg, probs).astype(BF)
            for r in range(reps):
                ctx[(g * reps + r) * dim:(g * reps + r + 1) * dim, lanes] = out[:, r * tokens:(r + 1) * tokens]
    ctx_b[...] = ctx[:, second]
    flush(ctx_b, ctx_h)
    copies[7].wait()
    hs[...] = (xs[...].astype(F32) + tn(ctx[...], wo[...]).astype(BF).astype(F32)).astype(BF)
    to_far.wait_recv()
    relay.start()
    flush(far_in, load_h.at[2])
    flush(hs.at[first], ha_h)
    flush(hs.at[second], hb_h)
    ua[...] = rms_rows(hs[first], row_of(n2))
    flush(ua, ua_h)
    to_far.wait_send()
    to_near.wait()
    relay.wait()
    wait_all(outs)


def attn_fwd(x_a, x_b, dy, fields, n1, n2, wq, wk, wv, wo, kv_heads, reps, dim):
    tokens, model = x_a.shape
    q_dim, kv_dim = kv_heads * reps * dim, kv_heads * dim
    depth = 2 * fields[0].shape[0]
    vm = pl.BlockSpec(memory_space=pltpu.VMEM)
    hb = pl.BlockSpec(memory_space=pl.ANY)
    row = jax.ShapeDtypeStruct((tokens, model), BF)
    return pl.pallas_call(
        functools.partial(attn_fwd_kernel, kv_heads, reps, dim),
        out_shape=(row, row, row, row, jax.ShapeDtypeStruct((q_dim + 2 * kv_dim, tokens), BF), jax.ShapeDtypeStruct((q_dim, tokens), BF), jax.ShapeDtypeStruct((4, tokens + depth, model), BF)),
        in_specs=[hb] * 9 + [vm] * 2 + [hb] * 4,
        out_specs=(hb,) * 7,
        scratch_shapes=[
            pltpu.VMEM((2 * tokens, model), BF),
            pltpu.VMEM((q_dim, model), BF), pltpu.VMEM((kv_dim, model), BF), pltpu.VMEM((kv_dim, model), BF), pltpu.VMEM((q_dim, model), BF),
            pltpu.VMEM((2 * tokens, model), BF), pltpu.VMEM((model, 2 * tokens), BF),
            pltpu.VMEM((q_dim, 2 * tokens), BF), pltpu.VMEM((kv_dim, 2 * tokens), BF), pltpu.VMEM((kv_dim, 2 * tokens), BF), pltpu.VMEM((q_dim, 2 * tokens), BF),
            pltpu.VMEM((q_dim + 2 * kv_dim, tokens), BF), pltpu.VMEM((q_dim, tokens), BF), pltpu.VMEM((2 * tokens, model), BF), pltpu.VMEM((tokens, model), BF),
            pltpu.VMEM((tokens + depth, model), BF), pltpu.VMEM((tokens + depth, model), BF),
            pltpu.VMEM((4,) + fields[0].shape, jnp.int32), pltpu.VMEM((2,) + fields[2].shape, BF),
            pltpu.SemaphoreType.DMA((8,)), pltpu.SemaphoreType.DMA((8,)), pltpu.SemaphoreType.DMA((3,)), pltpu.SemaphoreType.DMA((3,)), pltpu.SemaphoreType.DMA((6,)),
        ],
        compiler_params=pltpu.CompilerParams(vmem_limit_bytes=VMEM_BYTES, collective_id=0, has_side_effects=True),
        cost_estimate=pl.CostEstimate(flops=10 ** 10, bytes_accessed=14 * 10 ** 6, transcendentals=0),
        name="attn_fwd",
    )(x_a, x_b, dy, *fields, n1, n2, wq, wk, wv, wo)


def attn_bwd_kernel(kv_heads, reps, dim, du_in, dy, h_b, x_b, nb, qkv, ctx, n1, n2, wo_h, wq_h, wk_h, wv_h,
                    dx, gq, gk, gv, go, gn1, gn2,
                    wo, wq, wk, wv, oq, ok, ov, oo, dctx, dq, dk, dv, sems, osems):
    copies = [pltpu.make_async_copy(s, d, sems.at[i]) for i, (s, d) in enumerate(((wo_h, wo), (wq_h, wq), (wk_h, wk), (wv_h, wv)))]
    for c in copies:
        c.start()
    tokens = x_b.shape[0]
    q_dim, kv_dim = kv_heads * reps * dim, kv_heads * dim
    du = du_in[...].astype(F32)
    grad_h, g2 = rms_pull(h_b[...].astype(F32), row_of(n2), du)
    gn2[...] = g2
    dh = (dy[...].astype(F32) + grad_h).astype(BF)
    copies[0].wait()
    outs = []

    def flush(src, dst):
        c = pltpu.make_async_copy(src, dst, osems.at[len(outs)])
        c.start()
        outs.append(c)

    step = q_dim // 4
    for i in range(4):
        dctx[i * step:(i + 1) * step] = nt(wo[i * step:(i + 1) * step], dh).astype(BF)
    for i in range(4):
        part = slice(i * step, (i + 1) * step)
        oo[part] = nn(ctx[part], dh).astype(BF).astype(F32)
        flush(oo.at[part], go.at[part])
    every = slice(0, tokens)
    normed = nb[...]
    for g in range(kv_heads):
        kv = slice(g * dim, (g + 1) * dim)
        kg = qkv[q_dim + g * dim:q_dim + (g + 1) * dim]
        vg = qkv[q_dim + kv_dim + g * dim:q_dim + kv_dim + (g + 1) * dim]
        qg = heads_to_lanes(qkv, g, reps, dim, every)
        dg = heads_to_lanes(dctx, g, reps, dim, every)
        probs = probs_of(tn(kg, qg) * dim ** -0.5)
        dprobs = tn(vg, dg).astype(BF).astype(F32)
        weighted = probs * dprobs
        dscores = ((weighted - probs * jnp.sum(weighted, axis=0, keepdims=True)) * dim ** -0.5).astype(BF)
        dv[kv] = nt(dg, probs.astype(BF)).astype(BF)
        dk[kv] = nt(qg, dscores).astype(BF)
        dqg = nn(kg, dscores).astype(BF)
        for r in range(reps):
            dq[(g * reps + r) * dim:(g * reps + r + 1) * dim] = dqg[:, r * tokens:(r + 1) * tokens]
        if g % 2 == 1:
            part = slice((g - 1) * reps * dim, (g + 1) * reps * dim)
            oq[part] = nn(dq[part], normed).astype(BF).astype(F32)
            flush(oq.at[part], gq.at[part])
    ok[...] = nn(dk[...], normed).astype(BF).astype(F32)
    flush(ok, gk)
    ov[...] = nn(dv[...], normed).astype(BF).astype(F32)
    flush(ov, gv)
    for c in copies[1:]:
        c.wait()
    dn = (tn(dq[...], wq[...]) + tn(dk[...], wk[...]) + tn(dv[...], wv[...])).astype(BF).astype(F32)
    grad_x, g1 = rms_pull(x_b[...].astype(F32), row_of(n1), dn)
    gn1[...] = g1
    dx[...] = (dh.astype(F32) + grad_x).astype(BF)
    for c in outs:
        c.wait()


def attn_bwd(du, dy, h_b, x_b, nb, qkv, ctx, n1, n2, wo, wq, wk, wv, kv_heads, reps, dim):
    tokens, model = x_b.shape
    q_dim, kv_dim = kv_heads * reps * dim, kv_heads * dim
    vm = pl.BlockSpec(memory_space=pltpu.VMEM)
    hb = pl.BlockSpec(memory_space=pl.ANY)
    n_out = 4 + kv_heads // 2 + 2
    return pl.pallas_call(
        functools.partial(attn_bwd_kernel, kv_heads, reps, dim),
        out_shape=(
            jax.ShapeDtypeStruct((tokens, model), BF), jax.ShapeDtypeStruct((q_dim, model), F32), jax.ShapeDtypeStruct((kv_dim, model), F32),
            jax.ShapeDtypeStruct((kv_dim, model), F32), jax.ShapeDtypeStruct((q_dim, model), F32), jax.ShapeDtypeStruct((1, model), F32), jax.ShapeDtypeStruct((1, model), F32),
        ),
        in_specs=[vm] * 9 + [hb] * 4,
        out_specs=(vm, hb, hb, hb, hb, vm, vm),
        scratch_shapes=[
            pltpu.VMEM((q_dim, model), BF), pltpu.VMEM((q_dim, model), BF), pltpu.VMEM((kv_dim, model), BF), pltpu.VMEM((kv_dim, model), BF),
            pltpu.VMEM((q_dim, model), F32), pltpu.VMEM((kv_dim, model), F32), pltpu.VMEM((kv_dim, model), F32), pltpu.VMEM((q_dim, model), F32),
            pltpu.VMEM((q_dim, tokens), BF), pltpu.VMEM((q_dim, tokens), BF), pltpu.VMEM((kv_dim, tokens), BF), pltpu.VMEM((kv_dim, tokens), BF),
            pltpu.SemaphoreType.DMA((4,)), pltpu.SemaphoreType.DMA((n_out,)),
        ],
        compiler_params=pltpu.CompilerParams(vmem_limit_bytes=60 * 1024 * 1024),
        cost_estimate=pl.CostEstimate(flops=14 * 10 ** 9, bytes_accessed=40 * 10 ** 6, transcendentals=0),
        name="attn_bwd",
    )(du, dy, h_b, x_b, nb, qkv, ctx, n1, n2, wo, wq, wk, wv)


def route_rows(info, base, expert):
    group, _, width = info.shape
    tokens = width // 3
    top_k = info.shape[1] // 2
    wide = [info[r].astype(F32)[base * top_k:(base + 1) * top_k] for r in range(group)]

    def field(i):
        return jnp.concatenate([w[:, i * tokens:(i + 1) * tokens] for w in wide], axis=1)

    eid, slot, gate = field(0), field(1), field(2)
    hit = (eid == expert.astype(F32)) & (slot >= 0.0)
    slot_row = jnp.sum(jnp.where(hit, slot + 1.0, 0.0), axis=0, keepdims=True) - 1.0
    gate_row = jnp.sum(jnp.where(hit, gate, 0.0), axis=0, keepdims=True)
    return slot_row, gate_row


def ring_copies(pairs, sem, idx, ring):
    s = lax.rem(idx, ring)
    return [pltpu.make_async_copy(src.at[idx], dst.at[s], sem.at[s, i]) for i, (src, dst) in enumerate(pairs)]


def row_copies(refs, rows, sem):
    tokens = rows.shape[0] // len(refs)
    return [pltpu.make_async_copy(ref.at[0:tokens], rows.at[r * tokens:(r + 1) * tokens], sem.at[r]) for r, ref in enumerate(refs)]


def info_copy(load, info, sem):
    depth, width = info.shape
    first = load.shape[0] - depth
    return pltpu.make_async_copy(load.at[first:first + depth, 0:width], info, sem)


def hits(slot_row, tokens, capacity):
    source = lax.broadcasted_iota(jnp.int32, slot_row.shape, 1) // tokens
    col_row = jnp.where(slot_row >= 0.0, slot_row.astype(jnp.int32) + source * capacity, -1)
    return lax.broadcasted_iota(jnp.int32, (4 * capacity, slot_row.shape[1]), 0) == col_row


def start_all(copies, priority=0):
    for c in copies:
        c.start(priority=priority)


def wait_all(copies):
    for c in copies:
        c.wait()


def keep_routes(slots, gates, q, slot_row, gate_row):
    slots[pl.ds(q, 1), :] = slot_row
    gates[pl.ds(q, 1), :] = gate_row


def stash(outs, q, capacity, lanes, res):
    for r in range(outs.shape[0]):
        outs[r, pl.ds(pl.multiple_of(q * BLOCK, BLOCK), capacity), lanes] = res[r * capacity:(r + 1) * capacity].astype(BF)


def mix_into(acc, outs, slots, gates, q, weighted):
    tokens = acc.shape[0] // outs.shape[0]
    depth = lax.broadcasted_iota(jnp.int32, (BLOCK, tokens), 0).astype(F32)
    for r in range(outs.shape[0]):
        lanes = slice(r * tokens, (r + 1) * tokens)
        blocks = []
        for k in range(QUAD):
            weight = gates[k:k + 1, lanes] if weighted else 1.0
            slot = jnp.where(q >= k, slots[k:k + 1, lanes], -1.0)
            blocks.append(jnp.where(depth == slot, weight, 0.0))
        pick = jnp.transpose(jnp.concatenate(blocks, axis=0).astype(BF))
        for n in range(acc.shape[1] // 512):
            part = slice(n * 512, (n + 1) * 512)
            acc[lanes, part] += nn(pick, outs[r, :, part])


def expert_bwd_kernel(capacity, loads, u_h, w1_h, w2_h, w3_h,
                      g1, g2, g3, p0, p1, p2, p3,
                      rows, info, us, w1s, w2s, w3s, slots, gates, du_all, d_out, hid, da1, da3, o1, o2, o3, acc, rsem, wsem, sems, psem):
    e = pl.program_id(0)
    count = pl.num_programs(0)
    me = lax.axis_index('expert')
    slot_e = lax.rem(e, 2)
    ring, _, model = us.shape
    tokens = rows.shape[0] // 4
    ff = w1s.shape[2]
    order = [jnp.bitwise_xor(me, r) for r in range(4)]
    arrivals = row_copies([loads.at[p] for p in order], rows, rsem) + [info_copy(loads.at[p], info.at[r], rsem.at[4 + r]) for r, p in enumerate(order)]
    pairs = ((u_h, us), (w1_h, w1s), (w3_h, w3s), (w2_h, w2s))

    @pl.when(e == 0)
    def _():
        start_all(arrivals + ring_copies(pairs, wsem, 0, ring) + ring_copies(pairs, wsem, 1, ring))
        acc[...] = jnp.zeros_like(acc)
        du_all[...] = jnp.zeros_like(du_all)
        wait_all(arrivals)

    @pl.when(e + 2 < count)
    def _():
        start_all(ring_copies(pairs, wsem, e + 2, ring))

    slot_row, gate_row = route_rows(info, 1, me * count + e)
    q = lax.rem(e, QUAD)
    keep_routes(slots, gates, q, slot_row, gate_row)
    hot = hits(slot_row, tokens, capacity)
    d_out[...] = nn(jnp.where(hot, gate_row, 0.0).astype(BF), rows[...]).astype(BF)

    def flush(idx):
        s = lax.rem(idx, 2)
        return [pltpu.make_async_copy(src.at[s], dst.at[idx], sems.at[s, i]) for i, (src, dst) in enumerate(((o1, g1), (o2, g2), (o3, g3)))]

    wait_all(ring_copies(pairs, wsem, e, ring))
    now = lax.rem(e, ring)
    u, w1, w2, w3 = us.at[now], w1s.at[now], w2s.at[now], w3s.at[now]
    uv = u[...]
    dov = d_out[...]
    for n in range(ff // 256):
        part = slice(n * 256, (n + 1) * 256)
        pre1 = nn(uv, w1[:, part]).astype(BF).astype(F32)
        pre3 = nn(uv, w3[:, part]).astype(BF).astype(F32)
        grad_hid = nt(dov, w2[part, :]).astype(BF).astype(F32)
        sigma = jax.nn.sigmoid(pre1)
        silu = pre1 * sigma
        hid[:, part] = (silu * pre3).astype(BF)
        da1[:, part] = (grad_hid * pre3 * sigma * (1.0 + pre1 * (1.0 - sigma))).astype(BF)
        da3[:, part] = (grad_hid * silu).astype(BF)

    @pl.when(e >= 2)
    def _():
        wait_all(flush(e - 2))

    fresh = flush(e)
    for m in range(ff // 256):
        part = slice(m * 256, (m + 1) * 256)
        o2[slot_e, part] = tn(hid[:, part], dov)
    fresh[1].start()
    for m in range(model // 256):
        part = slice(m * 256, (m + 1) * 256)
        o1[slot_e, part] = tn(u[:, part], da1[...])
        o3[slot_e, part] = tn(u[:, part], da3[...])
    fresh[0].start()
    fresh[2].start()
    for n in range(model // 256):
        part = slice(n * 256, (n + 1) * 256)
        stash(du_all, q, capacity, part, nt(da1[...], w1[part]) + nt(da3[...], w3[part]))

    @pl.when((q == QUAD - 1) | (e == count - 1))
    def _():
        mix_into(acc, du_all, slots, gates, q, False)

    @pl.when(e == count - 1)
    def _():
        sends = [pltpu.make_async_copy(acc.at[pl.ds(pl.multiple_of(p * tokens, tokens), tokens)], ref, psem.at[r]) for r, (p, ref) in enumerate(zip(order, (p0, p1, p2, p3)))]
        start_all(sends)
        wait_all(flush(e - 1))
        wait_all(flush(e))
        wait_all(sends)


def expert_bwd(loads, u, w1, w2, w3, tokens):
    model = loads.shape[2]
    count, cols, _ = u.shape
    ff = w1.shape[2]
    ring = 3
    hb = pl.BlockSpec(memory_space=pl.ANY)
    part = jax.ShapeDtypeStruct((tokens, model), F32)
    return pl.pallas_call(
        functools.partial(expert_bwd_kernel, cols // 4),
        grid=(count,),
        out_shape=(jax.ShapeDtypeStruct((count, model, ff), F32), jax.ShapeDtypeStruct((count, ff, model), F32), jax.ShapeDtypeStruct((count, model, ff), F32), part, part, part, part),
        in_specs=[hb] * 5,
        out_specs=(hb,) * 7,
        scratch_shapes=[
            pltpu.VMEM((4 * tokens, model), BF), pltpu.VMEM((4, loads.shape[1] - tokens, 3 * tokens), BF),
            pltpu.VMEM((ring, cols, model), BF), pltpu.VMEM((ring, model, ff), BF), pltpu.VMEM((ring, ff, model), BF), pltpu.VMEM((ring, model, ff), BF),
            pltpu.VMEM((8, 4 * tokens), F32), pltpu.VMEM((8, 4 * tokens), F32), pltpu.VMEM((4, QUAD * BLOCK, model), BF),
            pltpu.VMEM((cols, model), BF), pltpu.VMEM((cols, ff), BF), pltpu.VMEM((cols, ff), BF), pltpu.VMEM((cols, ff), BF),
            pltpu.VMEM((2, model, ff), F32), pltpu.VMEM((2, ff, model), F32), pltpu.VMEM((2, model, ff), F32),
            pltpu.VMEM((4 * tokens, model), F32),
            pltpu.SemaphoreType.DMA((8,)), pltpu.SemaphoreType.DMA((ring, 4)), pltpu.SemaphoreType.DMA((2, 3)), pltpu.SemaphoreType.DMA((4,)),
        ],
        compiler_params=pltpu.CompilerParams(vmem_limit_bytes=VMEM_BYTES, dimension_semantics=("arbitrary",)),
        cost_estimate=pl.CostEstimate(flops=50 * 10 ** 9, bytes_accessed=150 * 10 ** 6, transcendentals=0),
        name="expert_bwd",
    )(loads, u, w1, w2, w3)


def expert_fwd_kernel(capacity, u0, u1, u2, u3, loads, b0, b1, b2, b3, w1_h, w2_h, w3_h, du_o, mine_o, out_o,
                      rows, info, w1s, w2s, w3s, slots, gates, out_all, acc, loc0, loc2, rx1, rx3, rxf, ra1, ra3, rsem, wsem, bsem, ssem, xsem):
    e = pl.program_id(0)
    count = pl.num_programs(0)
    me = lax.axis_index('expert')
    near, far = neighbours()
    ring, model, ff = w1s.shape
    q = e % QUAD
    tokens = rows.shape[0] // 4
    arrivals = row_copies((u0, u1, u2, u3), rows, rsem) + [info_copy(loads.at[r], info.at[r], rsem.at[4 + r]) for r in range(4)]
    pairs = ((w1_h, w1s), (w3_h, w3s), (w2_h, w2s))
    local = [pltpu.make_async_copy(b0, loc0, bsem.at[0]), pltpu.make_async_copy(b2, loc2, bsem.at[1])]
    swap3 = remote(b3, rx3, ssem.at[0], xsem.at[0], near)
    swap1 = remote(b1, rx1, ssem.at[1], xsem.at[1], near)
    over = remote(loc2, rxf, ssem.at[2], xsem.at[2], far)
    part = [slice(r * tokens, (r + 1) * tokens) for r in range(4)]
    late3 = remote(acc.at[part[3]], ra3, ssem.at[3], xsem.at[3], near)
    late1 = remote(acc.at[part[1]], ra1, ssem.at[4], xsem.at[4], near)

    @pl.when(e == 0)
    def _():
        start_all(arrivals + local)
        start_all(ring_copies(pairs, wsem, 0, ring) + ring_copies(pairs, wsem, 1, ring), 1)
        greet((near, far))
        swap3.start()
        acc[...] = jnp.zeros_like(acc)
        out_all[...] = jnp.zeros_like(out_all)
        wait_all(arrivals)

    @pl.when(e == 1)
    def _():
        wait_all(local)
        swap3.wait()
        loc2[...] += rx3[...]
        over.start()
        swap1.start()

    @pl.when(e + 2 < count)
    def _():
        start_all(ring_copies(pairs, wsem, e + 2, ring), 1)

    slot_row, gate_row = route_rows(info, 0, me * count + e)
    keep_routes(slots, gates, q, slot_row, gate_row)
    v = nn(jnp.where(hits(slot_row, tokens, capacity), 1.0, 0.0).astype(BF), rows[...]).astype(BF)
    wait_all(ring_copies(pairs, wsem, e, ring))
    now = e % ring
    w1, w2, w3 = w1s.at[now], w2s.at[now], w3s.at[now]
    pieces = []
    for n in range(ff // 256):
        lanes = slice(n * 256, (n + 1) * 256)
        a1 = nn(v, w1[:, lanes]).astype(BF).astype(F32)
        a3 = nn(v, w3[:, lanes]).astype(BF).astype(F32)
        pieces.append((a1 * jax.nn.sigmoid(a1) * a3).astype(BF))
    hidden = jnp.concatenate(pieces, axis=1)
    for n in range(model // 256):
        lanes = slice(n * 256, (n + 1) * 256)
        stash(out_all, q, capacity, lanes, nn(hidden, w2[:, lanes]))

    @pl.when((q == QUAD - 1) | (e == count - 1))
    def _():
        mix_into(acc, out_all, slots, gates, q, True)

    @pl.when(e == count - 1)
    def _():
        late3.start()
        late1.start()
        swap1.wait()
        over.wait()
        du_o[...] = ((loc0[...] + rx1[...]) + rxf[...]).astype(BF)
        late3.wait()
        out_o[...] = acc[part[2]] + ra3[...]
        late1.wait()
        mine_o[...] = acc[part[0]] + ra1[...]


def whole(shape):
    return pl.BlockSpec(shape, lambda e: (0,) * len(shape), pipeline_mode=pl.Buffered(1))


def expert_fwd(us, loads, sums, w1, w2, w3, capacity):
    tokens, model = us[0].shape
    count, _, ff = w1.shape
    ring = 3
    part = jax.ShapeDtypeStruct((tokens, model), F32)
    hb = pl.BlockSpec(memory_space=pl.ANY)
    tile = pltpu.VMEM((tokens, model), F32)
    return pl.pallas_call(
        functools.partial(expert_fwd_kernel, capacity),
        grid=(count,),
        out_shape=(jax.ShapeDtypeStruct((tokens, model), BF), part, part),
        in_specs=[hb] * 12,
        out_specs=(whole((tokens, model)),) * 3,
        scratch_shapes=[
            pltpu.VMEM((4 * tokens, model), BF), pltpu.VMEM((4, loads.shape[1] - tokens, 3 * tokens), BF),
            pltpu.VMEM((ring, model, ff), BF), pltpu.VMEM((ring, ff, model), BF), pltpu.VMEM((ring, model, ff), BF),
            pltpu.VMEM((8, 4 * tokens), F32), pltpu.VMEM((8, 4 * tokens), F32), pltpu.VMEM((4, QUAD * BLOCK, model), BF), pltpu.VMEM((4 * tokens, model), F32),
            tile, tile, tile, tile, tile, tile, tile,
            pltpu.SemaphoreType.DMA((8,)), pltpu.SemaphoreType.DMA((ring, 3)), pltpu.SemaphoreType.DMA((2,)), pltpu.SemaphoreType.DMA((5,)), pltpu.SemaphoreType.DMA((5,)),
        ],
        compiler_params=pltpu.CompilerParams(vmem_limit_bytes=VMEM_BYTES, dimension_semantics=("arbitrary",), collective_id=1, has_side_effects=True),
        cost_estimate=pl.CostEstimate(flops=16 * 10 ** 9, bytes_accessed=50 * 10 ** 6, transcendentals=0),
        name="expert_fwd",
    )(*us, loads, *sums, w1, w2, w3)


def solution(mesh):
    group = mesh.shape['expert']

    def hop(value, bits):
        return lax.ppermute(value, 'expert', [(i, i ^ bits) for i in range(group)])

    def local_step(x_a, x_b, dy_b, eid_a, slot_a, gate_a, eid_b, slot_b, gate_b, u_b, norm_1, norm_2, w_q, w_k, w_v, w_o, w_1, w_2, w_3):
        model, heads, dim = w_q.shape
        kv_heads = w_k.shape[1]
        reps = heads // kv_heads
        wq_t, wk_t, wv_t = (w.transpose(1, 2, 0).reshape(-1, model) for w in (w_q, w_k, w_v))
        wo = w_o.reshape(-1, model)
        fields = [a.T for a in (eid_a, slot_a, gate_a, eid_b, slot_b, gate_b)]
        h_a, u_a, h_b, nb, qkv_b, ctx_b, loads = attn_fwd(x_a, x_b, dy_b, fields, norm_1, norm_2, wq_t, wk_t, wv_t, wo, kv_heads, reps, dim)
        us = (u_a, hop(u_a, 1), hop(u_a, 2), hop(u_a, 3))
        g1, g2, g3, *sums = expert_bwd(loads, u_b, w_1, w_2, w_3, x_a.shape[0])
        du, mine_a, out_a = expert_fwd(us, loads, sums, w_1, w_2, w_3, u_b.shape[1] // group)
        far_a = hop(out_a, 2)
        dx_b, g_q, g_k, g_v, g_o, g_n1, g_n2 = attn_bwd(du, dy_b, h_b, x_b, nb, qkv_b, ctx_b, norm_1, norm_2, wo, wq_t, wk_t, wv_t, kv_heads, reps, dim)
        y_a = (h_a.astype(F32) + (mine_a + far_a)).astype(BF)
        g_q = g_q.reshape(heads, dim, model).transpose(2, 0, 1)
        g_k = g_k.reshape(kv_heads, dim, model).transpose(2, 0, 1)
        g_v = g_v.reshape(kv_heads, dim, model).transpose(2, 0, 1)
        g_o = g_o.reshape(heads, dim, model)
        return (y_a, dx_b, g1, g2, g3, g_q[None], g_k[None], g_v[None], g_o[None], g_n1, g_n2)

    row_spec = P(('data', 'expert'), None)
    cube_spec = P(('data', 'expert'), None, None)
    quad_spec = P(('data', 'expert'), None, None, None)
    expert_spec = P('expert', None, None)
    in_specs = (row_spec, row_spec, row_spec, row_spec, row_spec, row_spec, row_spec, row_spec, row_spec, cube_spec, P(), P(), P(), P(), P(), P(), expert_spec, expert_spec, expert_spec)
    out_specs = (row_spec, row_spec, cube_spec, cube_spec, cube_spec, quad_spec, quad_spec, quad_spec, quad_spec, row_spec, row_spec)
    return jax.shard_map(local_step, mesh=mesh, in_specs=in_specs, out_specs=out_specs, check_vma=False)
```

```python
import functools

import jax
import jax.numpy as jnp
from jax import lax
from jax.experimental import pallas as pl
from jax.experimental.pallas import tpu as pltpu
from jax.sharding import PartitionSpec as P


NORM_EPS = 1e-6
BF = jnp.bfloat16
F32 = jnp.float32
VMEM_BYTES = 67043328
QUAD = 4
BLOCK = 64


def nn(a, b):
    return lax.dot_general(a, b, (((1,), (0,)), ((), ())), preferred_element_type=F32)


def nt(a, b):
    return lax.dot_general(a, b, (((1,), (1,)), ((), ())), preferred_element_type=F32)


def tn(a, b):
    return lax.dot_general(a, b, (((0,), (0,)), ((), ())), preferred_element_type=F32)


def row_of(ref):
    return ref[...].astype(F32).reshape(1, ref.shape[0])


def rms_scale(wide):
    return lax.rsqrt(jnp.mean(wide * wide, axis=-1, keepdims=True) + NORM_EPS)


def rms_rows(values, gain):
    wide = values.astype(F32)
    return (wide * rms_scale(wide) * gain).astype(BF)


def rms_pull(wide, gain, cot):
    scale = rms_scale(wide)
    scaled = wide * scale
    grad_gain = jnp.sum(cot * scaled, axis=0, keepdims=True).astype(BF).astype(F32)
    inner = cot * gain
    pull = jnp.mean(inner * wide, axis=-1, keepdims=True)
    grad = scale * inner - scaled * (scale * scale * pull)
    return grad.astype(BF).astype(F32), grad_gain


def probs_of(scores_t):
    rows = lax.broadcasted_iota(jnp.int32, scores_t.shape, 0)
    cols = lax.broadcasted_iota(jnp.int32, scores_t.shape, 1) % scores_t.shape[0]
    masked = jnp.where(rows <= cols, scores_t, -1e30)
    top = jnp.max(masked, axis=0, keepdims=True)
    unnorm = jnp.exp(masked - top)
    return unnorm / jnp.sum(unnorm, axis=0, keepdims=True)


def heads_to_lanes(ref, group, reps, dim, lanes):
    return jnp.concatenate([ref[(group * reps + r) * dim:(group * reps + r + 1) * dim, lanes] for r in range(reps)], axis=1)


def neighbours():
    me = lax.axis_index('expert')
    return me + 1 - 2 * (me % 2), (me + 2) % 4


def greet(peers):
    barrier = pltpu.get_barrier_semaphore()
    for peer in peers:
        pl.semaphore_signal(barrier, inc=1, device_id={'expert': peer}, device_id_type=pl.DeviceIdType.MESH)
    pl.semaphore_wait(barrier, len(peers))


def remote(src, dst, send, recv, peer):
    return pltpu.make_async_remote_copy(src_ref=src, dst_ref=dst, send_sem=send, recv_sem=recv, device_id={'expert': peer}, device_id_type=pl.DeviceIdType.MESH)


def attn_fwd_kernel(kv_heads, reps, dim, xa_h, xb_h, dy_h, ea, sa, ga, eb, sb, gb, n1, n2, wq_h, wk_h, wv_h, wo_h,
                    ha_h, ua_h, hb_h, nb_h, qkv_h, ctx_h, load_h,
                    xs, wq, wk, wv, wo, nrm, nrm_t, q_t, k_t, v_t, ctx, q_b, ctx_b, hs, ua, mine, far_in, ints, gates, sems, osems, ssem, rsem, tsem):
    near, far = neighbours()
    tokens = xs.shape[0] // 2
    small = ((ea, ints.at[0]), (sa, ints.at[1]), (eb, ints.at[2]), (sb, ints.at[3]), (ga, gates.at[0]), (gb, gates.at[1]))
    tiny = [pltpu.make_async_copy(s, d, tsem.at[i]) for i, (s, d) in enumerate(small)]
    heads = kv_heads * reps
    first, second = slice(0, tokens), slice(tokens, 2 * tokens)
    half = heads * dim // 2
    moves = ((dy_h, mine.at[0:tokens]), (xa_h, xs.at[first]), (xb_h, xs.at[second]), (wk_h, wk), (wv_h, wv), (wq_h.at[0:half], wq.at[0:half]), (wq_h.at[half:], wq.at[half:]), (wo_h, wo))
    copies = [pltpu.make_async_copy(s, d, sems.at[i]) for i, (s, d) in enumerate(moves)]
    start_all(copies[0:1] + tiny + copies[1:3])
    start_all(copies[3:], 1)
    outs = []

    def flush(src, dst):
        c = pltpu.make_async_copy(src, dst, osems.at[len(outs)])
        c.start()
        outs.append(c)

    greet((near, far))
    wait_all(tiny)
    fields = [v.astype(F32) for v in (ints[0], ints[1], gates[0], ints[2], ints[3], gates[1])]
    both = jnp.concatenate([jnp.concatenate(fields[0:3], axis=1), jnp.concatenate(fields[3:6], axis=1)], axis=0)
    mine[tokens:] = jnp.concatenate([both, jnp.zeros((both.shape[0], mine.shape[1] - both.shape[1]), F32)], axis=1).astype(BF)
    copies[0].wait()
    to_far = remote(mine, far_in, ssem.at[0], rsem.at[0], far)
    to_near = remote(mine, load_h.at[1], ssem.at[1], rsem.at[1], near)
    relay = remote(far_in, load_h.at[3], ssem.at[2], rsem.at[2], near)
    to_far.start()
    to_near.start()
    flush(mine, load_h.at[0])

    wait_all(copies[1:3])
    nrm[...] = rms_rows(xs[...], row_of(n1))
    nrm_t[...] = jnp.transpose(nrm[...])
    flush(nrm.at[second], nb_h)
    copies[3].wait()
    k_t[...] = nn(wk[...], nrm_t[...]).astype(BF)
    copies[4].wait()
    v_t[...] = nn(wv[...], nrm_t[...]).astype(BF)
    for i in range(2):
        copies[5 + i].wait()
        part = slice(i * half, (i + 1) * half)
        q_t[part] = nn(wq[part], nrm_t[...]).astype(BF)
    q_b[0:heads * dim] = q_t[:, second]
    q_b[heads * dim:(heads + kv_heads) * dim] = k_t[:, second]
    q_b[(heads + kv_heads) * dim:] = v_t[:, second]
    flush(q_b, qkv_h)
    for lanes in (second, first):
        for g in range(kv_heads):
            kg = k_t[g * dim:(g + 1) * dim, lanes]
            vg = v_t[g * dim:(g + 1) * dim, lanes]
            qg = heads_to_lanes(q_t, g, reps, dim, lanes)
            probs = probs_of(tn(kg, qg) * dim ** -0.5).astype(BF)
            out = nn(vg, probs).astype(BF)
            for r in range(reps):
                ctx[(g * reps + r) * dim:(g * reps + r + 1) * dim, lanes] = out[:, r * tokens:(r + 1) * tokens]
    ctx_b[...] = ctx[:, second]
    flush(ctx_b, ctx_h)
    copies[7].wait()
    hs[...] = (xs[...].astype(F32) + tn(ctx[...], wo[...]).astype(BF).astype(F32)).astype(BF)
    to_far.wait_recv()
    relay.start()
    flush(far_in, load_h.at[2])
    flush(hs.at[first], ha_h)
    flush(hs.at[second], hb_h)
    ua[...] = rms_rows(hs[first], row_of(n2))
    flush(ua, ua_h)
    to_far.wait_send()
    to_near.wait()
    relay.wait()
    wait_all(outs)


def attn_fwd(x_a, x_b, dy, fields, n1, n2, wq, wk, wv, wo, kv_heads, reps, dim):
    tokens, model = x_a.shape
    q_dim, kv_dim = kv_heads * reps * dim, kv_heads * dim
    depth = 2 * fields[0].shape[0]
    vm = pl.BlockSpec(memory_space=pltpu.VMEM)
    hb = pl.BlockSpec(memory_space=pl.ANY)
    row = jax.ShapeDtypeStruct((tokens, model), BF)
    return pl.pallas_call(
        functools.partial(attn_fwd_kernel, kv_heads, reps, dim),
        out_shape=(row, row, row, row, jax.ShapeDtypeStruct((q_dim + 2 * kv_dim, tokens), BF), jax.ShapeDtypeStruct((q_dim, tokens), BF), jax.ShapeDtypeStruct((4, tokens + depth, model), BF)),
        in_specs=[hb] * 9 + [vm] * 2 + [hb] * 4,
        out_specs=(hb,) * 7,
        scratch_shapes=[
            pltpu.VMEM((2 * tokens, model), BF),
            pltpu.VMEM((q_dim, model), BF), pltpu.VMEM((kv_dim, model), BF), pltpu.VMEM((kv_dim, model), BF), pltpu.VMEM((q_dim, model), BF),
            pltpu.VMEM((2 * tokens, model), BF), pltpu.VMEM((model, 2 * tokens), BF),
            pltpu.VMEM((q_dim, 2 * tokens), BF), pltpu.VMEM((kv_dim, 2 * tokens), BF), pltpu.VMEM((kv_dim, 2 * tokens), BF), pltpu.VMEM((q_dim, 2 * tokens), BF),
            pltpu.VMEM((q_dim + 2 * kv_dim, tokens), BF), pltpu.VMEM((q_dim, tokens), BF), pltpu.VMEM((2 * tokens, model), BF), pltpu.VMEM((tokens, model), BF),
            pltpu.VMEM((tokens + depth, model), BF), pltpu.VMEM((tokens + depth, model), BF),
            pltpu.VMEM((4,) + fields[0].shape, jnp.int32), pltpu.VMEM((2,) + fields[2].shape, BF),
            pltpu.SemaphoreType.DMA((8,)), pltpu.SemaphoreType.DMA((8,)), pltpu.SemaphoreType.DMA((3,)), pltpu.SemaphoreType.DMA((3,)), pltpu.SemaphoreType.DMA((6,)),
        ],
        compiler_params=pltpu.CompilerParams(vmem_limit_bytes=VMEM_BYTES, collective_id=0, has_side_effects=True),
        cost_estimate=pl.CostEstimate(flops=10 ** 10, bytes_accessed=14 * 10 ** 6, transcendentals=0),
        name="attn_fwd",
    )(x_a, x_b, dy, *fields, n1, n2, wq, wk, wv, wo)


def attn_bwd_kernel(kv_heads, reps, dim, du_in, dy, h_b, x_b, nb, qkv, ctx, n1, n2, wo_h, wq_h, wk_h, wv_h, g1_in, g2_in, g3_in, u_h, hid_h, da1_h, da3_h, do_h,
                    dx, gq, gk, gv, go, gn1, gn2, g1, g2, g3,
                    wo, wq, wk, wv, oq, ok, ov, oo, dctx, dq, dk, dv, u, hid, da1, da3, d_out, o1, o2, o3, sems, osems, esems):
    last = u_h.shape[0] - 1
    extra = [pltpu.make_async_copy(s, d, esems.at[i]) for i, (s, d) in enumerate(((do_h, d_out), (hid_h, hid), (u_h.at[last], u), (da1_h, da1), (da3_h, da3)))]
    start_all(extra)
    copies = [pltpu.make_async_copy(s, d, sems.at[i]) for i, (s, d) in enumerate(((wo_h, wo), (wq_h, wq), (wk_h, wk), (wv_h, wv)))]
    start_all(copies, 1)
    tokens = x_b.shape[0]
    q_dim, kv_dim = kv_heads * reps * dim, kv_heads * dim
    du = du_in[...].astype(F32)
    grad_h, gain_2 = rms_pull(h_b[...].astype(F32), row_of(n2), du)
    gn2[...] = gain_2
    dh = (dy[...].astype(F32) + grad_h).astype(BF)
    outs = []

    def flush(src, dst):
        c = pltpu.make_async_copy(src, dst, osems.at[len(outs)])
        c.start()
        outs.append(c)

    wait_all(extra)
    for m in range(hid.shape[1] // 256):
        part = slice(m * 256, (m + 1) * 256)
        o2[part] = tn(hid[:, part], d_out[...])
    flush(o2, g2.at[last])
    for grad, cot, dst in ((o1, da1, g1), (o3, da3, g3)):
        for m in range(u.shape[1] // 256):
            part = slice(m * 256, (m + 1) * 256)
            grad[part] = tn(u[:, part], cot[...])
        flush(grad, dst.at[last])
    copies[0].wait()
    step = q_dim // 4
    for i in range(4):
        dctx[i * step:(i + 1) * step] = nt(wo[i * step:(i + 1) * step], dh).astype(BF)
    for i in range(4):
        part = slice(i * step, (i + 1) * step)
        oo[part] = nn(ctx[part], dh).astype(BF).astype(F32)
        flush(oo.at[part], go.at[part])
    every = slice(0, tokens)
    normed = nb[...]
    for g in range(kv_heads):
        kv = slice(g * dim, (g + 1) * dim)
        kg = qkv[q_dim + g * dim:q_dim + (g + 1) * dim]
        vg = qkv[q_dim + kv_dim + g * dim:q_dim + kv_dim + (g + 1) * dim]
        qg = heads_to_lanes(qkv, g, reps, dim, every)
        dg = heads_to_lanes(dctx, g, reps, dim, every)
        probs = probs_of(tn(kg, qg) * dim ** -0.5)
        dprobs = tn(vg, dg).astype(BF).astype(F32)
        weighted = probs * dprobs
        dscores = ((weighted - probs * jnp.sum(weighted, axis=0, keepdims=True)) * dim ** -0.5).astype(BF)
        dv[kv] = nt(dg, probs.astype(BF)).astype(BF)
        dk[kv] = nt(qg, dscores).astype(BF)
        dqg = nn(kg, dscores).astype(BF)
        for r in range(reps):
            dq[(g * reps + r) * dim:(g * reps + r + 1) * dim] = dqg[:, r * tokens:(r + 1) * tokens]
        if g % 2 == 1:
            part = slice((g - 1) * reps * dim, (g + 1) * reps * dim)
            oq[part] = nn(dq[part], normed).astype(BF).astype(F32)
            flush(oq.at[part], gq.at[part])
    ok[...] = nn(dk[...], normed).astype(BF).astype(F32)
    flush(ok, gk)
    ov[...] = nn(dv[...], normed).astype(BF).astype(F32)
    flush(ov, gv)
    for c in copies[1:]:
        c.wait()
    dn = (tn(dq[...], wq[...]) + tn(dk[...], wk[...]) + tn(dv[...], wv[...])).astype(BF).astype(F32)
    grad_x, gain_1 = rms_pull(x_b[...].astype(F32), row_of(n1), dn)
    gn1[...] = gain_1
    dx[...] = (dh.astype(F32) + grad_x).astype(BF)
    for c in outs:
        c.wait()


def attn_bwd(du, dy, h_b, x_b, nb, qkv, ctx, n1, n2, wo, wq, wk, wv, grads, u, keeps, kv_heads, reps, dim):
    tokens, model = x_b.shape
    q_dim, kv_dim = kv_heads * reps * dim, kv_heads * dim
    vm = pl.BlockSpec(memory_space=pltpu.VMEM)
    hb = pl.BlockSpec(memory_space=pl.ANY)
    n_out = 4 + kv_heads // 2 + 2 + 3
    cols, ff = keeps[0].shape
    kept = pltpu.VMEM((cols, ff), BF)
    return pl.pallas_call(
        functools.partial(attn_bwd_kernel, kv_heads, reps, dim),
        out_shape=(
            jax.ShapeDtypeStruct((tokens, model), BF), jax.ShapeDtypeStruct((q_dim, model), F32), jax.ShapeDtypeStruct((kv_dim, model), F32),
            jax.ShapeDtypeStruct((kv_dim, model), F32), jax.ShapeDtypeStruct((q_dim, model), F32), jax.ShapeDtypeStruct((1, model), F32), jax.ShapeDtypeStruct((1, model), F32),
        ) + tuple(jax.ShapeDtypeStruct(g.shape, F32) for g in grads),
        in_specs=[vm] * 9 + [hb] * 12,
        out_specs=(vm, hb, hb, hb, hb, vm, vm, hb, hb, hb),
        input_output_aliases={13: 7, 14: 8, 15: 9},
        scratch_shapes=[
            pltpu.VMEM((q_dim, model), BF), pltpu.VMEM((q_dim, model), BF), pltpu.VMEM((kv_dim, model), BF), pltpu.VMEM((kv_dim, model), BF),
            pltpu.VMEM((q_dim, model), F32), pltpu.VMEM((kv_dim, model), F32), pltpu.VMEM((kv_dim, model), F32), pltpu.VMEM((q_dim, model), F32),
            pltpu.VMEM((q_dim, tokens), BF), pltpu.VMEM((q_dim, tokens), BF), pltpu.VMEM((kv_dim, tokens), BF), pltpu.VMEM((kv_dim, tokens), BF),
            pltpu.VMEM((cols, model), BF), kept, kept, kept, pltpu.VMEM((cols, model), BF), pltpu.VMEM((model, ff), F32), pltpu.VMEM((ff, model), F32), pltpu.VMEM((model, ff), F32),
            pltpu.SemaphoreType.DMA((4,)), pltpu.SemaphoreType.DMA((n_out,)), pltpu.SemaphoreType.DMA((5,)),
        ],
        compiler_params=pltpu.CompilerParams(vmem_limit_bytes=60 * 1024 * 1024),
        cost_estimate=pl.CostEstimate(flops=14 * 10 ** 9, bytes_accessed=40 * 10 ** 6, transcendentals=0),
        name="attn_bwd",
    )(du, dy, h_b, x_b, nb, qkv, ctx, n1, n2, wo, wq, wk, wv, *grads, u, *keeps)


def route_rows(info, base, expert):
    group, _, width = info.shape
    tokens = width // 3
    top_k = info.shape[1] // 2
    wide = [info[r].astype(F32)[base * top_k:(base + 1) * top_k] for r in range(group)]

    def field(i):
        return jnp.concatenate([w[:, i * tokens:(i + 1) * tokens] for w in wide], axis=1)

    eid, slot, gate = field(0), field(1), field(2)
    hit = (eid == expert.astype(F32)) & (slot >= 0.0)
    slot_row = jnp.sum(jnp.where(hit, slot + 1.0, 0.0), axis=0, keepdims=True) - 1.0
    gate_row = jnp.sum(jnp.where(hit, gate, 0.0), axis=0, keepdims=True)
    return slot_row, gate_row


def ring_copies(pairs, sem, idx, ring):
    s = lax.rem(idx, ring)
    return [pltpu.make_async_copy(src.at[idx], dst.at[s], sem.at[s, i]) for i, (src, dst) in enumerate(pairs)]


def row_copies(refs, rows, sem):
    tokens = rows.shape[0] // len(refs)
    return [pltpu.make_async_copy(ref.at[0:tokens], rows.at[r * tokens:(r + 1) * tokens], sem.at[r]) for r, ref in enumerate(refs)]


def info_copy(load, info, sem):
    depth, width = info.shape
    first = load.shape[0] - depth
    return pltpu.make_async_copy(load.at[first:first + depth, 0:width], info, sem)


def hits(slot_row, tokens, capacity):
    source = lax.broadcasted_iota(jnp.int32, slot_row.shape, 1) // tokens
    col_row = jnp.where(slot_row >= 0.0, slot_row.astype(jnp.int32) + source * capacity, -1)
    return lax.broadcasted_iota(jnp.int32, (4 * capacity, slot_row.shape[1]), 0) == col_row


def start_all(copies, priority=0):
    for c in copies:
        c.start(priority=priority)


def wait_all(copies):
    for c in copies:
        c.wait()


def keep_routes(slots, gates, q, slot_row, gate_row):
    slots[pl.ds(q, 1), :] = slot_row
    gates[pl.ds(q, 1), :] = gate_row


def stash(outs, q, capacity, lanes, res):
    for r in range(outs.shape[0]):
        outs[r, pl.ds(pl.multiple_of(q * BLOCK, BLOCK), capacity), lanes] = res[r * capacity:(r + 1) * capacity].astype(BF)


def mix_into(acc, outs, slots, gates, q, weighted):
    tokens = acc.shape[0] // outs.shape[0]
    depth = lax.broadcasted_iota(jnp.int32, (BLOCK, tokens), 0).astype(F32)
    for r in range(outs.shape[0]):
        lanes = slice(r * tokens, (r + 1) * tokens)
        blocks = []
        for k in range(QUAD):
            weight = gates[k:k + 1, lanes] if weighted else 1.0
            slot = jnp.where(q >= k, slots[k:k + 1, lanes], -1.0)
            blocks.append(jnp.where(depth == slot, weight, 0.0))
        pick = jnp.transpose(jnp.concatenate(blocks, axis=0).astype(BF))
        for n in range(acc.shape[1] // 512):
            part = slice(n * 512, (n + 1) * 512)
            acc[lanes, part] += nn(pick, outs[r, :, part])


def expert_bwd_kernel(capacity, loads, u_h, w1_h, w2_h, w3_h,
                      g1, g2, g3, p0, p1, p2, p3, s_hid, s_da1, s_da3, s_do,
                      rows, info, us, w1s, w2s, w3s, slots, gates, du_all, d_out, hid, da1, da3, o1, o2, o3, acc, rsem, wsem, sems, psem, ksem):
    e = pl.program_id(0)
    count = pl.num_programs(0)
    me = lax.axis_index('expert')
    slot_e = lax.rem(e, 2)
    ring, _, model = us.shape
    tokens = rows.shape[0] // 4
    ff = w1s.shape[2]
    order = [jnp.bitwise_xor(me, r) for r in range(4)]
    arrivals = row_copies([loads.at[p] for p in order], rows, rsem) + [info_copy(loads.at[p], info.at[r], rsem.at[4 + r]) for r, p in enumerate(order)]
    pairs = ((u_h, us), (w1_h, w1s), (w3_h, w3s), (w2_h, w2s))

    @pl.when(e == 0)
    def _():
        start_all(arrivals + ring_copies(pairs, wsem, 0, ring) + ring_copies(pairs, wsem, 1, ring))
        acc[...] = jnp.zeros_like(acc)
        du_all[...] = jnp.zeros_like(du_all)
        wait_all(arrivals)

    @pl.when(e + 2 < count)
    def _():
        start_all(ring_copies(pairs, wsem, e + 2, ring))

    slot_row, gate_row = route_rows(info, 1, me * count + e)
    q = lax.rem(e, QUAD)
    keep_routes(slots, gates, q, slot_row, gate_row)
    hot = hits(slot_row, tokens, capacity)
    d_out[...] = nn(jnp.where(hot, gate_row, 0.0).astype(BF), rows[...]).astype(BF)

    def flush(idx):
        s = lax.rem(idx, 2)
        return [pltpu.make_async_copy(src.at[s], dst.at[idx], sems.at[s, i]) for i, (src, dst) in enumerate(((o1, g1), (o2, g2), (o3, g3)))]

    wait_all(ring_copies(pairs, wsem, e, ring))
    now = lax.rem(e, ring)
    u, w1, w2, w3 = us.at[now], w1s.at[now], w2s.at[now], w3s.at[now]
    uv = u[...]
    dov = d_out[...]
    for n in range(ff // 256):
        part = slice(n * 256, (n + 1) * 256)
        pre1 = nn(uv, w1[:, part]).astype(BF).astype(F32)
        pre3 = nn(uv, w3[:, part]).astype(BF).astype(F32)
        grad_hid = nt(dov, w2[part, :]).astype(BF).astype(F32)
        sigma = jax.nn.sigmoid(pre1)
        silu = pre1 * sigma
        hid[:, part] = (silu * pre3).astype(BF)
        da1[:, part] = (grad_hid * pre3 * sigma * (1.0 + pre1 * (1.0 - sigma))).astype(BF)
        da3[:, part] = (grad_hid * silu).astype(BF)

    keeps = [pltpu.make_async_copy(src, dst, ksem.at[i]) for i, (src, dst) in enumerate(((hid, s_hid), (da1, s_da1), (da3, s_da3), (d_out, s_do)))]

    @pl.when((e >= 2) & (e < count - 1))
    def _():
        wait_all(flush(e - 2))

    @pl.when(e < count - 1)
    def _():
        fresh = flush(e)
        for m in range(ff // 256):
            part = slice(m * 256, (m + 1) * 256)
            o2[slot_e, part] = tn(hid[:, part], d_out[...])
        fresh[1].start()
        for m in range(model // 256):
            part = slice(m * 256, (m + 1) * 256)
            o1[slot_e, part] = tn(u[:, part], da1[...])
        fresh[0].start()
        for m in range(model // 256):
            part = slice(m * 256, (m + 1) * 256)
            o3[slot_e, part] = tn(u[:, part], da3[...])
        fresh[2].start()

    @pl.when(e == count - 1)
    def _():
        start_all(keeps)

    for n in range(model // 256):
        part = slice(n * 256, (n + 1) * 256)
        stash(du_all, q, capacity, part, nt(da1[...], w1[part]) + nt(da3[...], w3[part]))

    @pl.when((q == QUAD - 1) | (e == count - 1))
    def _():
        mix_into(acc, du_all, slots, gates, q, False)

    @pl.when(e == count - 1)
    def _():
        sends = [pltpu.make_async_copy(acc.at[pl.ds(pl.multiple_of(p * tokens, tokens), tokens)], ref, psem.at[r]) for r, (p, ref) in enumerate(zip(order, (p0, p1, p2, p3)))]
        start_all(sends)
        wait_all(keeps)
        wait_all(flush(e - 2))
        wait_all(flush(e - 1))
        wait_all(sends)


def expert_bwd(loads, u, w1, w2, w3, tokens):
    model = loads.shape[2]
    count, cols, _ = u.shape
    ff = w1.shape[2]
    ring = 3
    hb = pl.BlockSpec(memory_space=pl.ANY)
    keep = jax.ShapeDtypeStruct((cols, ff), BF)
    part = jax.ShapeDtypeStruct((tokens, model), F32)
    return pl.pallas_call(
        functools.partial(expert_bwd_kernel, cols // 4),
        grid=(count,),
        out_shape=(jax.ShapeDtypeStruct((count, model, ff), F32), jax.ShapeDtypeStruct((count, ff, model), F32), jax.ShapeDtypeStruct((count, model, ff), F32), part, part, part, part, keep, keep, keep, jax.ShapeDtypeStruct((cols, model), BF)),
        in_specs=[hb] * 5,
        out_specs=(hb,) * 11,
        scratch_shapes=[
            pltpu.VMEM((4 * tokens, model), BF), pltpu.VMEM((4, loads.shape[1] - tokens, 3 * tokens), BF),
            pltpu.VMEM((ring, cols, model), BF), pltpu.VMEM((ring, model, ff), BF), pltpu.VMEM((ring, ff, model), BF), pltpu.VMEM((ring, model, ff), BF),
            pltpu.VMEM((8, 4 * tokens), F32), pltpu.VMEM((8, 4 * tokens), F32), pltpu.VMEM((4, QUAD * BLOCK, model), BF),
            pltpu.VMEM((cols, model), BF), pltpu.VMEM((cols, ff), BF), pltpu.VMEM((cols, ff), BF), pltpu.VMEM((cols, ff), BF),
            pltpu.VMEM((2, model, ff), F32), pltpu.VMEM((2, ff, model), F32), pltpu.VMEM((2, model, ff), F32),
            pltpu.VMEM((4 * tokens, model), F32),
            pltpu.SemaphoreType.DMA((8,)), pltpu.SemaphoreType.DMA((ring, 4)), pltpu.SemaphoreType.DMA((2, 3)), pltpu.SemaphoreType.DMA((4,)), pltpu.SemaphoreType.DMA((4,)),
        ],
        compiler_params=pltpu.CompilerParams(vmem_limit_bytes=VMEM_BYTES, dimension_semantics=("arbitrary",)),
        cost_estimate=pl.CostEstimate(flops=50 * 10 ** 9, bytes_accessed=150 * 10 ** 6, transcendentals=0),
        name="expert_bwd",
    )(loads, u, w1, w2, w3)


def expert_fwd_kernel(capacity, u0, u1, u2, u3, loads, b0, b1, b2, b3, w1_h, w2_h, w3_h, du_o, mine_o, out_o,
                      rows, info, w1s, w2s, w3s, slots, gates, out_all, acc, loc0, loc2, rx1, rx3, rxf, ra1, ra3, rsem, wsem, bsem, ssem, xsem):
    e = pl.program_id(0)
    count = pl.num_programs(0)
    me = lax.axis_index('expert')
    near, far = neighbours()
    ring, model, ff = w1s.shape
    q = e % QUAD
    tokens = rows.shape[0] // 4
    arrivals = row_copies((u0, u1, u2, u3), rows, rsem) + [info_copy(loads.at[r], info.at[r], rsem.at[4 + r]) for r in range(4)]
    pairs = ((w1_h, w1s), (w3_h, w3s), (w2_h, w2s))
    local = [pltpu.make_async_copy(b0, loc0, bsem.at[0]), pltpu.make_async_copy(b2, loc2, bsem.at[1])]
    swap3 = remote(b3, rx3, ssem.at[0], xsem.at[0], near)
    swap1 = remote(b1, rx1, ssem.at[1], xsem.at[1], near)
    over = remote(loc2, rxf, ssem.at[2], xsem.at[2], far)
    part = [slice(r * tokens, (r + 1) * tokens) for r in range(4)]
    late3 = remote(acc.at[part[3]], ra3, ssem.at[3], xsem.at[3], near)
    late1 = remote(acc.at[part[1]], ra1, ssem.at[4], xsem.at[4], near)

    @pl.when(e == 0)
    def _():
        start_all(arrivals + local)
        start_all(ring_copies(pairs, wsem, 0, ring) + ring_copies(pairs, wsem, 1, ring), 1)
        greet((near, far))
        swap3.start()
        acc[...] = jnp.zeros_like(acc)
        out_all[...] = jnp.zeros_like(out_all)
        wait_all(arrivals)

    @pl.when(e == 1)
    def _():
        wait_all(local)
        swap3.wait()
        loc2[...] += rx3[...]
        over.start()
        swap1.start()

    @pl.when(e + 2 < count)
    def _():
        start_all(ring_copies(pairs, wsem, e + 2, ring), 1)

    slot_row, gate_row = route_rows(info, 0, me * count + e)
    keep_routes(slots, gates, q, slot_row, gate_row)
    v = nn(jnp.where(hits(slot_row, tokens, capacity), 1.0, 0.0).astype(BF), rows[...]).astype(BF)
    wait_all(ring_copies(pairs, wsem, e, ring))
    now = e % ring
    w1, w2, w3 = w1s.at[now], w2s.at[now], w3s.at[now]
    pieces = []
    for n in range(ff // 256):
        lanes = slice(n * 256, (n + 1) * 256)
        a1 = nn(v, w1[:, lanes]).astype(BF).astype(F32)
        a3 = nn(v, w3[:, lanes]).astype(BF).astype(F32)
        pieces.append((a1 * jax.nn.sigmoid(a1) * a3).astype(BF))
    hidden = jnp.concatenate(pieces, axis=1)
    for n in range(model // 256):
        lanes = slice(n * 256, (n + 1) * 256)
        stash(out_all, q, capacity, lanes, nn(hidden, w2[:, lanes]))

    @pl.when((q == QUAD - 1) | (e == count - 1))
    def _():
        mix_into(acc, out_all, slots, gates, q, True)

    @pl.when(e == count - 1)
    def _():
        late3.start()
        late1.start()
        swap1.wait()
        over.wait()
        du_o[...] = ((loc0[...] + rx1[...]) + rxf[...]).astype(BF)
        late3.wait()
        out_o[...] = acc[part[2]] + ra3[...]
        late1.wait()
        mine_o[...] = acc[part[0]] + ra1[...]


def whole(shape):
    return pl.BlockSpec(shape, lambda e: (0,) * len(shape), pipeline_mode=pl.Buffered(1))


def expert_fwd(us, loads, sums, w1, w2, w3, capacity):
    tokens, model = us[0].shape
    count, _, ff = w1.shape
    ring = 3
    part = jax.ShapeDtypeStruct((tokens, model), F32)
    hb = pl.BlockSpec(memory_space=pl.ANY)
    tile = pltpu.VMEM((tokens, model), F32)
    return pl.pallas_call(
        functools.partial(expert_fwd_kernel, capacity),
        grid=(count,),
        out_shape=(jax.ShapeDtypeStruct((tokens, model), BF), part, part),
        in_specs=[hb] * 12,
        out_specs=(whole((tokens, model)),) * 3,
        scratch_shapes=[
            pltpu.VMEM((4 * tokens, model), BF), pltpu.VMEM((4, loads.shape[1] - tokens, 3 * tokens), BF),
            pltpu.VMEM((ring, model, ff), BF), pltpu.VMEM((ring, ff, model), BF), pltpu.VMEM((ring, model, ff), BF),
            pltpu.VMEM((8, 4 * tokens), F32), pltpu.VMEM((8, 4 * tokens), F32), pltpu.VMEM((4, QUAD * BLOCK, model), BF), pltpu.VMEM((4 * tokens, model), F32),
            tile, tile, tile, tile, tile, tile, tile,
            pltpu.SemaphoreType.DMA((8,)), pltpu.SemaphoreType.DMA((ring, 3)), pltpu.SemaphoreType.DMA((2,)), pltpu.SemaphoreType.DMA((5,)), pltpu.SemaphoreType.DMA((5,)),
        ],
        compiler_params=pltpu.CompilerParams(vmem_limit_bytes=VMEM_BYTES, dimension_semantics=("arbitrary",), collective_id=1, has_side_effects=True),
        cost_estimate=pl.CostEstimate(flops=16 * 10 ** 9, bytes_accessed=50 * 10 ** 6, transcendentals=0),
        name="expert_fwd",
    )(*us, loads, *sums, w1, w2, w3)


def solution(mesh):
    group = mesh.shape['expert']

    def hop(value, bits):
        return lax.ppermute(value, 'expert', [(i, i ^ bits) for i in range(group)])

    def local_step(x_a, x_b, dy_b, eid_a, slot_a, gate_a, eid_b, slot_b, gate_b, u_b, norm_1, norm_2, w_q, w_k, w_v, w_o, w_1, w_2, w_3):
        model, heads, dim = w_q.shape
        kv_heads = w_k.shape[1]
        reps = heads // kv_heads
        wq_t, wk_t, wv_t = (w.transpose(1, 2, 0).reshape(-1, model) for w in (w_q, w_k, w_v))
        wo = w_o.reshape(-1, model)
        fields = [a.T for a in (eid_a, slot_a, gate_a, eid_b, slot_b, gate_b)]
        h_a, u_a, h_b, nb, qkv_b, ctx_b, loads = attn_fwd(x_a, x_b, dy_b, fields, norm_1, norm_2, wq_t, wk_t, wv_t, wo, kv_heads, reps, dim)
        us = (u_a, hop(u_a, 1), hop(u_a, 2), hop(u_a, 3))
        g1, g2, g3, *rest = expert_bwd(loads, u_b, w_1, w_2, w_3, x_a.shape[0])
        du, mine_a, out_a = expert_fwd(us, loads, rest[0:4], w_1, w_2, w_3, u_b.shape[1] // group)
        far_a = hop(out_a, 2)
        dx_b, g_q, g_k, g_v, g_o, g_n1, g_n2, g1, g2, g3 = attn_bwd(du, dy_b, h_b, x_b, nb, qkv_b, ctx_b, norm_1, norm_2, wo, wq_t, wk_t, wv_t, (g1, g2, g3), u_b, rest[4:8], kv_heads, reps, dim)
        y_a = (h_a.astype(F32) + (mine_a + far_a)).astype(BF)
        g_q = g_q.reshape(heads, dim, model).transpose(2, 0, 1)
        g_k = g_k.reshape(kv_heads, dim, model).transpose(2, 0, 1)
        g_v = g_v.reshape(kv_heads, dim, model).transpose(2, 0, 1)
        g_o = g_o.reshape(heads, dim, model)
        return (y_a, dx_b, g1, g2, g3, g_q[None], g_k[None], g_v[None], g_o[None], g_n1, g_n2)

    row_spec = P(('data', 'expert'), None)
    cube_spec = P(('data', 'expert'), None, None)
    quad_spec = P(('data', 'expert'), None, None, None)
    expert_spec = P('expert', None, None)
    in_specs = (row_spec, row_spec, row_spec, row_spec, row_spec, row_spec, row_spec, row_spec, row_spec, cube_spec, P(), P(), P(), P(), P(), P(), expert_spec, expert_spec, expert_spec)
    out_specs = (row_spec, row_spec, cube_spec, cube_spec, cube_spec, quad_spec, quad_spec, quad_spec, quad_spec, row_spec, row_spec)
    return jax.shard_map(local_step, mesh=mesh, in_specs=in_specs, out_specs=out_specs, check_vma=False)
```

```python
import functools

import jax
import jax.numpy as jnp
from jax import lax
from jax.experimental import pallas as pl
from jax.experimental.pallas import tpu as pltpu
from jax.sharding import PartitionSpec as P


NORM_EPS = 1e-6
BF = jnp.bfloat16
F32 = jnp.float32
VMEM_BYTES = 67043328
QUAD = 4
BLOCK = 64


def nn(a, b):
    return lax.dot_general(a, b, (((1,), (0,)), ((), ())), preferred_element_type=F32)


def nt(a, b):
    return lax.dot_general(a, b, (((1,), (1,)), ((), ())), preferred_element_type=F32)


def tn(a, b):
    return lax.dot_general(a, b, (((0,), (0,)), ((), ())), preferred_element_type=F32)


def row_of(ref):
    return ref[...].astype(F32).reshape(1, ref.shape[0])


def rms_scale(wide):
    return lax.rsqrt(jnp.mean(wide * wide, axis=-1, keepdims=True) + NORM_EPS)


def rms_rows(values, gain):
    wide = values.astype(F32)
    return (wide * rms_scale(wide) * gain).astype(BF)


def rms_pull(wide, gain, cot):
    scale = rms_scale(wide)
    scaled = wide * scale
    grad_gain = jnp.sum(cot * scaled, axis=0, keepdims=True).astype(BF).astype(F32)
    inner = cot * gain
    pull = jnp.mean(inner * wide, axis=-1, keepdims=True)
    grad = scale * inner - scaled * (scale * scale * pull)
    return grad.astype(BF).astype(F32), grad_gain


def probs_of(scores_t):
    rows = lax.broadcasted_iota(jnp.int32, scores_t.shape, 0)
    cols = lax.broadcasted_iota(jnp.int32, scores_t.shape, 1) % scores_t.shape[0]
    masked = jnp.where(rows <= cols, scores_t, -1e30)
    top = jnp.max(masked, axis=0, keepdims=True)
    unnorm = jnp.exp(masked - top)
    return unnorm / jnp.sum(unnorm, axis=0, keepdims=True)


def heads_to_lanes(ref, group, reps, dim, lanes):
    return jnp.concatenate([ref[(group * reps + r) * dim:(group * reps + r + 1) * dim, lanes] for r in range(reps)], axis=1)


def neighbours():
    me = lax.axis_index('expert')
    return me + 1 - 2 * (me % 2), (me + 2) % 4


def greet(peers):
    barrier = pltpu.get_barrier_semaphore()
    for peer in peers:
        pl.semaphore_signal(barrier, inc=1, device_id={'expert': peer}, device_id_type=pl.DeviceIdType.MESH)
    pl.semaphore_wait(barrier, len(peers))


def remote(src, dst, send, recv, peer):
    return pltpu.make_async_remote_copy(src_ref=src, dst_ref=dst, send_sem=send, recv_sem=recv, device_id={'expert': peer}, device_id_type=pl.DeviceIdType.MESH)


def attn_fwd_kernel(kv_heads, reps, dim, xa_h, xb_h, dy_h, ea, sa, ga, eb, sb, gb, n1, n2, wq_h, wk_h, wv_h, wo_h,
                    ha_h, ua_h, hb_h, nb_h, qkv_h, ctx_h, load_h,
                    xs, wq, wk, wv, wo, nrm, nrm_t, q_t, k_t, v_t, ctx, q_b, ctx_b, hs, ua, mine, far_in, ints, gates, sems, osems, ssem, rsem, tsem):
    near, far = neighbours()
    tokens = xs.shape[0] // 2
    small = ((ea, ints.at[0]), (sa, ints.at[1]), (eb, ints.at[2]), (sb, ints.at[3]), (ga, gates.at[0]), (gb, gates.at[1]))
    tiny = [pltpu.make_async_copy(s, d, tsem.at[i]) for i, (s, d) in enumerate(small)]
    heads = kv_heads * reps
    first, second = slice(0, tokens), slice(tokens, 2 * tokens)
    half = heads * dim // 2
    moves = ((dy_h, mine.at[0:tokens]), (xa_h, xs.at[first]), (xb_h, xs.at[second]), (wk_h, wk), (wv_h, wv), (wq_h.at[0:half], wq.at[0:half]), (wq_h.at[half:], wq.at[half:]), (wo_h, wo))
    copies = [pltpu.make_async_copy(s, d, sems.at[i]) for i, (s, d) in enumerate(moves)]
    start_all(copies[0:1] + tiny + copies[1:3])
    start_all(copies[3:], 1)
    outs = []

    def flush(src, dst):
        c = pltpu.make_async_copy(src, dst, osems.at[len(outs)])
        c.start()
        outs.append(c)

    greet((near, far))
    wait_all(tiny)
    fields = [v.astype(F32) for v in (ints[0], ints[1], gates[0], ints[2], ints[3], gates[1])]
    both = jnp.concatenate([jnp.concatenate(fields[0:3], axis=1), jnp.concatenate(fields[3:6], axis=1)], axis=0)
    mine[tokens:] = jnp.concatenate([both, jnp.zeros((both.shape[0], mine.shape[1] - both.shape[1]), F32)], axis=1).astype(BF)
    copies[0].wait()
    to_far = remote(mine, far_in, ssem.at[0], rsem.at[0], far)
    to_near = remote(mine, load_h.at[1], ssem.at[1], rsem.at[1], near)
    relay = remote(far_in, load_h.at[3], ssem.at[2], rsem.at[2], near)
    to_far.start()
    to_near.start()
    flush(mine, load_h.at[0])

    wait_all(copies[1:3])
    nrm[...] = rms_rows(xs[...], row_of(n1))
    nrm_t[...] = jnp.transpose(nrm[...])
    flush(nrm.at[second], nb_h)
    copies[3].wait()
    k_t[...] = nn(wk[...], nrm_t[...]).astype(BF)
    copies[4].wait()
    v_t[...] = nn(wv[...], nrm_t[...]).astype(BF)
    for i in range(2):
        copies[5 + i].wait()
        part = slice(i * half, (i + 1) * half)
        q_t[part] = nn(wq[part], nrm_t[...]).astype(BF)
    q_b[0:heads * dim] = q_t[:, second]
    q_b[heads * dim:(heads + kv_heads) * dim] = k_t[:, second]
    q_b[(heads + kv_heads) * dim:] = v_t[:, second]
    flush(q_b, qkv_h)
    for lanes in (second, first):
        for g in range(kv_heads):
            kg = k_t[g * dim:(g + 1) * dim, lanes]
            vg = v_t[g * dim:(g + 1) * dim, lanes]
            qg = heads_to_lanes(q_t, g, reps, dim, lanes)
            probs = probs_of(tn(kg, qg) * dim ** -0.5).astype(BF)
            out = nn(vg, probs).astype(BF)
            for r in range(reps):
                ctx[(g * reps + r) * dim:(g * reps + r + 1) * dim, lanes] = out[:, r * tokens:(r + 1) * tokens]
    ctx_b[...] = ctx[:, second]
    flush(ctx_b, ctx_h)
    copies[7].wait()
    hs[...] = (xs[...].astype(F32) + tn(ctx[...], wo[...]).astype(BF).astype(F32)).astype(BF)
    to_far.wait_recv()
    relay.start()
    flush(far_in, load_h.at[2])
    flush(hs.at[first], ha_h)
    flush(hs.at[second], hb_h)
    ua[...] = rms_rows(hs[first], row_of(n2))
    flush(ua, ua_h)
    to_far.wait_send()
    to_near.wait()
    relay.wait()
    wait_all(outs)


def attn_fwd(x_a, x_b, dy, fields, n1, n2, wq, wk, wv, wo, kv_heads, reps, dim):
    tokens, model = x_a.shape
    q_dim, kv_dim = kv_heads * reps * dim, kv_heads * dim
    depth = 2 * fields[0].shape[0]
    vm = pl.BlockSpec(memory_space=pltpu.VMEM)
    hb = pl.BlockSpec(memory_space=pl.ANY)
    row = jax.ShapeDtypeStruct((tokens, model), BF)
    return pl.pallas_call(
        functools.partial(attn_fwd_kernel, kv_heads, reps, dim),
        out_shape=(row, row, row, row, jax.ShapeDtypeStruct((q_dim + 2 * kv_dim, tokens), BF), jax.ShapeDtypeStruct((q_dim, tokens), BF), jax.ShapeDtypeStruct((4, tokens + depth, model), BF)),
        in_specs=[hb] * 9 + [vm] * 2 + [hb] * 4,
        out_specs=(hb,) * 7,
        scratch_shapes=[
            pltpu.VMEM((2 * tokens, model), BF),
            pltpu.VMEM((q_dim, model), BF), pltpu.VMEM((kv_dim, model), BF), pltpu.VMEM((kv_dim, model), BF), pltpu.VMEM((q_dim, model), BF),
            pltpu.VMEM((2 * tokens, model), BF), pltpu.VMEM((model, 2 * tokens), BF),
            pltpu.VMEM((q_dim, 2 * tokens), BF), pltpu.VMEM((kv_dim, 2 * tokens), BF), pltpu.VMEM((kv_dim, 2 * tokens), BF), pltpu.VMEM((q_dim, 2 * tokens), BF),
            pltpu.VMEM((q_dim + 2 * kv_dim, tokens), BF), pltpu.VMEM((q_dim, tokens), BF), pltpu.VMEM((2 * tokens, model), BF), pltpu.VMEM((tokens, model), BF),
            pltpu.VMEM((tokens + depth, model), BF), pltpu.VMEM((tokens + depth, model), BF),
            pltpu.VMEM((4,) + fields[0].shape, jnp.int32), pltpu.VMEM((2,) + fields[2].shape, BF),
            pltpu.SemaphoreType.DMA((8,)), pltpu.SemaphoreType.DMA((8,)), pltpu.SemaphoreType.DMA((3,)), pltpu.SemaphoreType.DMA((3,)), pltpu.SemaphoreType.DMA((6,)),
        ],
        compiler_params=pltpu.CompilerParams(vmem_limit_bytes=VMEM_BYTES, collective_id=0, has_side_effects=True),
        cost_estimate=pl.CostEstimate(flops=10 ** 10, bytes_accessed=14 * 10 ** 6, transcendentals=0),
        name="attn_fwd",
    )(x_a, x_b, dy, *fields, n1, n2, wq, wk, wv, wo)


def attn_bwd_kernel(kv_heads, reps, dim, du_in, dy, h_b, x_b, nb, qkv, ctx, n1, n2, wo_h, wq_h, wk_h, wv_h, g1_in, g2_in, g3_in, u_h, hid_h, da1_h, da3_h, do_h, hid2_h, do2_h,
                    dx, gq, gk, gv, go, gn1, gn2, g1, g2, g3,
                    wo, wq, wk, wv, oq, ok, ov, oo, dctx, dq, dk, dv, u, hid, da1, da3, d_out, hid2, d_out2, o1, o2, o3, o2b, sems, osems, esems):
    last = u_h.shape[0] - 1
    extra = [pltpu.make_async_copy(s, d, esems.at[i]) for i, (s, d) in enumerate(((do_h, d_out), (hid_h, hid), (u_h.at[last], u), (da1_h, da1), (da3_h, da3), (hid2_h, hid2), (do2_h, d_out2)))]
    start_all(extra)
    copies = [pltpu.make_async_copy(s, d, sems.at[i]) for i, (s, d) in enumerate(((wo_h, wo), (wq_h, wq), (wk_h, wk), (wv_h, wv)))]
    start_all(copies, 1)
    tokens = x_b.shape[0]
    q_dim, kv_dim = kv_heads * reps * dim, kv_heads * dim
    du = du_in[...].astype(F32)
    grad_h, gain_2 = rms_pull(h_b[...].astype(F32), row_of(n2), du)
    gn2[...] = gain_2
    dh = (dy[...].astype(F32) + grad_h).astype(BF)
    outs = []

    def flush(src, dst):
        c = pltpu.make_async_copy(src, dst, osems.at[len(outs)])
        c.start()
        outs.append(c)

    wait_all(extra)
    for acts, cots, grad, which in ((hid, d_out, o2, last), (hid2, d_out2, o2b, last - 1)):
        for m in range(hid.shape[1] // 256):
            part = slice(m * 256, (m + 1) * 256)
            grad[part] = tn(acts[:, part], cots[...])
        flush(grad, g2.at[which])
    for grad, cot, dst in ((o1, da1, g1), (o3, da3, g3)):
        for m in range(u.shape[1] // 256):
            part = slice(m * 256, (m + 1) * 256)
            grad[part] = tn(u[:, part], cot[...])
        flush(grad, dst.at[last])
    copies[0].wait()
    step = q_dim // 4
    for i in range(4):
        dctx[i * step:(i + 1) * step] = nt(wo[i * step:(i + 1) * step], dh).astype(BF)
    for i in range(4):
        part = slice(i * step, (i + 1) * step)
        oo[part] = nn(ctx[part], dh).astype(BF).astype(F32)
        flush(oo.at[part], go.at[part])
    every = slice(0, tokens)
    normed = nb[...]
    for g in range(kv_heads):
        kv = slice(g * dim, (g + 1) * dim)
        kg = qkv[q_dim + g * dim:q_dim + (g + 1) * dim]
        vg = qkv[q_dim + kv_dim + g * dim:q_dim + kv_dim + (g + 1) * dim]
        qg = heads_to_lanes(qkv, g, reps, dim, every)
        dg = heads_to_lanes(dctx, g, reps, dim, every)
        probs = probs_of(tn(kg, qg) * dim ** -0.5)
        dprobs = tn(vg, dg).astype(BF).astype(F32)
        weighted = probs * dprobs
        dscores = ((weighted - probs * jnp.sum(weighted, axis=0, keepdims=True)) * dim ** -0.5).astype(BF)
        dv[kv] = nt(dg, probs.astype(BF)).astype(BF)
        dk[kv] = nt(qg, dscores).astype(BF)
        dqg = nn(kg, dscores).astype(BF)
        for r in range(reps):
            dq[(g * reps + r) * dim:(g * reps + r + 1) * dim] = dqg[:, r * tokens:(r + 1) * tokens]
        if g % 2 == 1:
            part = slice((g - 1) * reps * dim, (g + 1) * reps * dim)
            oq[part] = nn(dq[part], normed).astype(BF).astype(F32)
            flush(oq.at[part], gq.at[part])
    ok[...] = nn(dk[...], normed).astype(BF).astype(F32)
    flush(ok, gk)
    ov[...] = nn(dv[...], normed).astype(BF).astype(F32)
    flush(ov, gv)
    for c in copies[1:]:
        c.wait()
    dn = (tn(dq[...], wq[...]) + tn(dk[...], wk[...]) + tn(dv[...], wv[...])).astype(BF).astype(F32)
    grad_x, gain_1 = rms_pull(x_b[...].astype(F32), row_of(n1), dn)
    gn1[...] = gain_1
    dx[...] = (dh.astype(F32) + grad_x).astype(BF)
    for c in outs:
        c.wait()


def attn_bwd(du, dy, h_b, x_b, nb, qkv, ctx, n1, n2, wo, wq, wk, wv, grads, u, keeps, kv_heads, reps, dim):
    tokens, model = x_b.shape
    q_dim, kv_dim = kv_heads * reps * dim, kv_heads * dim
    vm = pl.BlockSpec(memory_space=pltpu.VMEM)
    hb = pl.BlockSpec(memory_space=pl.ANY)
    n_out = 4 + kv_heads // 2 + 2 + 4
    cols, ff = keeps[0].shape
    kept = pltpu.VMEM((cols, ff), BF)
    return pl.pallas_call(
        functools.partial(attn_bwd_kernel, kv_heads, reps, dim),
        out_shape=(
            jax.ShapeDtypeStruct((tokens, model), BF), jax.ShapeDtypeStruct((q_dim, model), F32), jax.ShapeDtypeStruct((kv_dim, model), F32),
            jax.ShapeDtypeStruct((kv_dim, model), F32), jax.ShapeDtypeStruct((q_dim, model), F32), jax.ShapeDtypeStruct((1, model), F32), jax.ShapeDtypeStruct((1, model), F32),
        ) + tuple(jax.ShapeDtypeStruct(g.shape, F32) for g in grads),
        in_specs=[vm] * 9 + [hb] * 14,
        out_specs=(vm, hb, hb, hb, hb, vm, vm, hb, hb, hb),
        input_output_aliases={13: 7, 14: 8, 15: 9},
        scratch_shapes=[
            pltpu.VMEM((q_dim, model), BF), pltpu.VMEM((q_dim, model), BF), pltpu.VMEM((kv_dim, model), BF), pltpu.VMEM((kv_dim, model), BF),
            pltpu.VMEM((q_dim, model), F32), pltpu.VMEM((kv_dim, model), F32), pltpu.VMEM((kv_dim, model), F32), pltpu.VMEM((q_dim, model), F32),
            pltpu.VMEM((q_dim, tokens), BF), pltpu.VMEM((q_dim, tokens), BF), pltpu.VMEM((kv_dim, tokens), BF), pltpu.VMEM((kv_dim, tokens), BF),
            pltpu.VMEM((cols, model), BF), kept, kept, kept, pltpu.VMEM((cols, model), BF), kept, pltpu.VMEM((cols, model), BF),
            pltpu.VMEM((model, ff), F32), pltpu.VMEM((ff, model), F32), pltpu.VMEM((model, ff), F32), pltpu.VMEM((ff, model), F32),
            pltpu.SemaphoreType.DMA((4,)), pltpu.SemaphoreType.DMA((n_out,)), pltpu.SemaphoreType.DMA((7,)),
        ],
        compiler_params=pltpu.CompilerParams(vmem_limit_bytes=60 * 1024 * 1024),
        cost_estimate=pl.CostEstimate(flops=14 * 10 ** 9, bytes_accessed=40 * 10 ** 6, transcendentals=0),
        name="attn_bwd",
    )(du, dy, h_b, x_b, nb, qkv, ctx, n1, n2, wo, wq, wk, wv, *grads, u, *keeps)


def route_rows(info, base, expert):
    group, _, width = info.shape
    tokens = width // 3
    top_k = info.shape[1] // 2
    wide = [info[r].astype(F32)[base * top_k:(base + 1) * top_k] for r in range(group)]

    def field(i):
        return jnp.concatenate([w[:, i * tokens:(i + 1) * tokens] for w in wide], axis=1)

    eid, slot, gate = field(0), field(1), field(2)
    hit = (eid == expert.astype(F32)) & (slot >= 0.0)
    slot_row = jnp.sum(jnp.where(hit, slot + 1.0, 0.0), axis=0, keepdims=True) - 1.0
    gate_row = jnp.sum(jnp.where(hit, gate, 0.0), axis=0, keepdims=True)
    return slot_row, gate_row


def ring_copies(pairs, sem, idx, ring):
    s = lax.rem(idx, ring)
    return [pltpu.make_async_copy(src.at[idx], dst.at[s], sem.at[s, i]) for i, (src, dst) in enumerate(pairs)]


def row_copies(refs, rows, sem):
    tokens = rows.shape[0] // len(refs)
    return [pltpu.make_async_copy(ref.at[0:tokens], rows.at[r * tokens:(r + 1) * tokens], sem.at[r]) for r, ref in enumerate(refs)]


def info_copy(load, info, sem):
    depth, width = info.shape
    first = load.shape[0] - depth
    return pltpu.make_async_copy(load.at[first:first + depth, 0:width], info, sem)


def hits(slot_row, tokens, capacity):
    source = lax.broadcasted_iota(jnp.int32, slot_row.shape, 1) // tokens
    col_row = jnp.where(slot_row >= 0.0, slot_row.astype(jnp.int32) + source * capacity, -1)
    return lax.broadcasted_iota(jnp.int32, (4 * capacity, slot_row.shape[1]), 0) == col_row


def start_all(copies, priority=0):
    for c in copies:
        c.start(priority=priority)


def wait_all(copies):
    for c in copies:
        c.wait()


def keep_routes(slots, gates, q, slot_row, gate_row):
    slots[pl.ds(q, 1), :] = slot_row
    gates[pl.ds(q, 1), :] = gate_row


def stash(outs, q, capacity, lanes, res):
    for r in range(outs.shape[0]):
        outs[r, pl.ds(pl.multiple_of(q * BLOCK, BLOCK), capacity), lanes] = res[r * capacity:(r + 1) * capacity].astype(BF)


def mix_into(acc, outs, slots, gates, q, weighted, order=(0, 1, 2, 3), after=lambda r: None):
    tokens = acc.shape[0] // outs.shape[0]
    depth = lax.broadcasted_iota(jnp.int32, (BLOCK, tokens), 0).astype(F32)
    for r in order:
        lanes = slice(r * tokens, (r + 1) * tokens)
        blocks = []
        for k in range(QUAD):
            weight = gates[k:k + 1, lanes] if weighted else 1.0
            slot = jnp.where(q >= k, slots[k:k + 1, lanes], -1.0)
            blocks.append(jnp.where(depth == slot, weight, 0.0))
        pick = jnp.transpose(jnp.concatenate(blocks, axis=0).astype(BF))
        for n in range(acc.shape[1] // 512):
            part = slice(n * 512, (n + 1) * 512)
            acc[lanes, part] += nn(pick, outs[r, :, part])
        after(r)


def expert_bwd_kernel(capacity, loads, u_h, w1_h, w2_h, w3_h,
                      g1, g2, g3, p0, p1, p2, p3, s_hid, s_da1, s_da3, s_do, s_hid2, s_do2,
                      rows, info, us, w1s, w2s, w3s, slots, gates, du_all, d_out, hid, da1, da3, o1, o2, o3, acc, rsem, wsem, sems, psem, ksem):
    e = pl.program_id(0)
    count = pl.num_programs(0)
    me = lax.axis_index('expert')
    slot_e = lax.rem(e, 2)
    ring, _, model = us.shape
    tokens = rows.shape[0] // 4
    ff = w1s.shape[2]
    order = [jnp.bitwise_xor(me, r) for r in range(4)]
    arrivals = row_copies([loads.at[p] for p in order], rows, rsem) + [info_copy(loads.at[p], info.at[r], rsem.at[4 + r]) for r, p in enumerate(order)]
    pairs = ((u_h, us), (w1_h, w1s), (w3_h, w3s), (w2_h, w2s))

    @pl.when(e == 0)
    def _():
        start_all(arrivals + ring_copies(pairs, wsem, 0, ring) + ring_copies(pairs, wsem, 1, ring))
        acc[...] = jnp.zeros_like(acc)
        du_all[...] = jnp.zeros_like(du_all)
        wait_all(arrivals)

    @pl.when(e + 2 < count)
    def _():
        start_all(ring_copies(pairs, wsem, e + 2, ring))

    slot_row, gate_row = route_rows(info, 1, me * count + e)
    early = [pltpu.make_async_copy(src, dst, ksem.at[4 + i]) for i, (src, dst) in enumerate(((hid, s_hid2), (d_out, s_do2)))]

    @pl.when(e == count - 1)
    def _():
        wait_all(early)

    q = lax.rem(e, QUAD)
    keep_routes(slots, gates, q, slot_row, gate_row)
    hot = hits(slot_row, tokens, capacity)
    d_out[...] = nn(jnp.where(hot, gate_row, 0.0).astype(BF), rows[...]).astype(BF)

    def flush(idx):
        s = lax.rem(idx, 2)
        return [pltpu.make_async_copy(src.at[s], dst.at[idx], sems.at[s, i]) for i, (src, dst) in enumerate(((o1, g1), (o2, g2), (o3, g3)))]

    wait_all(ring_copies(pairs, wsem, e, ring))
    now = lax.rem(e, ring)
    u, w1, w2, w3 = us.at[now], w1s.at[now], w2s.at[now], w3s.at[now]
    uv = u[...]
    dov = d_out[...]
    for n in range(ff // 256):
        part = slice(n * 256, (n + 1) * 256)
        pre1 = nn(uv, w1[:, part]).astype(BF).astype(F32)
        pre3 = nn(uv, w3[:, part]).astype(BF).astype(F32)
        grad_hid = nt(dov, w2[part, :]).astype(BF).astype(F32)
        sigma = jax.nn.sigmoid(pre1)
        silu = pre1 * sigma
        hid[:, part] = (silu * pre3).astype(BF)
        da1[:, part] = (grad_hid * pre3 * sigma * (1.0 + pre1 * (1.0 - sigma))).astype(BF)
        da3[:, part] = (grad_hid * silu).astype(BF)

    keeps = [pltpu.make_async_copy(src, dst, ksem.at[i]) for i, (src, dst) in enumerate(((hid, s_hid), (da1, s_da1), (da3, s_da3), (d_out, s_do)))]

    @pl.when((e >= 2) & (e < count - 1))
    def _():
        wait_all(flush(e - 2))

    @pl.when(e < count - 1)
    def _():
        fresh = flush(e)

        @pl.when(e < count - 2)
        def _():
            for m in range(ff // 256):
                part = slice(m * 256, (m + 1) * 256)
                o2[slot_e, part] = tn(hid[:, part], d_out[...])
            fresh[1].start()

        @pl.when(e == count - 2)
        def _():
            start_all(early)

        for m in range(model // 256):
            part = slice(m * 256, (m + 1) * 256)
            o1[slot_e, part] = tn(u[:, part], da1[...])
        fresh[0].start()
        for m in range(model // 256):
            part = slice(m * 256, (m + 1) * 256)
            o3[slot_e, part] = tn(u[:, part], da3[...])
        fresh[2].start()

    @pl.when(e == count - 1)
    def _():
        start_all(keeps)

    for n in range(model // 256):
        part = slice(n * 256, (n + 1) * 256)
        stash(du_all, q, capacity, part, nt(da1[...], w1[part]) + nt(da3[...], w3[part]))

    @pl.when((q == QUAD - 1) | (e == count - 1))
    def _():
        mix_into(acc, du_all, slots, gates, q, False)

    @pl.when(e == count - 1)
    def _():
        sends = [pltpu.make_async_copy(acc.at[pl.ds(pl.multiple_of(p * tokens, tokens), tokens)], ref, psem.at[r]) for r, (p, ref) in enumerate(zip(order, (p0, p1, p2, p3)))]
        start_all(sends)
        wait_all(keeps)
        wait_all(flush(e - 2))
        wait_all(flush(e - 1)[0:3:2])
        wait_all(sends)


def expert_bwd(loads, u, w1, w2, w3, tokens):
    model = loads.shape[2]
    count, cols, _ = u.shape
    ff = w1.shape[2]
    ring = 3
    hb = pl.BlockSpec(memory_space=pl.ANY)
    keep, keep_do = jax.ShapeDtypeStruct((cols, ff), BF), jax.ShapeDtypeStruct((cols, model), BF)
    part = jax.ShapeDtypeStruct((tokens, model), F32)
    return pl.pallas_call(
        functools.partial(expert_bwd_kernel, cols // 4),
        grid=(count,),
        out_shape=(jax.ShapeDtypeStruct((count, model, ff), F32), jax.ShapeDtypeStruct((count, ff, model), F32), jax.ShapeDtypeStruct((count, model, ff), F32), part, part, part, part, keep, keep, keep, keep_do, keep, keep_do),
        in_specs=[hb] * 5,
        out_specs=(hb,) * 13,
        scratch_shapes=[
            pltpu.VMEM((4 * tokens, model), BF), pltpu.VMEM((4, loads.shape[1] - tokens, 3 * tokens), BF),
            pltpu.VMEM((ring, cols, model), BF), pltpu.VMEM((ring, model, ff), BF), pltpu.VMEM((ring, ff, model), BF), pltpu.VMEM((ring, model, ff), BF),
            pltpu.VMEM((8, 4 * tokens), F32), pltpu.VMEM((8, 4 * tokens), F32), pltpu.VMEM((4, QUAD * BLOCK, model), BF),
            pltpu.VMEM((cols, model), BF), pltpu.VMEM((cols, ff), BF), pltpu.VMEM((cols, ff), BF), pltpu.VMEM((cols, ff), BF),
            pltpu.VMEM((2, model, ff), F32), pltpu.VMEM((2, ff, model), F32), pltpu.VMEM((2, model, ff), F32),
            pltpu.VMEM((4 * tokens, model), F32),
            pltpu.SemaphoreType.DMA((8,)), pltpu.SemaphoreType.DMA((ring, 4)), pltpu.SemaphoreType.DMA((2, 3)), pltpu.SemaphoreType.DMA((4,)), pltpu.SemaphoreType.DMA((6,)),
        ],
        compiler_params=pltpu.CompilerParams(vmem_limit_bytes=VMEM_BYTES, dimension_semantics=("arbitrary",)),
        cost_estimate=pl.CostEstimate(flops=50 * 10 ** 9, bytes_accessed=150 * 10 ** 6, transcendentals=0),
        name="expert_bwd",
    )(loads, u, w1, w2, w3)


def expert_fwd_kernel(capacity, u0, u1, u2, u3, loads, b0, b1, b2, b3, w1_h, w2_h, w3_h, du_o, mine_o, out_o,
                      rows, info, w1s, w2s, w3s, slots, gates, out_all, acc, loc0, loc2, rx1, rx3, rxf, ra1, ra3, dus, rsem, wsem, bsem, ssem, xsem, osem):
    e = pl.program_id(0)
    count = pl.num_programs(0)
    me = lax.axis_index('expert')
    near, far = neighbours()
    ring, model, ff = w1s.shape
    q = e % QUAD
    tokens = rows.shape[0] // 4
    arrivals = row_copies((u0, u1, u2, u3), rows, rsem) + [info_copy(loads.at[r], info.at[r], rsem.at[4 + r]) for r in range(4)]
    pairs = ((w1_h, w1s), (w3_h, w3s), (w2_h, w2s))
    local = [pltpu.make_async_copy(b0, loc0, bsem.at[0]), pltpu.make_async_copy(b2, loc2, bsem.at[1])]
    swap3 = remote(b3, rx3, ssem.at[0], xsem.at[0], near)
    swap1 = remote(b1, rx1, ssem.at[1], xsem.at[1], near)
    over = remote(loc2, rxf, ssem.at[2], xsem.at[2], far)
    part = [slice(r * tokens, (r + 1) * tokens) for r in range(4)]
    late3 = remote(acc.at[part[3]], ra3, ssem.at[3], xsem.at[3], near)
    late1 = remote(acc.at[part[1]], ra1, ssem.at[4], xsem.at[4], near)

    @pl.when(e == 0)
    def _():
        start_all(arrivals + local)
        start_all(ring_copies(pairs, wsem, 0, ring) + ring_copies(pairs, wsem, 1, ring), 1)
        greet((near, far))
        swap3.start()
        acc[...] = jnp.zeros_like(acc)
        out_all[...] = jnp.zeros_like(out_all)
        wait_all(arrivals)

    @pl.when(e == 1)
    def _():
        wait_all(local)
        swap3.wait()
        loc2[...] += rx3[...]
        over.start()
        swap1.start()

    @pl.when(e + 2 < count)
    def _():
        start_all(ring_copies(pairs, wsem, e + 2, ring), 1)

    slot_row, gate_row = route_rows(info, 0, me * count + e)
    keep_routes(slots, gates, q, slot_row, gate_row)
    v = nn(jnp.where(hits(slot_row, tokens, capacity), 1.0, 0.0).astype(BF), rows[...]).astype(BF)
    wait_all(ring_copies(pairs, wsem, e, ring))
    now = e % ring
    w1, w2, w3 = w1s.at[now], w2s.at[now], w3s.at[now]
    pieces = []
    for n in range(ff // 256):
        lanes = slice(n * 256, (n + 1) * 256)
        a1 = nn(v, w1[:, lanes]).astype(BF).astype(F32)
        a3 = nn(v, w3[:, lanes]).astype(BF).astype(F32)
        pieces.append((a1 * jax.nn.sigmoid(a1) * a3).astype(BF))
    hidden = jnp.concatenate(pieces, axis=1)
    for n in range(model // 256):
        lanes = slice(n * 256, (n + 1) * 256)
        stash(out_all, q, capacity, lanes, nn(hidden, w2[:, lanes]))

    @pl.when((q == QUAD - 1) & (e < count - 1))
    def _():
        mix_into(acc, out_all, slots, gates, q, True)

    @pl.when(e == count - 1)
    def _():
        late = {3: late3, 1: late1}
        mix_into(acc, out_all, slots, gates, q, True, (3, 1, 2, 0), lambda r: late[r].start() if r in late else None)
        moves = [pltpu.make_async_copy(src, dst, osem.at[i]) for i, (src, dst) in enumerate(((dus, du_o), (loc2, out_o), (loc0, mine_o)))]
        swap1.wait()
        over.wait()
        dus[...] = ((loc0[...] + rx1[...]) + rxf[...]).astype(BF)
        moves[0].start()
        late3.wait()
        loc2[...] = acc[part[2]] + ra3[...]
        moves[1].start()
        late1.wait()
        loc0[...] = acc[part[0]] + ra1[...]
        moves[2].start()
        wait_all(moves)


def expert_fwd(us, loads, sums, w1, w2, w3, capacity):
    tokens, model = us[0].shape
    count, _, ff = w1.shape
    ring = 3
    part = jax.ShapeDtypeStruct((tokens, model), F32)
    hb = pl.BlockSpec(memory_space=pl.ANY)
    tile = pltpu.VMEM((tokens, model), F32)
    return pl.pallas_call(
        functools.partial(expert_fwd_kernel, capacity),
        grid=(count,),
        out_shape=(jax.ShapeDtypeStruct((tokens, model), BF), part, part),
        in_specs=[hb] * 12,
        out_specs=(hb,) * 3,
        scratch_shapes=[
            pltpu.VMEM((4 * tokens, model), BF), pltpu.VMEM((4, loads.shape[1] - tokens, 3 * tokens), BF),
            pltpu.VMEM((ring, model, ff), BF), pltpu.VMEM((ring, ff, model), BF), pltpu.VMEM((ring, model, ff), BF),
            pltpu.VMEM((8, 4 * tokens), F32), pltpu.VMEM((8, 4 * tokens), F32), pltpu.VMEM((4, QUAD * BLOCK, model), BF), pltpu.VMEM((4 * tokens, model), F32),
            tile, tile, tile, tile, tile, tile, tile, pltpu.VMEM((tokens, model), BF),
            pltpu.SemaphoreType.DMA((8,)), pltpu.SemaphoreType.DMA((ring, 3)), pltpu.SemaphoreType.DMA((2,)), pltpu.SemaphoreType.DMA((5,)), pltpu.SemaphoreType.DMA((5,)), pltpu.SemaphoreType.DMA((3,)),
        ],
        compiler_params=pltpu.CompilerParams(vmem_limit_bytes=VMEM_BYTES, dimension_semantics=("arbitrary",), collective_id=1, has_side_effects=True),
        cost_estimate=pl.CostEstimate(flops=16 * 10 ** 9, bytes_accessed=50 * 10 ** 6, transcendentals=0),
        name="expert_fwd",
    )(*us, loads, *sums, w1, w2, w3)


def solution(mesh):
    group = mesh.shape['expert']

    def hop(value, bits):
        return lax.ppermute(value, 'expert', [(i, i ^ bits) for i in range(group)])

    def local_step(x_a, x_b, dy_b, eid_a, slot_a, gate_a, eid_b, slot_b, gate_b, u_b, norm_1, norm_2, w_q, w_k, w_v, w_o, w_1, w_2, w_3):
        model, heads, dim = w_q.shape
        kv_heads = w_k.shape[1]
        reps = heads // kv_heads
        wq_t, wk_t, wv_t = (w.transpose(1, 2, 0).reshape(-1, model) for w in (w_q, w_k, w_v))
        wo = w_o.reshape(-1, model)
        fields = [a.T for a in (eid_a, slot_a, gate_a, eid_b, slot_b, gate_b)]
        h_a, u_a, h_b, nb, qkv_b, ctx_b, loads = attn_fwd(x_a, x_b, dy_b, fields, norm_1, norm_2, wq_t, wk_t, wv_t, wo, kv_heads, reps, dim)
        us = (u_a, hop(u_a, 1), hop(u_a, 2), hop(u_a, 3))
        g1, g2, g3, *rest = expert_bwd(loads, u_b, w_1, w_2, w_3, x_a.shape[0])
        du, mine_a, out_a = expert_fwd(us, loads, rest[0:4], w_1, w_2, w_3, u_b.shape[1] // group)
        far_a = hop(out_a, 2)
        dx_b, g_q, g_k, g_v, g_o, g_n1, g_n2, g1, g2, g3 = attn_bwd(du, dy_b, h_b, x_b, nb, qkv_b, ctx_b, norm_1, norm_2, wo, wq_t, wk_t, wv_t, (g1, g2, g3), u_b, rest[4:10], kv_heads, reps, dim)
        y_a = (h_a.astype(F32) + (mine_a + far_a)).astype(BF)
        g_q = g_q.reshape(heads, dim, model).transpose(2, 0, 1)
        g_k = g_k.reshape(kv_heads, dim, model).transpose(2, 0, 1)
        g_v = g_v.reshape(kv_heads, dim, model).transpose(2, 0, 1)
        g_o = g_o.reshape(heads, dim, model)
        return (y_a, dx_b, g1, g2, g3, g_q[None], g_k[None], g_v[None], g_o[None], g_n1, g_n2)

    row_spec = P(('data', 'expert'), None)
    cube_spec = P(('data', 'expert'), None, None)
    quad_spec = P(('data', 'expert'), None, None, None)
    expert_spec = P('expert', None, None)
    in_specs = (row_spec, row_spec, row_spec, row_spec, row_spec, row_spec, row_spec, row_spec, row_spec, cube_spec, P(), P(), P(), P(), P(), P(), expert_spec, expert_spec, expert_spec)
    out_specs = (row_spec, row_spec, cube_spec, cube_spec, cube_spec, quad_spec, quad_spec, quad_spec, quad_spec, row_spec, row_spec)
    return jax.shard_map(local_step, mesh=mesh, in_specs=in_specs, out_specs=out_specs, check_vma=False)
```

```python
import functools

import jax
import jax.numpy as jnp
from jax import lax
from jax.experimental import pallas as pl
from jax.experimental.pallas import tpu as pltpu
from jax.sharding import PartitionSpec as P


NORM_EPS = 1e-6
BF = jnp.bfloat16
F32 = jnp.float32
VMEM_BYTES = 67043328
QUAD = 4
BLOCK = 64


def nn(a, b):
    return lax.dot_general(a, b, (((1,), (0,)), ((), ())), preferred_element_type=F32)


def nt(a, b):
    return lax.dot_general(a, b, (((1,), (1,)), ((), ())), preferred_element_type=F32)


def tn(a, b):
    return lax.dot_general(a, b, (((0,), (0,)), ((), ())), preferred_element_type=F32)


def row_of(ref):
    return ref[...].astype(F32).reshape(1, ref.shape[0])


def rms_scale(wide):
    return lax.rsqrt(jnp.mean(wide * wide, axis=-1, keepdims=True) + NORM_EPS)


def rms_rows(values, gain):
    wide = values.astype(F32)
    return (wide * rms_scale(wide) * gain).astype(BF)


def rms_pull(wide, gain, cot):
    scale = rms_scale(wide)
    scaled = wide * scale
    grad_gain = jnp.sum(cot * scaled, axis=0, keepdims=True).astype(BF).astype(F32)
    inner = cot * gain
    pull = jnp.mean(inner * wide, axis=-1, keepdims=True)
    grad = scale * inner - scaled * (scale * scale * pull)
    return grad.astype(BF).astype(F32), grad_gain


def probs_of(scores_t):
    rows = lax.broadcasted_iota(jnp.int32, scores_t.shape, 0)
    cols = lax.broadcasted_iota(jnp.int32, scores_t.shape, 1) % scores_t.shape[0]
    masked = jnp.where(rows <= cols, scores_t, -1e30)
    top = jnp.max(masked, axis=0, keepdims=True)
    unnorm = jnp.exp(masked - top)
    return unnorm / jnp.sum(unnorm, axis=0, keepdims=True)


def heads_to_lanes(ref, group, reps, dim, lanes):
    return jnp.concatenate([ref[(group * reps + r) * dim:(group * reps + r + 1) * dim, lanes] for r in range(reps)], axis=1)


def neighbours():
    me = lax.axis_index('expert')
    return me + 1 - 2 * (me % 2), (me + 2) % 4


def greet(peers):
    barrier = pltpu.get_barrier_semaphore()
    for peer in peers:
        pl.semaphore_signal(barrier, inc=1, device_id={'expert': peer}, device_id_type=pl.DeviceIdType.MESH)
    pl.semaphore_wait(barrier, len(peers))


def remote(src, dst, send, recv, peer):
    return pltpu.make_async_remote_copy(src_ref=src, dst_ref=dst, send_sem=send, recv_sem=recv, device_id={'expert': peer}, device_id_type=pl.DeviceIdType.MESH)


def attn_fwd_kernel(kv_heads, reps, dim, xa_h, xb_h, dy_h, ea, sa, ga, eb, sb, gb, n1, n2, wq_h, wk_h, wv_h, wo_h,
                    ha_h, ua_h, hb_h, nb_h, qkv_h, ctx_h, load_h,
                    xs, wq, wk, wv, wo, nrm, nrm_t, q_t, k_t, v_t, ctx, q_b, ctx_b, hs, ua, mine, far_in, ints, gates, sems, osems, ssem, rsem, tsem):
    near, far = neighbours()
    tokens = xs.shape[0] // 2
    small = ((ea, ints.at[0]), (sa, ints.at[1]), (eb, ints.at[2]), (sb, ints.at[3]), (ga, gates.at[0]), (gb, gates.at[1]))
    tiny = [pltpu.make_async_copy(s, d, tsem.at[i]) for i, (s, d) in enumerate(small)]
    heads = kv_heads * reps
    first, second = slice(0, tokens), slice(tokens, 2 * tokens)
    half = heads * dim // 2
    moves = ((dy_h, mine.at[0:tokens]), (xa_h, xs.at[first]), (xb_h, xs.at[second]), (wk_h, wk), (wv_h, wv), (wq_h.at[0:half], wq.at[0:half]), (wq_h.at[half:], wq.at[half:]), (wo_h, wo))
    copies = [pltpu.make_async_copy(s, d, sems.at[i]) for i, (s, d) in enumerate(moves)]
    start_all(copies[0:1] + tiny + copies[1:3])
    start_all(copies[3:], 1)
    outs = []

    def flush(src, dst):
        c = pltpu.make_async_copy(src, dst, osems.at[len(outs)])
        c.start()
        outs.append(c)

    greet((near, far))
    wait_all(tiny)
    fields = [v.astype(F32) for v in (ints[0], ints[1], gates[0], ints[2], ints[3], gates[1])]
    both = jnp.concatenate([jnp.concatenate(fields[0:3], axis=1), jnp.concatenate(fields[3:6], axis=1)], axis=0)
    mine[tokens:] = jnp.concatenate([both, jnp.zeros((both.shape[0], mine.shape[1] - both.shape[1]), F32)], axis=1).astype(BF)
    copies[0].wait()
    to_far = remote(mine, far_in, ssem.at[0], rsem.at[0], far)
    to_near = remote(mine, load_h.at[1], ssem.at[1], rsem.at[1], near)
    relay = remote(far_in, load_h.at[3], ssem.at[2], rsem.at[2], near)
    to_far.start()
    to_near.start()
    flush(mine, load_h.at[0])

    wait_all(copies[1:3])
    nrm[...] = rms_rows(xs[...], row_of(n1))
    nrm_t[...] = jnp.transpose(nrm[...])
    flush(nrm.at[second], nb_h)
    copies[3].wait()
    k_t[...] = nn(wk[...], nrm_t[...]).astype(BF)
    copies[4].wait()
    v_t[...] = nn(wv[...], nrm_t[...]).astype(BF)
    for i in range(2):
        copies[5 + i].wait()
        part = slice(i * half, (i + 1) * half)
        q_t[part] = nn(wq[part], nrm_t[...]).astype(BF)
    q_b[0:heads * dim] = q_t[:, second]
    q_b[heads * dim:(heads + kv_heads) * dim] = k_t[:, second]
    q_b[(heads + kv_heads) * dim:] = v_t[:, second]
    flush(q_b, qkv_h)
    for lanes in (second, first):
        for g in range(kv_heads):
            kg = k_t[g * dim:(g + 1) * dim, lanes]
            vg = v_t[g * dim:(g + 1) * dim, lanes]
            qg = heads_to_lanes(q_t, g, reps, dim, lanes)
            probs = probs_of(tn(kg, qg) * dim ** -0.5).astype(BF)
            out = nn(vg, probs).astype(BF)
            for r in range(reps):
                ctx[(g * reps + r) * dim:(g * reps + r + 1) * dim, lanes] = out[:, r * tokens:(r + 1) * tokens]
    ctx_b[...] = ctx[:, second]
    flush(ctx_b, ctx_h)
    copies[7].wait()
    hs[...] = (xs[...].astype(F32) + tn(ctx[...], wo[...]).astype(BF).astype(F32)).astype(BF)
    to_far.wait_recv()
    relay.start()
    flush(far_in, load_h.at[2])
    flush(hs.at[first], ha_h)
    flush(hs.at[second], hb_h)
    ua[...] = rms_rows(hs[first], row_of(n2))
    flush(ua, ua_h)
    to_far.wait_send()
    to_near.wait()
    relay.wait()
    wait_all(outs)


def attn_fwd(x_a, x_b, dy, fields, n1, n2, wq, wk, wv, wo, kv_heads, reps, dim):
    tokens, model = x_a.shape
    q_dim, kv_dim = kv_heads * reps * dim, kv_heads * dim
    depth = 2 * fields[0].shape[0]
    vm = pl.BlockSpec(memory_space=pltpu.VMEM)
    hb = pl.BlockSpec(memory_space=pl.ANY)
    row = jax.ShapeDtypeStruct((tokens, model), BF)
    return pl.pallas_call(
        functools.partial(attn_fwd_kernel, kv_heads, reps, dim),
        out_shape=(row, row, row, row, jax.ShapeDtypeStruct((q_dim + 2 * kv_dim, tokens), BF), jax.ShapeDtypeStruct((q_dim, tokens), BF), jax.ShapeDtypeStruct((4, tokens + depth, model), BF)),
        in_specs=[hb] * 9 + [vm] * 2 + [hb] * 4,
        out_specs=(hb,) * 7,
        scratch_shapes=[
            pltpu.VMEM((2 * tokens, model), BF),
            pltpu.VMEM((q_dim, model), BF), pltpu.VMEM((kv_dim, model), BF), pltpu.VMEM((kv_dim, model), BF), pltpu.VMEM((q_dim, model), BF),
            pltpu.VMEM((2 * tokens, model), BF), pltpu.VMEM((model, 2 * tokens), BF),
            pltpu.VMEM((q_dim, 2 * tokens), BF), pltpu.VMEM((kv_dim, 2 * tokens), BF), pltpu.VMEM((kv_dim, 2 * tokens), BF), pltpu.VMEM((q_dim, 2 * tokens), BF),
            pltpu.VMEM((q_dim + 2 * kv_dim, tokens), BF), pltpu.VMEM((q_dim, tokens), BF), pltpu.VMEM((2 * tokens, model), BF), pltpu.VMEM((tokens, model), BF),
            pltpu.VMEM((tokens + depth, model), BF), pltpu.VMEM((tokens + depth, model), BF),
            pltpu.VMEM((4,) + fields[0].shape, jnp.int32), pltpu.VMEM((2,) + fields[2].shape, BF),
            pltpu.SemaphoreType.DMA((8,)), pltpu.SemaphoreType.DMA((8,)), pltpu.SemaphoreType.DMA((3,)), pltpu.SemaphoreType.DMA((3,)), pltpu.SemaphoreType.DMA((6,)),
        ],
        compiler_params=pltpu.CompilerParams(vmem_limit_bytes=VMEM_BYTES, collective_id=0, has_side_effects=True),
        cost_estimate=pl.CostEstimate(flops=10 ** 10, bytes_accessed=14 * 10 ** 6, transcendentals=0),
        name="attn_fwd",
    )(x_a, x_b, dy, *fields, n1, n2, wq, wk, wv, wo)


def attn_bwd_kernel(kv_heads, reps, dim, du_in, dy, h_b, x_b, nb, qkv, ctx, n1, n2, wo_h, wq_h, wk_h, wv_h, g1_in, g2_in, g3_in, u_h, hid_h, da1_h, da3_h, do_h,
                    dx, gq, gk, gv, go, gn1, gn2, g1, g2, g3,
                    wo, wq, wk, wv, oq, ok, ov, oo, dctx, dq, dk, dv, u, hid, da1, da3, d_out, o1, o2, o3, sems, osems, esems):
    last = u_h.shape[0] - 1
    extra = [pltpu.make_async_copy(s, d, esems.at[i]) for i, (s, d) in enumerate(((do_h, d_out), (hid_h, hid), (u_h.at[last], u), (da1_h, da1), (da3_h, da3)))]
    start_all(extra)
    copies = [pltpu.make_async_copy(s, d, sems.at[i]) for i, (s, d) in enumerate(((wo_h, wo), (wq_h, wq), (wk_h, wk), (wv_h, wv)))]
    start_all(copies, 1)
    tokens = x_b.shape[0]
    q_dim, kv_dim = kv_heads * reps * dim, kv_heads * dim
    du = du_in[...].astype(F32)
    grad_h, gain_2 = rms_pull(h_b[...].astype(F32), row_of(n2), du)
    gn2[...] = gain_2
    dh = (dy[...].astype(F32) + grad_h).astype(BF)
    outs = []

    def flush(src, dst):
        c = pltpu.make_async_copy(src, dst, osems.at[len(outs)])
        c.start()
        outs.append(c)

    wait_all(extra)
    for m in range(hid.shape[1] // 256):
        part = slice(m * 256, (m + 1) * 256)
        o2[part] = tn(hid[:, part], d_out[...])
    flush(o2, g2.at[last])
    for grad, cot, dst in ((o1, da1, g1), (o3, da3, g3)):
        for m in range(u.shape[1] // 256):
            part = slice(m * 256, (m + 1) * 256)
            grad[part] = tn(u[:, part], cot[...])
        flush(grad, dst.at[last])
    copies[0].wait()
    step = q_dim // 4
    for i in range(4):
        dctx[i * step:(i + 1) * step] = nt(wo[i * step:(i + 1) * step], dh).astype(BF)
    for i in range(4):
        part = slice(i * step, (i + 1) * step)
        oo[part] = nn(ctx[part], dh).astype(BF).astype(F32)
        flush(oo.at[part], go.at[part])
    every = slice(0, tokens)
    normed = nb[...]
    for g in range(kv_heads):
        kv = slice(g * dim, (g + 1) * dim)
        kg = qkv[q_dim + g * dim:q_dim + (g + 1) * dim]
        vg = qkv[q_dim + kv_dim + g * dim:q_dim + kv_dim + (g + 1) * dim]
        qg = heads_to_lanes(qkv, g, reps, dim, every)
        dg = heads_to_lanes(dctx, g, reps, dim, every)
        probs = probs_of(tn(kg, qg) * dim ** -0.5)
        dprobs = tn(vg, dg).astype(BF).astype(F32)
        weighted = probs * dprobs
        dscores = ((weighted - probs * jnp.sum(weighted, axis=0, keepdims=True)) * dim ** -0.5).astype(BF)
        dv[kv] = nt(dg, probs.astype(BF)).astype(BF)
        dk[kv] = nt(qg, dscores).astype(BF)
        dqg = nn(kg, dscores).astype(BF)
        for r in range(reps):
            dq[(g * reps + r) * dim:(g * reps + r + 1) * dim] = dqg[:, r * tokens:(r + 1) * tokens]
        if g % 2 == 1:
            part = slice((g - 1) * reps * dim, (g + 1) * reps * dim)
            oq[part] = nn(dq[part], normed).astype(BF).astype(F32)
            flush(oq.at[part], gq.at[part])
    ok[...] = nn(dk[...], normed).astype(BF).astype(F32)
    flush(ok, gk)
    ov[...] = nn(dv[...], normed).astype(BF).astype(F32)
    flush(ov, gv)
    for c in copies[1:]:
        c.wait()
    dn = (tn(dq[...], wq[...]) + tn(dk[...], wk[...]) + tn(dv[...], wv[...])).astype(BF).astype(F32)
    grad_x, gain_1 = rms_pull(x_b[...].astype(F32), row_of(n1), dn)
    gn1[...] = gain_1
    dx[...] = (dh.astype(F32) + grad_x).astype(BF)
    for c in outs:
        c.wait()


def attn_bwd(du, dy, h_b, x_b, nb, qkv, ctx, n1, n2, wo, wq, wk, wv, grads, u, keeps, kv_heads, reps, dim):
    tokens, model = x_b.shape
    q_dim, kv_dim = kv_heads * reps * dim, kv_heads * dim
    vm = pl.BlockSpec(memory_space=pltpu.VMEM)
    hb = pl.BlockSpec(memory_space=pl.ANY)
    n_out = 4 + kv_heads // 2 + 2 + 3
    cols, ff = keeps[0].shape
    kept = pltpu.VMEM((cols, ff), BF)
    return pl.pallas_call(
        functools.partial(attn_bwd_kernel, kv_heads, reps, dim),
        out_shape=(
            jax.ShapeDtypeStruct((tokens, model), BF), jax.ShapeDtypeStruct((q_dim, model), F32), jax.ShapeDtypeStruct((kv_dim, model), F32),
            jax.ShapeDtypeStruct((kv_dim, model), F32), jax.ShapeDtypeStruct((q_dim, model), F32), jax.ShapeDtypeStruct((1, model), F32), jax.ShapeDtypeStruct((1, model), F32),
        ) + tuple(jax.ShapeDtypeStruct(g.shape, F32) for g in grads),
        in_specs=[vm] * 9 + [hb] * 12,
        out_specs=(vm, hb, hb, hb, hb, vm, vm, hb, hb, hb),
        input_output_aliases={13: 7, 14: 8, 15: 9},
        scratch_shapes=[
            pltpu.VMEM((q_dim, model), BF), pltpu.VMEM((q_dim, model), BF), pltpu.VMEM((kv_dim, model), BF), pltpu.VMEM((kv_dim, model), BF),
            pltpu.VMEM((q_dim, model), F32), pltpu.VMEM((kv_dim, model), F32), pltpu.VMEM((kv_dim, model), F32), pltpu.VMEM((q_dim, model), F32),
            pltpu.VMEM((q_dim, tokens), BF), pltpu.VMEM((q_dim, tokens), BF), pltpu.VMEM((kv_dim, tokens), BF), pltpu.VMEM((kv_dim, tokens), BF),
            pltpu.VMEM((cols, model), BF), kept, kept, kept, pltpu.VMEM((cols, model), BF), pltpu.VMEM((model, ff), F32), pltpu.VMEM((ff, model), F32), pltpu.VMEM((model, ff), F32),
            pltpu.SemaphoreType.DMA((4,)), pltpu.SemaphoreType.DMA((n_out,)), pltpu.SemaphoreType.DMA((5,)),
        ],
        compiler_params=pltpu.CompilerParams(vmem_limit_bytes=60 * 1024 * 1024),
        cost_estimate=pl.CostEstimate(flops=14 * 10 ** 9, bytes_accessed=40 * 10 ** 6, transcendentals=0),
        name="attn_bwd",
    )(du, dy, h_b, x_b, nb, qkv, ctx, n1, n2, wo, wq, wk, wv, *grads, u, *keeps)


def route_rows(info, base, expert):
    group, _, width = info.shape
    tokens = width // 3
    top_k = info.shape[1] // 2
    wide = [info[r].astype(F32)[base * top_k:(base + 1) * top_k] for r in range(group)]

    def field(i):
        return jnp.concatenate([w[:, i * tokens:(i + 1) * tokens] for w in wide], axis=1)

    eid, slot, gate = field(0), field(1), field(2)
    hit = (eid == expert.astype(F32)) & (slot >= 0.0)
    slot_row = jnp.sum(jnp.where(hit, slot + 1.0, 0.0), axis=0, keepdims=True) - 1.0
    gate_row = jnp.sum(jnp.where(hit, gate, 0.0), axis=0, keepdims=True)
    return slot_row, gate_row


def ring_copies(pairs, sem, idx, ring):
    s = lax.rem(idx, ring)
    return [pltpu.make_async_copy(src.at[idx], dst.at[s], sem.at[s, i]) for i, (src, dst) in enumerate(pairs)]


def row_copies(refs, rows, sem):
    tokens = rows.shape[0] // len(refs)
    return [pltpu.make_async_copy(ref.at[0:tokens], rows.at[r * tokens:(r + 1) * tokens], sem.at[r]) for r, ref in enumerate(refs)]


def info_copy(load, info, sem):
    depth, width = info.shape
    first = load.shape[0] - depth
    return pltpu.make_async_copy(load.at[first:first + depth, 0:width], info, sem)


def hits(slot_row, tokens, capacity):
    source = lax.broadcasted_iota(jnp.int32, slot_row.shape, 1) // tokens
    col_row = jnp.where(slot_row >= 0.0, slot_row.astype(jnp.int32) + source * capacity, -1)
    return lax.broadcasted_iota(jnp.int32, (4 * capacity, slot_row.shape[1]), 0) == col_row


def start_all(copies, priority=0):
    for c in copies:
        c.start(priority=priority)


def wait_all(copies):
    for c in copies:
        c.wait()


def keep_routes(slots, gates, q, slot_row, gate_row):
    slots[pl.ds(q, 1), :] = slot_row
    gates[pl.ds(q, 1), :] = gate_row


def stash(outs, q, capacity, lanes, res):
    for r in range(outs.shape[0]):
        outs[r, pl.ds(pl.multiple_of(q * BLOCK, BLOCK), capacity), lanes] = res[r * capacity:(r + 1) * capacity].astype(BF)


def mix_into(acc, outs, slots, gates, q, weighted, order, after=lambda r: r):
    tokens = acc.shape[0] // outs.shape[0]
    depth = lax.broadcasted_iota(jnp.int32, (BLOCK, tokens), 0).astype(F32)
    for r in order:
        lanes = slice(r * tokens, (r + 1) * tokens)
        blocks = []
        for k in range(QUAD):
            weight = gates[k:k + 1, lanes] if weighted else 1.0
            slot = jnp.where(q >= k, slots[k:k + 1, lanes], -1.0)
            blocks.append(jnp.where(depth == slot, weight, 0.0))
        pick = jnp.transpose(jnp.concatenate(blocks, axis=0).astype(BF))
        for n in range(acc.shape[1] // 512):
            part = slice(n * 512, (n + 1) * 512)
            acc[lanes, part] += nn(pick, outs[r, :, part])
        after(r)


def expert_bwd_kernel(capacity, loads, u_h, w1_h, w2_h, w3_h,
                      g1, g2, g3, p0, p1, p2, p3, s_hid, s_da1, s_da3, s_do,
                      rows, info, us, w1s, w2s, w3s, slots, gates, du_all, d_out, hid, da1, da3, o1, o2, o3, acc, rsem, wsem, sems, psem, ksem):
    e = pl.program_id(0)
    count = pl.num_programs(0)
    me = lax.axis_index('expert')
    slot_e = lax.rem(e, 2)
    ring, _, model = us.shape
    tokens = rows.shape[0] // 4
    ff = w1s.shape[2]
    order = [jnp.bitwise_xor(me, r) for r in range(4)]
    arrivals = row_copies([loads.at[p] for p in order], rows, rsem) + [info_copy(loads.at[p], info.at[r], rsem.at[4 + r]) for r, p in enumerate(order)]
    pairs = ((u_h, us), (w1_h, w1s), (w3_h, w3s), (w2_h, w2s))

    @pl.when(e == 0)
    def _():
        start_all(arrivals + ring_copies(pairs, wsem, 0, ring) + ring_copies(pairs, wsem, 1, ring))
        acc[...] = jnp.zeros_like(acc)
        du_all[...] = jnp.zeros_like(du_all)
        wait_all(arrivals)

    @pl.when(e + 2 < count)
    def _():
        start_all(ring_copies(pairs, wsem, e + 2, ring))

    slot_row, gate_row = route_rows(info, 1, me * count + e)
    q = lax.rem(e, QUAD)
    keep_routes(slots, gates, q, slot_row, gate_row)
    hot = hits(slot_row, tokens, capacity)
    d_out[...] = nn(jnp.where(hot, gate_row, 0.0).astype(BF), rows[...]).astype(BF)

    def flush(idx):
        s = lax.rem(idx, 2)
        return [pltpu.make_async_copy(src.at[s], dst.at[idx], sems.at[s, i]) for i, (src, dst) in enumerate(((o1, g1), (o2, g2), (o3, g3)))]

    wait_all(ring_copies(pairs, wsem, e, ring))
    now = lax.rem(e, ring)
    u, w1, w2, w3 = us.at[now], w1s.at[now], w2s.at[now], w3s.at[now]
    uv = u[...]
    dov = d_out[...]
    for n in range(ff // 256):
        part = slice(n * 256, (n + 1) * 256)
        pre1 = nn(uv, w1[:, part]).astype(BF).astype(F32)
        pre3 = nn(uv, w3[:, part]).astype(BF).astype(F32)
        grad_hid = nt(dov, w2[part, :]).astype(BF).astype(F32)
        sigma = jax.nn.sigmoid(pre1)
        silu = pre1 * sigma
        hid[:, part] = (silu * pre3).astype(BF)
        da1[:, part] = (grad_hid * pre3 * sigma * (1.0 + pre1 * (1.0 - sigma))).astype(BF)
        da3[:, part] = (grad_hid * silu).astype(BF)

    keeps = [pltpu.make_async_copy(src, dst, ksem.at[i]) for i, (src, dst) in enumerate(((hid, s_hid), (da1, s_da1), (da3, s_da3), (d_out, s_do)))]

    @pl.when((e >= 2) & (e < count - 1))
    def _():
        wait_all(flush(e - 2))

    @pl.when(e < count - 1)
    def _():
        fresh = flush(e)
        for m in range(ff // 256):
            part = slice(m * 256, (m + 1) * 256)
            o2[slot_e, part] = tn(hid[:, part], d_out[...])
        fresh[1].start()
        for m in range(model // 256):
            part = slice(m * 256, (m + 1) * 256)
            o1[slot_e, part] = tn(u[:, part], da1[...])
        fresh[0].start()
        for m in range(model // 256):
            part = slice(m * 256, (m + 1) * 256)
            o3[slot_e, part] = tn(u[:, part], da3[...])
        fresh[2].start()

    @pl.when(e == count - 1)
    def _():
        start_all(keeps)

    for n in range(model // 256):
        part = slice(n * 256, (n + 1) * 256)
        stash(du_all, q, capacity, part, nt(da1[...], w1[part]) + nt(da3[...], w3[part]))

    @pl.when((q == QUAD - 1) | (e == count - 1))
    def _():
        mix_into(acc, du_all, slots, gates, q, False, range(QUAD))

    @pl.when(e == count - 1)
    def _():
        sends = [pltpu.make_async_copy(acc.at[pl.ds(pl.multiple_of(p * tokens, tokens), tokens)], ref, psem.at[r]) for r, (p, ref) in enumerate(zip(order, (p0, p1, p2, p3)))]
        start_all(sends)
        wait_all(keeps)
        wait_all(flush(e - 2))
        wait_all(flush(e - 1))
        wait_all(sends)


def expert_bwd(loads, u, w1, w2, w3, tokens):
    model = loads.shape[2]
    count, cols, _ = u.shape
    ff = w1.shape[2]
    ring = 3
    hb = pl.BlockSpec(memory_space=pl.ANY)
    keep = jax.ShapeDtypeStruct((cols, ff), BF)
    part = jax.ShapeDtypeStruct((tokens, model), F32)
    return pl.pallas_call(
        functools.partial(expert_bwd_kernel, cols // 4),
        grid=(count,),
        out_shape=(jax.ShapeDtypeStruct((count, model, ff), F32), jax.ShapeDtypeStruct((count, ff, model), F32), jax.ShapeDtypeStruct((count, model, ff), F32), part, part, part, part, keep, keep, keep, jax.ShapeDtypeStruct((cols, model), BF)),
        in_specs=[hb] * 5,
        out_specs=(hb,) * 11,
        scratch_shapes=[
            pltpu.VMEM((4 * tokens, model), BF), pltpu.VMEM((4, loads.shape[1] - tokens, 3 * tokens), BF),
            pltpu.VMEM((ring, cols, model), BF), pltpu.VMEM((ring, model, ff), BF), pltpu.VMEM((ring, ff, model), BF), pltpu.VMEM((ring, model, ff), BF),
            pltpu.VMEM((8, 4 * tokens), F32), pltpu.VMEM((8, 4 * tokens), F32), pltpu.VMEM((4, QUAD * BLOCK, model), BF),
            pltpu.VMEM((cols, model), BF), pltpu.VMEM((cols, ff), BF), pltpu.VMEM((cols, ff), BF), pltpu.VMEM((cols, ff), BF),
            pltpu.VMEM((2, model, ff), F32), pltpu.VMEM((2, ff, model), F32), pltpu.VMEM((2, model, ff), F32),
            pltpu.VMEM((4 * tokens, model), F32),
            pltpu.SemaphoreType.DMA((8,)), pltpu.SemaphoreType.DMA((ring, 4)), pltpu.SemaphoreType.DMA((2, 3)), pltpu.SemaphoreType.DMA((4,)), pltpu.SemaphoreType.DMA((4,)),
        ],
        compiler_params=pltpu.CompilerParams(vmem_limit_bytes=VMEM_BYTES, dimension_semantics=("arbitrary",)),
        cost_estimate=pl.CostEstimate(flops=50 * 10 ** 9, bytes_accessed=150 * 10 ** 6, transcendentals=0),
        name="expert_bwd",
    )(loads, u, w1, w2, w3)


def expert_fwd_kernel(capacity, u0, u1, u2, u3, loads, b0, b1, b2, b3, w1_h, w2_h, w3_h, du_o, mine_o, out_o,
                      rows, info, w1s, w2s, w3s, slots, gates, out_all, acc, loc0, loc2, rx1, rx3, rxf, ra1, ra3, dus, rsem, wsem, bsem, ssem, xsem, osem):
    e = pl.program_id(0)
    count = pl.num_programs(0)
    me = lax.axis_index('expert')
    near, far = neighbours()
    ring, model, ff = w1s.shape
    q = e % QUAD
    tokens = rows.shape[0] // 4
    arrivals = row_copies((u0, u1, u2, u3), rows, rsem) + [info_copy(loads.at[r], info.at[r], rsem.at[4 + r]) for r in range(4)]
    pairs = ((w1_h, w1s), (w3_h, w3s), (w2_h, w2s))
    local = [pltpu.make_async_copy(b0, loc0, bsem.at[0]), pltpu.make_async_copy(b2, loc2, bsem.at[1])]
    swap3 = remote(b3, rx3, ssem.at[0], xsem.at[0], near)
    swap1 = remote(b1, rx1, ssem.at[1], xsem.at[1], near)
    over = remote(loc2, rxf, ssem.at[2], xsem.at[2], far)
    part = [slice(r * tokens, (r + 1) * tokens) for r in range(4)]
    late3 = remote(acc.at[part[3]], ra3, ssem.at[3], xsem.at[3], near)
    late1 = remote(acc.at[part[1]], ra1, ssem.at[4], xsem.at[4], near)

    @pl.when(e == 0)
    def _():
        start_all(arrivals + local)
        start_all(ring_copies(pairs, wsem, 0, ring) + ring_copies(pairs, wsem, 1, ring), 1)
        greet((near, far))
        swap3.start()
        acc[...] = jnp.zeros_like(acc)
        out_all[...] = jnp.zeros_like(out_all)
        wait_all(arrivals)

    @pl.when(e == 1)
    def _():
        wait_all(local)
        swap3.wait()
        loc2[...] += rx3[...]
        over.start()
        swap1.start()

    @pl.when(e + 2 < count)
    def _():
        start_all(ring_copies(pairs, wsem, e + 2, ring), 1)

    slot_row, gate_row = route_rows(info, 0, me * count + e)
    keep_routes(slots, gates, q, slot_row, gate_row)
    v = nn(jnp.where(hits(slot_row, tokens, capacity), 1.0, 0.0).astype(BF), rows[...]).astype(BF)
    wait_all(ring_copies(pairs, wsem, e, ring))
    now = e % ring
    w1, w2, w3 = w1s.at[now], w2s.at[now], w3s.at[now]
    pieces = []
    for n in range(ff // 256):
        lanes = slice(n * 256, (n + 1) * 256)
        a1 = nn(v, w1[:, lanes]).astype(BF).astype(F32)
        a3 = nn(v, w3[:, lanes]).astype(BF).astype(F32)
        pieces.append((a1 * jax.nn.sigmoid(a1) * a3).astype(BF))
    hidden = jnp.concatenate(pieces, axis=1)
    for n in range(model // 256):
        lanes = slice(n * 256, (n + 1) * 256)
        stash(out_all, q, capacity, lanes, nn(hidden, w2[:, lanes]))

    final = e == count - 1

    @pl.when((q == QUAD - 1) & jnp.logical_not(final))
    def _():
        mix_into(acc, out_all, slots, gates, q, True, range(QUAD))

    @pl.when(final)
    def _():
        late = {3: late3, 1: late1}
        mix_into(acc, out_all, slots, gates, q, True, (3, 1, 2, 0), lambda r: late[r].start() if r in late else r)
        to_du, to_out, to_mine = [pltpu.make_async_copy(src, dst, osem.at[i]) for i, (src, dst) in enumerate(((dus, du_o), (loc2, out_o), (loc0, mine_o)))]
        swap1.wait()
        over.wait()
        dus[...] = ((loc0[...] + rx1[...]) + rxf[...]).astype(BF)
        to_du.start()
        late3.wait()
        loc2[...] = acc[part[2]] + ra3[...]
        to_out.start()
        late1.wait()
        loc0[...] = acc[part[0]] + ra1[...]
        to_mine.start()
        wait_all((to_du, to_out, to_mine))


def expert_fwd(us, loads, sums, w1, w2, w3, capacity):
    tokens, model = us[0].shape
    count, _, ff = w1.shape
    ring = 3
    part = jax.ShapeDtypeStruct((tokens, model), F32)
    hb = pl.BlockSpec(memory_space=pl.ANY)
    tile = pltpu.VMEM((tokens, model), F32)
    return pl.pallas_call(
        functools.partial(expert_fwd_kernel, capacity),
        grid=(count,),
        out_shape=(jax.ShapeDtypeStruct((tokens, model), BF), part, part),
        in_specs=[hb] * 12,
        out_specs=(hb,) * 3,
        scratch_shapes=[
            pltpu.VMEM((4 * tokens, model), BF), pltpu.VMEM((4, loads.shape[1] - tokens, 3 * tokens), BF),
            pltpu.VMEM((ring, model, ff), BF), pltpu.VMEM((ring, ff, model), BF), pltpu.VMEM((ring, model, ff), BF),
            pltpu.VMEM((8, 4 * tokens), F32), pltpu.VMEM((8, 4 * tokens), F32), pltpu.VMEM((4, QUAD * BLOCK, model), BF), pltpu.VMEM((4 * tokens, model), F32),
            tile, tile, tile, tile, tile, tile, tile, pltpu.VMEM((tokens, model), BF),
            pltpu.SemaphoreType.DMA((8,)), pltpu.SemaphoreType.DMA((ring, 3)), pltpu.SemaphoreType.DMA((2,)), pltpu.SemaphoreType.DMA((5,)), pltpu.SemaphoreType.DMA((5,)), pltpu.SemaphoreType.DMA((3,)),
        ],
        compiler_params=pltpu.CompilerParams(vmem_limit_bytes=VMEM_BYTES, dimension_semantics=("arbitrary",), collective_id=1, has_side_effects=True),
        cost_estimate=pl.CostEstimate(flops=16 * 10 ** 9, bytes_accessed=50 * 10 ** 6, transcendentals=0),
        name="expert_fwd",
    )(*us, loads, *sums, w1, w2, w3)


def solution(mesh):
    group = mesh.shape['expert']

    def hop(value, bits):
        return lax.ppermute(value, 'expert', [(i, i ^ bits) for i in range(group)])

    def local_step(x_a, x_b, dy_b, eid_a, slot_a, gate_a, eid_b, slot_b, gate_b, u_b, norm_1, norm_2, w_q, w_k, w_v, w_o, w_1, w_2, w_3):
        model, heads, dim = w_q.shape
        kv_heads = w_k.shape[1]
        reps = heads // kv_heads
        wq_t, wk_t, wv_t = (w.transpose(1, 2, 0).reshape(-1, model) for w in (w_q, w_k, w_v))
        wo = w_o.reshape(-1, model)
        fields = [a.T for a in (eid_a, slot_a, gate_a, eid_b, slot_b, gate_b)]
        h_a, u_a, h_b, nb, qkv_b, ctx_b, loads = attn_fwd(x_a, x_b, dy_b, fields, norm_1, norm_2, wq_t, wk_t, wv_t, wo, kv_heads, reps, dim)
        us = (u_a, hop(u_a, 1), hop(u_a, 2), hop(u_a, 3))
        g1, g2, g3, *rest = expert_bwd(loads, u_b, w_1, w_2, w_3, x_a.shape[0])
        du, mine_a, out_a = expert_fwd(us, loads, rest[0:4], w_1, w_2, w_3, u_b.shape[1] // group)
        far_a = hop(out_a, 2)
        dx_b, g_q, g_k, g_v, g_o, g_n1, g_n2, g1, g2, g3 = attn_bwd(du, dy_b, h_b, x_b, nb, qkv_b, ctx_b, norm_1, norm_2, wo, wq_t, wk_t, wv_t, (g1, g2, g3), u_b, rest[4:8], kv_heads, reps, dim)
        y_a = (h_a.astype(F32) + (mine_a + far_a)).astype(BF)
        g_q = g_q.reshape(heads, dim, model).transpose(2, 0, 1)
        g_k = g_k.reshape(kv_heads, dim, model).transpose(2, 0, 1)
        g_v = g_v.reshape(kv_heads, dim, model).transpose(2, 0, 1)
        g_o = g_o.reshape(heads, dim, model)
        return (y_a, dx_b, g1, g2, g3, g_q[None], g_k[None], g_v[None], g_o[None], g_n1, g_n2)

    row_spec = P(('data', 'expert'), None)
    cube_spec = P(('data', 'expert'), None, None)
    quad_spec = P(('data', 'expert'), None, None, None)
    expert_spec = P('expert', None, None)
    in_specs = (row_spec, row_spec, row_spec, row_spec, row_spec, row_spec, row_spec, row_spec, row_spec, cube_spec, P(), P(), P(), P(), P(), P(), expert_spec, expert_spec, expert_spec)
    out_specs = (row_spec, row_spec, cube_spec, cube_spec, cube_spec, quad_spec, quad_spec, quad_spec, quad_spec, row_spec, row_spec)
    return jax.shard_map(local_step, mesh=mesh, in_specs=in_specs, out_specs=out_specs, check_vma=False)
```
